32 devices in a mesh: dp: 8 (over z, core), mp: 4 (over y, x).
Axes of the slice: x: 2, y: 2, z: 4, core: 2. Of those that a mesh axis runs over, the one named last changes fastest.
Arguments:
- hidden_states: bfloat16 [32, 640, 1280], P(('dp', 'mp')), may hold values from -6 to 6
- ln_attn_gain: float32 [1280], replicated, may hold values from 0.1 to 1.9
- w_qkv: bfloat16 [1280, 16, 192], P(None, 'mp'), may hold values from -0.15625 to 0.15625
- output_weight: bfloat16 [64, 16, 1280], P(None, 'mp'), may hold values from -0.75 to 0.75
- ln_final_gain: float32 [1280], replicated, may hold values from 0.1 to 1.9
- dense_weight: bfloat16 [1280, 1280], replicated, may hold values from -0.15625 to 0.15625
- decoder_weight: bfloat16 [1280, 33], replicated, may hold values from -0.5390625 to 0.5390625
- decoder_bias: float32 [33], replicated, may hold values from -4 to 4
- seq_tokens: int32 [24, 640], replicated, may hold values from 4 to 23
- seq_lengths: int32 [24], replicated, may hold values from 128 to 640
- copy_sequence: int32 [32], replicated, may hold values from 0 to 23
- mask_code: int32 [32, 64], replicated, may hold values from 0 to 1048575
- copy_owner: int32 [32], replicated, may hold values from 0 to 31, each once
Outputs:
- pll: float32 [32, 64], P('dp', 'mp')
The draws below stay inside these ranges and needn't reach their ends.
Inputs may be any that keep to these rules, and one draw needn't show every extreme that they name: `seq_tokens`: amino-acid token ids. `copy_owner`: every row of pll is named by exactly one copy.
All inputs are finite; a program needn't handle non-finite values.
Results may differ from the reference program's by a relative error of at most 0.0038.
Values may be sent and summed in bfloat16 or wider, within the bound.
A program may use at most 128 MiB of HBM per device.

```python
import jax
import jax.numpy as jnp
from jax import lax

D = 1280
HD = 64
VOCAB = 33
HEADS = 16
LMAX = 640
MASKS = 64
SEQS = 24
COPIES = 32


def place_ends(entries, own_key, low, high):
    longest = entries.shape.index(max(entries.shape))
    spots = []
    for shift in (0, 1):
        where = [jax.random.randint(jax.random.fold_in(own_key, axis), (), 0, length) for axis, length in enumerate(entries.shape)]
        where[longest] = (where[longest] + shift) % entries.shape[longest]
        spots.append(tuple(where))
    return entries.at[spots[0]].set(low).at[spots[1]].set(high)


def levels(stream_key, dims, split, least, high):
    loudness, own = 1.0, jax.random.fold_in(stream_key, 6)
    for axis_at, blocks in split:
        steps = jnp.exp(jax.random.uniform(jax.random.fold_in(own, axis_at), (blocks,), jnp.float32, least / len(split), high / len(split)))
        loudness = loudness * jnp.repeat(steps, dims[axis_at] // blocks).reshape([-1 if axis == axis_at else 1 for axis in range(len(dims))])
    return loudness


def bell_draw(key, shape, spread, limit, cuts=(), kind=jnp.bfloat16):
    loudness = levels(key, shape, cuts, -0.22, 0.18) if cuts else 1.0
    array = jax.random.normal(key, shape, jnp.float32) * spread * loudness
    return jnp.minimum(jnp.maximum(array, -limit), limit).astype(kind)


def setup_inputs(seed: int = 0) -> dict:
    streams_of = jax.random.split(jax.random.key(seed), 14)
    hidden_states = bell_draw(streams_of[0], (COPIES, LMAX, D), 1.0, 6.0, ((0, 32),))
    ln_attn_gain = jnp.clip(1.0 + 0.18 * jax.random.normal(streams_of[1], (D,), jnp.float32), 0.1, 1.9)
    w_qkv = bell_draw(streams_of[2], (D, HEADS, 3 * HD), D ** -0.5, 0.15625, ((1, 4),))
    output_weight = bell_draw(streams_of[3], (HD, HEADS, D), 0.125, 0.75, ((1, 4),))
    ln_final_gain = jnp.clip(1.0 + 0.18 * jax.random.normal(streams_of[4], (D,), jnp.float32), 0.1, 1.9)
    dense_weight = bell_draw(streams_of[5], (D, D), D ** -0.5, 0.15625)
    decoder_weight = bell_draw(streams_of[6], (D, VOCAB), 0.09, 0.5390625)
    decoder_bias = bell_draw(streams_of[7], (VOCAB,), 1.0, 4.0, (), jnp.float32)
    seq_tokens = place_ends(jax.random.randint(streams_of[8], (SEQS, LMAX), 4, 24), jax.random.fold_in(streams_of[8], 1), 4, 23).astype(jnp.int32)
    seq_lengths = place_ends(jax.random.randint(streams_of[9], (SEQS,), LMAX // 5, LMAX + 1), jax.random.fold_in(streams_of[9], 1), LMAX // 5, LMAX).astype(jnp.int32)
    copy_sequence = place_ends(jax.random.randint(streams_of[10], (COPIES,), 0, SEQS), jax.random.fold_in(streams_of[10], 1), 0, SEQS - 1).astype(jnp.int32)
    mask_code = place_ends(jax.random.randint(streams_of[11], (COPIES, MASKS), 0, 1048576), jax.random.fold_in(streams_of[11], 1), 0, 1048575).astype(jnp.int32)
    copy_owner = jax.random.permutation(streams_of[12], COPIES).astype(jnp.int32)
    return {"hidden_states": hidden_states, "ln_attn_gain": ln_attn_gain, "w_qkv": w_qkv, "output_weight": output_weight, "ln_final_gain": ln_final_gain, "dense_weight": dense_weight, "decoder_weight": decoder_weight, "decoder_bias": decoder_bias, "seq_tokens": seq_tokens, "seq_lengths": seq_lengths, "copy_sequence": copy_sequence, "mask_code": mask_code, "copy_owner": copy_owner}


epsilon = 1e-05

def layer_norm(inputs):
    average = lax.optimization_barrier(jnp.mean(inputs, axis=-1, keepdims=True))
    centred = inputs - average
    variance = lax.optimization_barrier(jnp.mean(centred * centred, axis=-1, keepdims=True))
    return centred * lax.rsqrt(variance + epsilon)

def rotary_tables(seq_span, head_size):
    half_width = head_size // 2
    frequency = 1.0 / 10000.0 ** (jnp.arange(half_width, dtype=jnp.float32) * (2.0 / head_size))
    angles = jnp.arange(seq_span, dtype=jnp.float32)[:, None] * frequency[None, :]
    angles = jnp.concatenate([angles, angles], axis=-1)
    return (jnp.cos(angles), jnp.sin(angles))

def rotate(inputs, cosine, sine):
    half_width = inputs.shape[-1] // 2
    turned = jnp.concatenate([-inputs[..., half_width:], inputs[..., :half_width]], axis=-1)
    return inputs * cosine + turned * sine

def score_rows(residual, ln_final_gain, dense_weight, decoder_weight, decoder_bias, targets):
    feature = residual.shape[-1]
    normed_final = (layer_norm(residual) * ln_final_gain).astype(jnp.bfloat16).reshape(-1, feature)
    dense_out = jnp.dot(normed_final, dense_weight, preferred_element_type=jnp.float32)
    headed = layer_norm(jax.nn.gelu(dense_out, approximate=False)).astype(jnp.bfloat16)
    logits = jnp.dot(headed, decoder_weight, preferred_element_type=jnp.float32) + decoder_bias
    log_probs = logits - jax.nn.logsumexp(logits, axis=-1, keepdims=True)
    vocab_ids = jnp.arange(logits.shape[-1], dtype=jnp.int32)
    flat_targets = targets.reshape(-1)
    picked = lax.optimization_barrier(jnp.sum(jnp.where(flat_targets[:, None] == vocab_ids[None, :], log_probs, 0.0), axis=-1))
    return picked.reshape(targets.shape)

def one_copy(states, length, positions, ln_attn_gain, w_qkv, output_weight, cosine, sine):
    seq_span, feature = states.shape
    head_count = w_qkv.shape[1]
    head_size = w_qkv.shape[2] // 3
    normed = (layer_norm(states.astype(jnp.float32)) * ln_attn_gain).astype(jnp.bfloat16)
    projected = jnp.dot(normed, w_qkv.reshape(feature, -1), preferred_element_type=jnp.float32)
    projected = projected.reshape(seq_span, head_count, 3, head_size)
    key_matrix = rotate(projected[:, :, 1], cosine[:, None, :], sine[:, None, :]).astype(jnp.bfloat16)
    value_matrix = projected[:, :, 2].astype(jnp.bfloat16)
    query_matrix = projected[positions, :, 0] * head_size ** (-0.5)
    query_matrix = rotate(query_matrix, cosine[positions][:, None, :], sine[positions][:, None, :]).astype(jnp.bfloat16)
    attention_logits = jnp.einsum('fop,yop->ofy', query_matrix.astype(jnp.float32), key_matrix.astype(jnp.float32))
    alive = jnp.arange(seq_span, dtype=jnp.int32) < length
    attention_logits = jnp.where(alive[None, None, :], attention_logits, -1e+30)
    largest = lax.optimization_barrier(jnp.max(attention_logits, axis=-1, keepdims=True))
    weights = jnp.exp(attention_logits - largest)
    attention_probs = (weights / lax.optimization_barrier(jnp.sum(weights, axis=-1, keepdims=True))).astype(jnp.bfloat16)
    context_vectors = jnp.einsum('vuy,yvx->uvx', attention_probs.astype(jnp.float32), value_matrix.astype(jnp.float32)).astype(jnp.bfloat16)
    attention_mixed = jnp.einsum('frn,nrl->fl', context_vectors.astype(jnp.float32), output_weight.astype(jnp.float32))
    return states[positions].astype(jnp.float32) + attention_mixed

def reference(hidden_states, ln_attn_gain, w_qkv, output_weight, ln_final_gain, dense_weight, decoder_weight, decoder_bias, seq_tokens, seq_lengths, copy_sequence, mask_code, copy_owner):
    cosine, sine = rotary_tables(LMAX, HD)
    lengths = seq_lengths[copy_sequence]
    positions = (mask_code % lengths[:, None]).astype(jnp.int32)
    targets = jnp.take_along_axis(seq_tokens[copy_sequence], positions, axis=1)

    def per_copy(items):
        states, length, spots = items
        return one_copy(states, length, spots, ln_attn_gain, w_qkv, output_weight, cosine, sine)
    residual = lax.map(per_copy, (hidden_states, lengths, positions))
    attention_logits = score_rows(residual, ln_final_gain, dense_weight, decoder_weight, decoder_bias, targets)
    return jnp.zeros_like(attention_logits).at[copy_owner].set(attention_logits)
```

```python
import functools

import jax
import jax.numpy as jnp
import numpy as np
from jax import lax
from jax.experimental import pallas as pl
from jax.experimental.pallas import tpu as pltpu
from jax.sharding import PartitionSpec as P

epsilon = 1e-05
MESH = pl.DeviceIdType.MESH
f32 = jnp.float32
bf16 = jnp.bfloat16
LANES = 128


def layer_norm(inputs):
    average = jnp.mean(inputs, axis=-1, keepdims=True)
    centred = inputs - average
    variance = jnp.mean(centred * centred, axis=-1, keepdims=True)
    return centred * lax.rsqrt(variance + epsilon)


def rotary_tables(seq_span, head_size):
    half = head_size // 2
    frequency = (1.0 / 10000.0 ** (np.arange(half, dtype=np.float32) * (2.0 / head_size))).astype(
        np.float32
    )
    angles = np.arange(seq_span, dtype=np.float32)[:, None] * frequency[None, :]
    cosine, sine = np.cos(angles), np.sin(angles)
    times = LANES // head_size
    return (
        np.tile(np.concatenate([cosine, cosine], axis=1), (1, times)).astype(np.float32),
        np.tile(np.concatenate([-sine, sine], axis=1), (1, times)).astype(np.float32),
    )


def flip(index, mask):
    bit = 1
    out = index
    while bit <= mask:
        if mask & bit:
            out = out + bit * (1 - 2 * ((index // bit) % 2))
        bit *= 2
    return out


def kernel(
    sizes,
    sequence_ref,
    lengths_ref,
    codes_ref,
    tokens_ref,
    owner_ref,
    gain_ref,
    final_gain_ref,
    decoder_ref,
    bias_ref,
    hidden_hbm,
    weight_hbm,
    out_weight_hbm,
    dense_hbm,
    cos_hbm,
    sin_hbm,
    out_ref,
    hidden,
    normed,
    wbuf,
    obuf,
    dense,
    cos,
    sin,
    pbuf,
    context,
    mixed,
    scores,
    local_sem,
    direct_sem,
    relay_sem,
    exchange_sem,
    share_sem,
    arrive_sem,
    shared_sem,
    score_send_sem,
    score_sem,
):
    n_dp, n_mp, head_size, heads_in_chunk, chunks = sizes
    devices = n_dp * n_mp
    dp = lax.axis_index("dp")
    mp = lax.axis_index("mp")
    core = dp % 2
    partner = dp + 1 - 2 * core
    me = dp * n_mp + mp
    seq_span, feature = hidden.shape
    masks = codes_ref.shape[1]
    chunk_heads = heads_in_chunk * head_size
    out_rows = obuf.shape[1]
    piece_rows = out_rows // 4

    def local(index, source, target):
        copy = pltpu.make_async_copy(source, target, local_sem.at[index])
        copy.start()
        return copy

    weight_copy = local(1, weight_hbm, wbuf.at[0])
    hidden_copy = local(0, hidden_hbm, hidden)

    barrier = pltpu.get_barrier_semaphore()

    def greet(step, carry):
        other = (me + step) % devices
        pl.semaphore_signal(
            barrier, inc=1, device_id=(other // n_mp, other % n_mp), device_id_type=MESH
        )
        return carry

    lax.fori_loop(1, devices, greet, 0)

    parity = (dp // 2) % 2
    above = dp + 2 - 4 * parity
    part_rows = wbuf.shape[2] // 4

    def part(chunk, odd):
        return 2 * chunk + odd

    def place(relation, item, half):
        if item < 2 * chunks:
            chunk, odd = divmod(item, 2)
            which = 1 - parity if odd else parity
            start = (2 * half + which) * part_rows
            return wbuf.at[relation, chunk, pl.ds(pl.multiple_of(start, 16), part_rows), :]
        start = (2 * half + item - 2 * chunks) * piece_rows
        return obuf.at[relation, pl.ds(pl.multiple_of(start, 16), piece_rows), :]

    def view(relation, item):
        return place(relation, item, core)

    def partner_view(relation, item):
        return place(relation, item, 1 - core)

    sent = []

    def to_group(target, source_relation, relation, item, semaphore):
        copy = pltpu.make_async_remote_copy(
            src_ref=view(source_relation, item),
            dst_ref=view(relation, item),
            send_sem=semaphore,
            recv_sem=arrive_sem.at[relation, item],
            device_id=(dp, flip(mp, target)),
            device_id_type=MESH,
        )
        copy.start()
        sent.append(copy)

    def direct(target, item):
        to_group(target, 0, target, item, direct_sem.at[target, item])

    def relay(target, source_relation, item):
        to_group(target, source_relation, source_relation ^ target, item, relay_sem.at[item])

    def exchange(relation, chunk):
        copy = pltpu.make_async_remote_copy(
            src_ref=view(relation, part(chunk, 0)),
            dst_ref=view(relation, part(chunk, 0)),
            send_sem=exchange_sem.at[relation, chunk],
            recv_sem=arrive_sem.at[relation, part(chunk, 1)],
            device_id=(above, mp),
            device_id_type=MESH,
        )
        copy.start()
        sent.append(copy)

    def arrived(relation, item):
        landing = view(relation, item)
        pltpu.make_async_copy(landing, landing, arrive_sem.at[relation, item]).wait()

    def share(relation, item):
        copy = pltpu.make_async_remote_copy(
            src_ref=view(relation, item),
            dst_ref=view(relation, item),
            send_sem=share_sem.at[relation, item],
            recv_sem=shared_sem.at[relation, item],
            device_id=(partner, mp),
            device_id_type=MESH,
        )
        copy.start()
        sent.append(copy)

    def was_shared(relation, item):
        landing = partner_view(relation, item)
        pltpu.make_async_copy(landing, landing, shared_sem.at[relation, item]).wait()

    sequence = sequence_ref[me]
    length = lengths_ref[sequence].astype(f32)
    codes = codes_ref[pl.ds(me, 1), :].astype(f32)
    quotient = jnp.floor(codes / length)
    row_positions = codes - quotient * length
    row_positions = jnp.where(row_positions < 0.0, row_positions + length, row_positions)
    row_positions = jnp.where(row_positions >= length, row_positions - length, row_positions)
    eye = lax.broadcasted_iota(jnp.int32, (masks, masks), 0) == lax.broadcasted_iota(
        jnp.int32, (masks, masks), 1
    )
    positions = jnp.sum(jnp.where(eye, row_positions, 0.0), axis=1, keepdims=True)
    places = lax.broadcasted_iota(jnp.int32, (masks, seq_span), 1).astype(f32)
    chosen = places == positions
    onehot = jnp.where(chosen, 1.0, 0.0)
    onehot_bf = onehot.astype(bf16)
    tokens = tokens_ref[pl.ds(sequence, 1), :].astype(f32)
    targets = jnp.sum(jnp.where(chosen, tokens, 0.0), axis=1, keepdims=True)
    alive = lax.broadcasted_iota(jnp.int32, (1, seq_span), 1).astype(f32) < length

    weight_copy.wait()
    pl.semaphore_wait(barrier, devices - 1)
    items = 2 * chunks + 2
    routed = n_mp == 4 and chunks == 2 and n_dp % 4 == 0
    if routed:
        direct(1, part(1, 0))
        direct(2, part(0, 0))
        direct(1, part(0, 0))
        direct(2, part(1, 0))
    cos_copy = local(3, cos_hbm, cos)
    sin_copy = local(4, sin_hbm, sin)
    out_weight_copy = local(2, out_weight_hbm, obuf.at[0])
    dense_copy = local(5, dense_hbm, dense)
    if not routed:
        out_weight_copy.wait()
        for item in range(items):
            for target in range(1, n_mp):
                direct(target, item)

    hidden_copy.wait()
    tile = 128 if seq_span % 128 == 0 else 8

    def norm_rows(step, carry):
        rows = pl.ds(pl.multiple_of(step * tile, tile), tile)
        normed[rows, :] = (layer_norm(hidden[rows, :].astype(f32)) * gain_ref[...].reshape(1, feature)).astype(bf16)
        return carry

    lax.fori_loop(0, seq_span // tile, norm_rows, 0)
    masked_rows = jnp.dot(onehot_bf, normed[...], preferred_element_type=f32).astype(bf16)
    own_rows = jnp.dot(onehot_bf, hidden[...], preferred_element_type=f32)
    mixed[...] = own_rows
    cos_copy.wait()
    sin_copy.wait()
    exact = dict(preferred_element_type=f32, precision=lax.Precision.HIGHEST)
    query_cos = jnp.dot(onehot, cos[...], **exact)
    query_sin = jnp.dot(onehot, sin[...], **exact)
    lane = lax.broadcasted_iota(jnp.int32, (1, LANES), 1)
    first = lane % head_size < head_size // 2

    def rotate(inputs, cosine, sine):
        turned = jnp.where(
            first,
            pltpu.roll(inputs, LANES - head_size // 2, 1),
            pltpu.roll(inputs, head_size // 2, 1),
        )
        return inputs * cosine + turned * sine

    transposed = (((1,), (1,)), ((), ()))
    low = lane < head_size
    span = seq_span // 2 if seq_span % 32 == 0 else seq_span
    head_rows = 3 * head_size

    def attend(relation, chunk):
        weights = wbuf.at[relation, chunk]
        pairs = [
            weights[head * head_rows + head_size : (head + 1) * head_rows, :]
            for head in range(heads_in_chunk)
        ]
        pair_weights = pairs[0] if heads_in_chunk == 1 else jnp.concatenate(pairs, axis=0)

        def project(step, carry):
            rows = pl.ds(pl.multiple_of(step * span, 16), span)
            made = lax.dot_general(
                normed[rows, :], pair_weights, transposed, preferred_element_type=f32
            )
            for head in range(heads_in_chunk):
                block = made[:, head * LANES : (head + 1) * LANES]
                block = jnp.where(low, rotate(block, cos[rows, :], sin[rows, :]), block)
                pbuf[rows, head * LANES : (head + 1) * LANES] = block.astype(bf16)
            return carry

        lax.fori_loop(0, seq_span // span, project, 0)
        if heads_in_chunk == 1:
            query_weights = weights[: 2 * head_size, :]
        else:
            query_weights = jnp.concatenate(
                [weights[:head_size, :], weights[head_rows : head_rows + head_size, :]], axis=0
            )
        made = lax.dot_general(masked_rows, query_weights, transposed, preferred_element_type=f32)
        turned = rotate(made * head_size ** (-0.5), query_cos, query_sin)
        vectors = []
        for head in range(heads_in_chunk):
            query = turned if head == 0 else pltpu.roll(turned, head_size, 1)
            query = jnp.where(low, query, 0.0).astype(bf16)
            block = pbuf[:, head * LANES : (head + 1) * LANES]
            logits = lax.dot_general(query, block, transposed, preferred_element_type=f32)
            logits = jnp.where(alive, logits, -1e30)
            weight = jnp.exp(logits - jnp.max(logits, axis=-1, keepdims=True))
            probs = (weight / jnp.sum(weight, axis=-1, keepdims=True)).astype(bf16)
            vectors.append(jnp.dot(probs, block, preferred_element_type=f32))
        total = pltpu.roll(vectors[0], head_size, 1)
        if heads_in_chunk > 1:
            total = jnp.where(low, total, vectors[1])
        context[relation, chunk] = total[:, :chunk_heads].astype(bf16)

    def mix(relation):
        for chunk in range(chunks):
            rows = slice(chunk * chunk_heads, (chunk + 1) * chunk_heads)
            mixed[...] += jnp.dot(
                context[relation, chunk], obuf[relation, rows, :], preferred_element_type=f32
            )

    def fetch(*pairs):
        for pair in pairs:
            arrived(*pair)
            share(*pair)

    def attend_shared(relation, chunk):
        was_shared(relation, part(chunk, 0))
        was_shared(relation, part(chunk, 1))
        attend(relation, chunk)

    attend(0, 0)
    if routed:
        first_piece, second_piece = 2 * chunks, 2 * chunks + 1
        arrived(1, part(1, 0))
        relay(2, 1, part(1, 0))
        exchange(1, 1)
        share(1, part(1, 0))
        arrived(2, part(0, 0))
        relay(1, 2, part(0, 0))
        exchange(2, 0)
        share(2, part(0, 0))
        direct(1, part(0, 1))
        direct(2, part(1, 1))
        out_weight_copy.wait()
        direct(1, first_piece)
        direct(2, second_piece)
        direct(1, second_piece)
        direct(2, first_piece)
    for chunk in range(1, chunks):
        attend(0, chunk)
    mix(0)
    if routed:
        fetch((1, part(0, 0)), (2, part(1, 0)), (1, part(1, 1)))
        arrived(3, part(0, 0))
        exchange(3, 0)
        share(3, part(0, 0))
        arrived(3, part(1, 0))
        exchange(3, 1)
        share(3, part(1, 0))
        fetch((2, part(0, 1)))
        attend_shared(1, 1)
        attend_shared(2, 0)
        fetch((1, part(0, 1)), (2, part(1, 1)), (3, part(0, 1)))
        attend_shared(1, 0)
        arrived(1, first_piece)
        relay(2, 1, first_piece)
        share(1, first_piece)
        arrived(2, second_piece)
        relay(1, 2, second_piece)
        share(2, second_piece)
        attend_shared(2, 1)
        fetch((3, part(1, 1)))
        attend_shared(3, 0)
        fetch((1, second_piece), (2, first_piece))
        attend_shared(3, 1)
        for relation in (1, 2):
            was_shared(relation, first_piece)
            was_shared(relation, second_piece)
            mix(relation)
        fetch((3, first_piece), (3, second_piece))
        was_shared(3, first_piece)
        was_shared(3, second_piece)
        mix(3)
    else:
        for relation in range(1, n_mp):
            fetch(*[(relation, item) for item in range(items)])
        for relation in range(1, n_mp):
            for item in range(items):
                was_shared(relation, item)
            for chunk in range(chunks):
                attend(relation, chunk)
            mix(relation)

    normed_final = (layer_norm(mixed[...]) * final_gain_ref[...].reshape(1, feature)).astype(bf16)
    dense_copy.wait()
    dense_out = jnp.dot(normed_final, dense[...], preferred_element_type=f32)
    headed = layer_norm(0.5 * dense_out * (1.0 + lax.erf(dense_out * 0.5**0.5))).astype(bf16)
    logits = lax.dot_general(headed, decoder_ref[...], transposed, preferred_element_type=f32) + bias_ref[...]
    largest = jnp.max(logits, axis=-1, keepdims=True)
    scale = jnp.log(jnp.sum(jnp.exp(logits - largest), axis=-1, keepdims=True)) + largest
    vocabulary = lax.broadcasted_iota(jnp.int32, logits.shape, 1).astype(f32)
    picked = jnp.sum(jnp.where(vocabulary == targets, logits - scale, 0.0), axis=1, keepdims=True)
    row = jnp.sum(jnp.where(eye, picked, 0.0), axis=0, keepdims=True)
    padded = jnp.pad(row, ((0, 0), (0, LANES - masks)))
    scores[me] = jnp.broadcast_to(padded, scores.shape[1:])

    def score_copy(step):
        other = (me + step) % devices
        return pltpu.make_async_remote_copy(
            src_ref=scores.at[me, pl.ds(0, 1), :],
            dst_ref=scores.at[me, pl.ds(0, 1), :],
            send_sem=score_send_sem.at[step],
            recv_sem=score_sem.at[me],
            device_id=(other // n_mp, other % n_mp),
            device_id_type=MESH,
        )

    def send_scores(step, carry):
        score_copy(step).start()
        return carry

    lax.fori_loop(1, devices, send_scores, 0)
    for copy in sent:
        copy.wait_send()

    def wait_scores(step, carry):
        source = (me + step) % devices
        landing = scores.at[source, pl.ds(0, 1), :]
        pltpu.make_async_copy(landing, landing, score_sem.at[source]).wait()
        return carry

    lax.fori_loop(1, devices, wait_scores, 0)

    def wait_sends(step, carry):
        score_copy(step).wait_send()
        return carry

    lax.fori_loop(1, devices, wait_sends, 0)
    group = out_ref.shape[0]
    wanted = dp * group + lax.broadcasted_iota(jnp.int32, (group, owner_ref.shape[1]), 0)
    select = jnp.where(owner_ref[...] == wanted, 1.0, 0.0)
    out_ref[...] = jnp.dot(select, scores[:, 0, :], **exact)


KF, VF, QF, OF, KS, VS, QS, OS = range(8)


def split_kernel(
    sizes,
    sequence_ref,
    lengths_ref,
    codes_ref,
    tokens_ref,
    owner_ref,
    gain_ref,
    final_gain_ref,
    decoder_ref,
    bias_ref,
    hidden_hbm,
    weight_hbm,
    out_weight_hbm,
    dense_hbm,
    cos_hbm,
    sin_hbm,
    split_hbm,
    out_ref,
    hidden,
    normed,
    rows_buf,
    wbuf,
    obuf,
    dense,
    cos,
    sin,
    split,
    pbuf,
    context,
    mixed,
    inbox,
    scores,
    local_sem,
    send_sem,
    arrive_sem,
    norm_send_sem,
    norm_sem,
    swap_send_sem,
    swap_sem,
    score_send_sem,
    score_sem,
    token_sem,
):
    n_dp, n_mp, head_size = sizes
    devices = n_dp * n_mp
    layers = n_dp // 2
    dp = lax.axis_index("dp")
    mp = lax.axis_index("mp")
    core = dp % 2
    layer = dp // 2
    partner = dp + 1 - 2 * core
    me = dp * n_mp + mp
    mate = partner * n_mp + mp
    parity = layer % 2
    above = dp + 2 - 4 * parity
    seq_span, feature = hidden.shape
    masks = codes_ref.shape[1]
    head_rows = 3 * head_size

    barrier = pltpu.get_barrier_semaphore()

    def signal(semaphore, where):
        pl.semaphore_signal(semaphore, inc=1, device_id=where, device_id_type=MESH)

    signal(barrier, (partner, mp))
    signal(barrier, (dp, flip(mp, 1)))
    signal(barrier, (dp, flip(mp, 2)))

    @pl.when(layer > 0)
    def _():
        signal(barrier, (dp - 2, mp))

    @pl.when(layer < layers - 1)
    def _():
        signal(barrier, (dp + 2, mp))

    def local(index, source, target):
        copy = pltpu.make_async_copy(source, target, local_sem.at[index])
        copy.start()
        return copy

    weight_copy = local(1, weight_hbm.at[core], wbuf.at[0])
    hidden_copy = local(0, hidden_hbm, hidden)
    cos_copy = local(3, cos_hbm, cos)
    sin_copy = local(4, sin_hbm, sin)
    split_copy = local(6, split_hbm, split)
    out_weight_copy = local(2, out_weight_hbm.at[pl.ds(pl.multiple_of(core * 2 * head_size, 128), 2 * head_size), :], obuf.at[0])
    dense_copy = local(5, dense_hbm, dense)

    def head_of(item):
        return parity if item < KS else 1 - parity

    def view(relation, item):
        head, kind = head_of(item), item % 4
        if kind == OF:
            return obuf.at[relation, pl.ds(pl.multiple_of(head * head_size, head_size), head_size), :]
        start = head * head_rows + (head_size, 2 * head_size, 0)[kind]
        return wbuf.at[relation, pl.ds(pl.multiple_of(start, head_size), head_size), :]

    sent = []

    def send(source_relation, item, relation, landing, where):
        copy = pltpu.make_async_remote_copy(
            src_ref=view(source_relation, item),
            dst_ref=view(source_relation ^ relation if relation != 4 else source_relation, item),
            send_sem=send_sem.at[len(sent)],
            recv_sem=arrive_sem.at[source_relation ^ relation if relation != 4 else source_relation, landing],
            device_id=where,
            device_id_type=MESH,
        )
        copy.start()
        sent.append(copy)

    def to_x(item, source_relation=0):
        send(source_relation, item, 1, item, (dp, flip(mp, 1)))

    def to_y(item, source_relation=0):
        send(source_relation, item, 2, item, (dp, flip(mp, 2)))

    def to_z(item, source_relation):
        send(source_relation, item, 4, item + 4, (above, mp))

    def arrived(relation, *items):
        for item in items:
            landing = view(relation, item)
            pltpu.make_async_copy(landing, landing, arrive_sem.at[relation, item]).wait()

    weight_copy.wait()
    pl.semaphore_wait(barrier, 3 + (layer > 0).astype(jnp.int32) + (layer < layers - 1).astype(jnp.int32))
    for item in (KF, VF, QF):
        to_x(item)
        to_y(item)
    signal(token_sem.at[0], (partner, mp))

    def tokens_step(step):
        if step == 0:
            pl.semaphore_wait(token_sem.at[0], 1)
            signal(token_sem.at[1], (dp, flip(mp, 1)))
        elif step == 1:
            pl.semaphore_wait(token_sem.at[1], 1)
            signal(token_sem.at[2], (dp, flip(mp, 2)))
        else:
            hop = step - 3
            if hop < 0:
                pl.semaphore_wait(token_sem.at[2], 1)
            else:

                @pl.when(layer == hop + 1)
                def _():
                    pl.semaphore_wait(token_sem.at[3], 1)

                @pl.when(layer == layers - 2 - hop)
                def _():
                    pl.semaphore_wait(token_sem.at[4], 1)

            if hop + 1 < layers - 1:

                @pl.when(layer == hop + 1)
                def _():
                    signal(token_sem.at[3], (dp + 2, mp))

                @pl.when(layer == layers - 2 - hop)
                def _():
                    signal(token_sem.at[4], (dp - 2, mp))

    eye = lax.broadcasted_iota(jnp.int32, (masks, masks), 0) == lax.broadcasted_iota(
        jnp.int32, (masks, masks), 1
    )
    places = lax.broadcasted_iota(jnp.int32, (masks, seq_span), 1).astype(f32)

    def locate(which):
        length = lengths_ref[sequence_ref[which]].astype(f32)
        codes = codes_ref[pl.ds(which, 1), :].astype(f32)
        quotient = jnp.floor(codes / length)
        spots = codes - quotient * length
        spots = jnp.where(spots < 0.0, spots + length, spots)
        spots = jnp.where(spots >= length, spots - length, spots)
        spots = jnp.sum(jnp.where(eye, spots, 0.0), axis=1, keepdims=True)
        live = lax.broadcasted_iota(jnp.int32, (1, seq_span), 1).astype(f32) < length
        return places == spots, live

    chosen, own_alive = locate(me)
    mate_chosen, mate_alive = locate(mate)
    alive = (own_alive, mate_alive)
    tokens = tokens_ref[pl.ds(sequence_ref[me], 1), :].astype(f32)
    targets = jnp.sum(jnp.where(chosen, tokens, 0.0), axis=1, keepdims=True)
    onehot = jnp.where(chosen, 1.0, 0.0).astype(bf16)
    both = jnp.concatenate([onehot, jnp.where(mate_chosen, 1.0, 0.0).astype(bf16)], axis=0)

    hidden_copy.wait()
    tile = 128

    def norm_copy(step):
        rows = pl.ds(pl.multiple_of(step * tile, tile), tile)
        return pltpu.make_async_remote_copy(
            src_ref=normed.at[0, rows, :],
            dst_ref=normed.at[1, rows, :],
            send_sem=norm_send_sem.at[step],
            recv_sem=norm_sem.at[step],
            device_id=(partner, mp),
            device_id_type=MESH,
        )

    def norm_rows(step, carry):
        rows = pl.ds(pl.multiple_of(step * tile, tile), tile)
        normed[0, rows, :] = (layer_norm(hidden[rows, :].astype(f32)) * gain_ref[...].reshape(1, feature)).astype(bf16)
        return carry

    lax.fori_loop(0, seq_span // tile, norm_rows, 0)
    for step in range(seq_span // tile):
        norm_copy(step).start()
    rows_buf[0] = jnp.dot(onehot, normed[0], preferred_element_type=f32).astype(bf16)
    mixed[:masks, :] = jnp.dot(onehot, hidden[...], preferred_element_type=f32)
    mixed[masks:, :] = jnp.zeros((masks, feature), f32)
    rows_copy = pltpu.make_async_remote_copy(
        src_ref=rows_buf.at[0],
        dst_ref=rows_buf.at[1],
        send_sem=swap_send_sem.at[1],
        recv_sem=swap_sem.at[1],
        device_id=(partner, mp),
        device_id_type=MESH,
    )
    rows_copy.start()
    split_copy.wait()
    table = jnp.dot(both, split[...], preferred_element_type=f32)
    query_cos = table[:, :LANES] + table[:, LANES : 2 * LANES]
    query_sin = table[:, 2 * LANES : 3 * LANES] + table[:, 3 * LANES :]
    lane = lax.broadcasted_iota(jnp.int32, (1, LANES), 1)
    first = lane % head_size < head_size // 2
    low = lane < head_size
    transposed = (((1,), (1,)), ((), ()))

    def rotate(inputs, cosine, sine):
        turned = jnp.where(
            first,
            pltpu.roll(inputs, LANES - head_size // 2, 1),
            pltpu.roll(inputs, head_size // 2, 1),
        )
        return inputs * cosine + turned * sine

    span = seq_span // 2

    def stack(refs):
        return jnp.concatenate([ref[...] for ref in refs], axis=0)

    def weights_of(unit):
        keys = []
        for relation, item in unit:
            start = head_of(item) * head_rows + head_size
            keys.append(wbuf.at[relation, pl.ds(pl.multiple_of(start, head_size), 2 * head_size), :])
        return keys

    def project(unit, buffer, low_slot, high_slot):
        keys = stack(weights_of(unit))

        def step_of(step, carry):
            slot = step // 2
            rows = pl.ds(pl.multiple_of((step % 2) * span, 16), span)
            made = lax.dot_general(normed[slot, rows, :], keys, transposed, preferred_element_type=f32)
            for head in range(2):
                block = made[:, head * LANES : (head + 1) * LANES]
                block = jnp.where(low, rotate(block, cos[rows, :], sin[rows, :]), block)
                pbuf[buffer, slot, rows, head * LANES : (head + 1) * LANES] = block.astype(bf16)
            return carry

        lax.fori_loop(2 * low_slot, 2 * high_slot, step_of, 0)

    def queries(unit, low_slot, high_slot):
        weights = stack([view(relation, item - item % 4 + QF) for relation, item in unit])
        rows = slice(low_slot * masks, high_slot * masks)
        source = rows_buf[low_slot:high_slot].reshape((high_slot - low_slot) * masks, feature)
        made = lax.dot_general(source, weights, transposed, preferred_element_type=f32)
        return rotate(made * head_size ** (-0.5), query_cos[rows], query_sin[rows])

    def attend(which, buffer, slot, query):
        empty = jnp.zeros((masks, LANES), bf16)
        near = jnp.where(low, query, 0.0).astype(bf16)
        far = jnp.where(low, pltpu.roll(query, head_size, 1), 0.0).astype(bf16)
        pair = jnp.concatenate(
            [jnp.concatenate([near, empty], axis=1), jnp.concatenate([empty, far], axis=1)], axis=0
        )
        block = pbuf[buffer, slot]
        logits = lax.dot_general(pair, block, transposed, preferred_element_type=f32)
        logits = jnp.where(alive[slot], logits, -1e30)
        weight = jnp.exp(logits - jnp.max(logits, axis=-1, keepdims=True))
        probs = (weight / jnp.sum(weight, axis=-1, keepdims=True)).astype(bf16)
        vectors = jnp.dot(probs, block, preferred_element_type=f32)
        total = jnp.where(low, pltpu.roll(vectors[:masks, :LANES], head_size, 1), vectors[masks:, LANES:])
        context[slot * masks : (slot + 1) * masks, which * LANES : (which + 1) * LANES] = total.astype(bf16)

    def attend_both(which, unit, buffer):
        query = queries(unit, 0, 2)
        for slot in range(2):
            attend(which, buffer, slot, query[slot * masks : (slot + 1) * masks])

    def mix(units):
        out_weights = stack([view(relation, item - item % 4 + OF) for unit in units.values() for relation, item in unit])
        lo, hi = min(units), max(units) + 1
        mixed[...] += jnp.dot(context[:, lo * LANES : hi * LANES], out_weights, preferred_element_type=f32)

    own = ((0, KF), (0, KS))
    firsts = ((1, KF), (2, KF))
    seconds = ((1, KS), (2, KS))
    across = ((3, KF), (3, KS))

    cos_copy.wait()
    sin_copy.wait()
    project(own, 0, 0, 1)
    attend(0, 0, 0, queries(own, 0, 1))
    arrived(1, KF)
    to_z(KF, 1)
    arrived(2, KF)
    to_z(KF, 2)
    to_x(KF, 2)
    tokens_step(0)
    for step in range(seq_span // tile):
        norm_copy(step).wait_recv()
    rows_copy.wait_recv()
    project(own, 0, 1, 2)
    arrived(1, VF)
    to_z(VF, 1)
    arrived(2, VF)
    to_z(VF, 2)
    to_x(VF, 2)
    to_x(QS)
    out_weight_copy.wait()
    to_x(OF)
    attend(0, 0, 1, queries(own, 1, 2))
    tokens_step(1)
    mix({0: own})
    project(firsts, 1, 0, 2)
    arrived(1, QF)
    to_y(QF, 1)
    to_y(QS)
    arrived(2, QF)
    tokens_step(2)
    attend_both(1, firsts, 1)
    arrived(1, KS)
    to_y(KS, 1)
    arrived(3, KF)
    arrived(2, KS)
    tokens_step(3)
    arrived(1, VS)
    arrived(2, VS)
    project(seconds, 0, 0, 2)
    arrived(3, VF)
    to_z(VF, 3)
    arrived(1, QS)
    to_y(QS, 1)
    to_y(OF)
    arrived(2, QS)
    tokens_step(4)
    attend_both(2, seconds, 0)
    arrived(1, OF)
    to_z(OF, 1)
    arrived(3, QF)
    arrived(3, VS)
    tokens_step(5)
    arrived(3, KS)
    project(across, 1, 0, 2)
    arrived(2, OF)
    to_z(OF, 2)
    to_x(OF, 2)
    arrived(3, QS)
    attend_both(3, across, 1)
    arrived(3, OF)
    to_z(OF, 3)
    for relation in (1, 2, 3):
        arrived(relation, OS)
    mix({1: firsts, 2: seconds, 3: across})
    inbox_copy = pltpu.make_async_remote_copy(
        src_ref=mixed.at[pl.ds(masks, masks), :],
        dst_ref=inbox,
        send_sem=swap_send_sem.at[0],
        recv_sem=swap_sem.at[0],
        device_id=(partner, mp),
        device_id_type=MESH,
    )
    inbox_copy.start()
    dense_copy.wait()
    for step in range(seq_span // tile):
        norm_copy(step).wait_send()
    rows_copy.wait_send()
    for copy in sent:
        copy.wait_send()
    inbox_copy.wait_recv()
    residual = mixed[:masks, :] + inbox[...]
    normed_final = (layer_norm(residual) * final_gain_ref[...].reshape(1, feature)).astype(bf16)
    dense_out = jnp.dot(normed_final, dense[...], preferred_element_type=f32)
    headed = layer_norm(0.5 * dense_out * (1.0 + lax.erf(dense_out * 0.5**0.5))).astype(bf16)
    logits = lax.dot_general(headed, decoder_ref[...], transposed, preferred_element_type=f32) + bias_ref[...]
    largest = jnp.max(logits, axis=-1, keepdims=True)
    scale = jnp.log(jnp.sum(jnp.exp(logits - largest), axis=-1, keepdims=True)) + largest
    vocabulary = lax.broadcasted_iota(jnp.int32, logits.shape, 1).astype(f32)
    picked = jnp.sum(jnp.where(vocabulary == targets, logits - scale, 0.0), axis=1, keepdims=True)
    row = jnp.sum(jnp.where(eye, picked, 0.0), axis=0, keepdims=True)
    padded = jnp.pad(row, ((0, 0), (0, LANES - masks)))
    scores[me] = jnp.broadcast_to(padded, scores.shape[1:])

    def score_copy(step):
        other = (me + step) % devices
        return pltpu.make_async_remote_copy(
            src_ref=scores.at[me, pl.ds(0, 1), :],
            dst_ref=scores.at[me, pl.ds(0, 1), :],
            send_sem=score_send_sem.at[step],
            recv_sem=score_sem.at[me],
            device_id=(other // n_mp, other % n_mp),
            device_id_type=MESH,
        )

    def send_scores(step, carry):
        score_copy(step).start()
        return carry

    lax.fori_loop(1, devices, send_scores, 0)
    inbox_copy.wait_send()

    def wait_scores(step, carry):
        source = (me + step) % devices
        landing = scores.at[source, pl.ds(0, 1), :]
        pltpu.make_async_copy(landing, landing, score_sem.at[source]).wait()
        return carry

    lax.fori_loop(1, devices, wait_scores, 0)

    def wait_sends(step, carry):
        score_copy(step).wait_send()
        return carry

    lax.fori_loop(1, devices, wait_sends, 0)
    group = out_ref.shape[0]
    wanted = dp * group + lax.broadcasted_iota(jnp.int32, (group, owner_ref.shape[1]), 0)
    select = jnp.where(owner_ref[...] == wanted, 1.0, 0.0)
    out_ref[...] = jnp.dot(select, scores[:, 0, :], preferred_element_type=f32, precision=lax.Precision.HIGHEST)


def split_call(shape, inputs, weight, out_weight, hidden, dense_weight, cosine, sine, group, head_size):
    n_dp, n_mp = shape
    devices = n_dp * n_mp
    seq_span, feature = hidden.shape
    width = weight.shape[1]
    masks = inputs[2].shape[1]
    high = [t.astype(jnp.bfloat16).astype(np.float32) for t in (cosine, sine)]
    parts = [high[0], cosine - high[0], high[1], sine - high[1]]
    split = np.concatenate(parts, axis=1).astype(jnp.bfloat16)
    dma = pltpu.SemaphoreType.DMA
    vmem = pl.BlockSpec(memory_space=pltpu.VMEM)
    smem = pl.BlockSpec(memory_space=pltpu.SMEM)
    anywhere = pl.BlockSpec(memory_space=pl.ANY)
    tiles = seq_span // 128
    return pl.pallas_call(
        functools.partial(split_kernel, (n_dp, n_mp, head_size)),
        name="score_split",
        out_shape=jax.ShapeDtypeStruct((group, LANES), f32),
        in_specs=[smem] * 2 + [vmem] * 7 + [anywhere] * 7,
        out_specs=vmem,
        scratch_shapes=[
            pltpu.VMEM((seq_span, feature), bf16),
            pltpu.VMEM((2, seq_span, feature), bf16),
            pltpu.VMEM((2, masks, feature), bf16),
            pltpu.VMEM((n_mp, width, feature), bf16),
            pltpu.VMEM((n_mp, 2 * head_size, feature), bf16),
            pltpu.VMEM((feature, feature), bf16),
            pltpu.VMEM((seq_span, LANES), f32),
            pltpu.VMEM((seq_span, LANES), f32),
            pltpu.VMEM((seq_span, 4 * LANES), bf16),
            pltpu.VMEM((2, 2, seq_span, 2 * LANES), bf16),
            pltpu.VMEM((2 * masks, 4 * LANES), bf16),
            pltpu.VMEM((2 * masks, feature), f32),
            pltpu.VMEM((masks, feature), f32),
            pltpu.VMEM((devices, 8, LANES), f32),
            dma((7,)),
            dma((32,)),
            dma((n_mp, 8)),
            dma((tiles,)),
            dma((tiles,)),
            dma((2,)),
            dma((2,)),
            dma((devices,)),
            dma((devices,)),
            pltpu.SemaphoreType.REGULAR((5,)),
        ],
        compiler_params=pltpu.CompilerParams(collective_id=1, has_side_effects=True),
    )(
        *inputs,
        hidden,
        weight,
        out_weight,
        dense_weight,
        jnp.asarray(cosine),
        jnp.asarray(sine),
        jnp.asarray(split),
    )


def on_device(
    shape,
    hidden_states,
    ln_attn_gain,
    w_qkv,
    output_weight,
    ln_final_gain,
    dense_weight,
    decoder_weight,
    decoder_bias,
    seq_tokens,
    seq_lengths,
    copy_sequence,
    mask_code,
    copy_owner,
):
    n_dp, n_mp = shape
    devices = n_dp * n_mp
    lane_copies, seq_span, feature = hidden_states.shape
    head_size, heads, _ = output_weight.shape
    copies, masks = mask_code.shape
    assert lane_copies == 1 and copies == devices and n_dp % 2 == 0
    assert 2 * head_size == LANES and masks <= LANES
    in_chunk = 2 if heads % 2 == 0 else 1
    chunks = heads // in_chunk
    width = in_chunk * 3 * head_size
    weight = jnp.transpose(w_qkv.reshape(feature, chunks, width), (1, 2, 0))
    out_weight = jnp.swapaxes(output_weight, 0, 1).reshape(heads * head_size, feature)
    cosine, sine = rotary_tables(seq_span, head_size)
    group = copies // n_dp
    items = 2 * chunks + 2
    dma = pltpu.SemaphoreType.DMA
    vmem = pl.BlockSpec(memory_space=pltpu.VMEM)
    smem = pl.BlockSpec(memory_space=pltpu.SMEM)
    anywhere = pl.BlockSpec(memory_space=pl.ANY)
    own = masks // n_mp
    inputs = (
        copy_sequence,
        seq_lengths,
        mask_code,
        seq_tokens,
        copy_owner.reshape(1, -1),
        ln_attn_gain,
        ln_final_gain,
        decoder_weight.T,
        decoder_bias.reshape(1, -1),
    )
    if n_mp == 4 and n_dp == 8 and heads == 4 and seq_span % 128 == 0:
        hidden = hidden_states.reshape(seq_span, feature)
        rows = split_call(shape, inputs, weight, out_weight, hidden, dense_weight, cosine, sine, group, head_size)
        return lax.dynamic_slice_in_dim(rows, lax.axis_index("mp") * own, own, 1)
    rows = pl.pallas_call(
        functools.partial(kernel, (n_dp, n_mp, head_size, in_chunk, chunks)),
        name="score_copies",
        out_shape=jax.ShapeDtypeStruct((group, LANES), f32),
        in_specs=[smem] * 2 + [vmem] * 7 + [anywhere] * 6,
        out_specs=vmem,
        scratch_shapes=[
            pltpu.VMEM((seq_span, feature), bf16),
            pltpu.VMEM((seq_span, feature), bf16),
            pltpu.VMEM((n_mp, chunks, width, feature), bf16),
            pltpu.VMEM((n_mp, heads * head_size, feature), bf16),
            pltpu.VMEM((feature, feature), bf16),
            pltpu.VMEM((seq_span, LANES), f32),
            pltpu.VMEM((seq_span, LANES), f32),
            pltpu.VMEM((seq_span, in_chunk * LANES), bf16),
            pltpu.VMEM((n_mp, chunks, masks, in_chunk * head_size), bf16),
            pltpu.VMEM((masks, feature), f32),
            pltpu.VMEM((devices, 8, LANES), f32),
            dma((6,)),
            dma((n_mp, items)),
            dma((items,)),
            dma((n_mp, chunks)),
            dma((n_mp, items)),
            dma((n_mp, items)),
            dma((n_mp, items)),
            dma((devices,)),
            dma((devices,)),
        ],
        compiler_params=pltpu.CompilerParams(collective_id=0, has_side_effects=True),
    )(
        copy_sequence,
        seq_lengths,
        mask_code,
        seq_tokens,
        copy_owner.reshape(1, -1),
        ln_attn_gain,
        ln_final_gain,
        decoder_weight.T,
        decoder_bias.reshape(1, -1),
        hidden_states.reshape(seq_span, feature),
        weight,
        out_weight,
        dense_weight,
        jnp.asarray(cosine),
        jnp.asarray(sine),
    )
    return lax.dynamic_slice_in_dim(rows, lax.axis_index("mp") * own, own, 1)


def solution(mesh):
    placed = (
        P(("dp", "mp"), None, None),
        P(),
        P(None, "mp", None),
        P(None, "mp", None),
        P(),
        P(),
        P(),
        P(),
        P(),
        P(),
        P(),
        P(),
        P(),
    )
    shape = (mesh.shape["dp"], mesh.shape["mp"])
    return jax.shard_map(
        functools.partial(on_device, shape),
        mesh=mesh,
        in_specs=placed,
        out_specs=P("dp", "mp"),
        check_vma=False,
    )
```

```python
import functools

import jax
import jax.numpy as jnp
import numpy as np
from jax import lax
from jax.experimental import pallas as pl
from jax.experimental.pallas import tpu as pltpu
from jax.sharding import PartitionSpec as P

epsilon = 1e-05
MESH = pl.DeviceIdType.MESH
f32 = jnp.float32
bf16 = jnp.bfloat16
LANES = 128


def layer_norm(inputs):
    average = jnp.mean(inputs, axis=-1, keepdims=True)
    centred = inputs - average
    variance = jnp.mean(centred * centred, axis=-1, keepdims=True)
    return centred * lax.rsqrt(variance + epsilon)


def rotary_tables(seq_span, head_size):
    half = head_size // 2
    frequency = (1.0 / 10000.0 ** (np.arange(half, dtype=np.float32) * (2.0 / head_size))).astype(
        np.float32
    )
    angles = np.arange(seq_span, dtype=np.float32)[:, None] * frequency[None, :]
    cosine, sine = np.cos(angles), np.sin(angles)
    times = LANES // head_size
    return (
        np.tile(np.concatenate([cosine, cosine], axis=1), (1, times)).astype(np.float32),
        np.tile(np.concatenate([-sine, sine], axis=1), (1, times)).astype(np.float32),
    )


def flip(index, mask):
    bit = 1
    out = index
    while bit <= mask:
        if mask & bit:
            out = out + bit * (1 - 2 * ((index // bit) % 2))
        bit *= 2
    return out


def kernel(
    sizes,
    sequence_ref,
    lengths_ref,
    codes_ref,
    tokens_ref,
    owner_ref,
    gain_ref,
    final_gain_ref,
    decoder_ref,
    bias_ref,
    hidden_hbm,
    weight_hbm,
    out_weight_hbm,
    dense_hbm,
    cos_hbm,
    sin_hbm,
    out_ref,
    hidden,
    normed,
    wbuf,
    obuf,
    dense,
    cos,
    sin,
    pbuf,
    context,
    mixed,
    scores,
    local_sem,
    direct_sem,
    relay_sem,
    exchange_sem,
    share_sem,
    arrive_sem,
    shared_sem,
    score_send_sem,
    score_sem,
):
    n_dp, n_mp, head_size, heads_in_chunk, chunks = sizes
    devices = n_dp * n_mp
    dp = lax.axis_index("dp")
    mp = lax.axis_index("mp")
    core = dp % 2
    partner = dp + 1 - 2 * core
    me = dp * n_mp + mp
    seq_span, feature = hidden.shape
    masks = codes_ref.shape[1]
    chunk_heads = heads_in_chunk * head_size
    out_rows = obuf.shape[1]
    piece_rows = out_rows // 4

    def local(index, source, target):
        copy = pltpu.make_async_copy(source, target, local_sem.at[index])
        copy.start()
        return copy

    weight_copy = local(1, weight_hbm, wbuf.at[0])
    hidden_copy = local(0, hidden_hbm, hidden)

    barrier = pltpu.get_barrier_semaphore()

    def greet(step, carry):
        other = (me + step) % devices
        pl.semaphore_signal(
            barrier, inc=1, device_id=(other // n_mp, other % n_mp), device_id_type=MESH
        )
        return carry

    lax.fori_loop(1, devices, greet, 0)

    parity = (dp // 2) % 2
    above = dp + 2 - 4 * parity
    part_rows = wbuf.shape[2] // 4

    def part(chunk, odd):
        return 2 * chunk + odd

    def place(relation, item, half):
        if item < 2 * chunks:
            chunk, odd = divmod(item, 2)
            which = 1 - parity if odd else parity
            start = (2 * half + which) * part_rows
            return wbuf.at[relation, chunk, pl.ds(pl.multiple_of(start, 16), part_rows), :]
        start = (2 * half + item - 2 * chunks) * piece_rows
        return obuf.at[relation, pl.ds(pl.multiple_of(start, 16), piece_rows), :]

    def view(relation, item):
        return place(relation, item, core)

    def partner_view(relation, item):
        return place(relation, item, 1 - core)

    sent = []

    def to_group(target, source_relation, relation, item, semaphore):
        copy = pltpu.make_async_remote_copy(
            src_ref=view(source_relation, item),
            dst_ref=view(relation, item),
            send_sem=semaphore,
            recv_sem=arrive_sem.at[relation, item],
            device_id=(dp, flip(mp, target)),
            device_id_type=MESH,
        )
        copy.start()
        sent.append(copy)

    def direct(target, item):
        to_group(target, 0, target, item, direct_sem.at[target, item])

    def relay(target, source_relation, item):
        to_group(target, source_relation, source_relation ^ target, item, relay_sem.at[item])

    def exchange(relation, chunk):
        copy = pltpu.make_async_remote_copy(
            src_ref=view(relation, part(chunk, 0)),
            dst_ref=view(relation, part(chunk, 0)),
            send_sem=exchange_sem.at[relation, chunk],
            recv_sem=arrive_sem.at[relation, part(chunk, 1)],
            device_id=(above, mp),
            device_id_type=MESH,
        )
        copy.start()
        sent.append(copy)

    def arrived(relation, item):
        landing = view(relation, item)
        pltpu.make_async_copy(landing, landing, arrive_sem.at[relation, item]).wait()

    def share(relation, item):
        copy = pltpu.make_async_remote_copy(
            src_ref=view(relation, item),
            dst_ref=view(relation, item),
            send_sem=share_sem.at[relation, item],
            recv_sem=shared_sem.at[relation, item],
            device_id=(partner, mp),
            device_id_type=MESH,
        )
        copy.start()
        sent.append(copy)

    def was_shared(relation, item):
        landing = partner_view(relation, item)
        pltpu.make_async_copy(landing, landing, shared_sem.at[relation, item]).wait()

    sequence = sequence_ref[me]
    length = lengths_ref[sequence].astype(f32)
    codes = codes_ref[pl.ds(me, 1), :].astype(f32)
    quotient = jnp.floor(codes / length)
    row_positions = codes - quotient * length
    row_positions = jnp.where(row_positions < 0.0, row_positions + length, row_positions)
    row_positions = jnp.where(row_positions >= length, row_positions - length, row_positions)
    eye = lax.broadcasted_iota(jnp.int32, (masks, masks), 0) == lax.broadcasted_iota(
        jnp.int32, (masks, masks), 1
    )
    positions = jnp.sum(jnp.where(eye, row_positions, 0.0), axis=1, keepdims=True)
    places = lax.broadcasted_iota(jnp.int32, (masks, seq_span), 1).astype(f32)
    chosen = places == positions
    onehot = jnp.where(chosen, 1.0, 0.0)
    onehot_bf = onehot.astype(bf16)
    tokens = tokens_ref[pl.ds(sequence, 1), :].astype(f32)
    targets = jnp.sum(jnp.where(chosen, tokens, 0.0), axis=1, keepdims=True)
    alive = lax.broadcasted_iota(jnp.int32, (1, seq_span), 1).astype(f32) < length

    weight_copy.wait()
    pl.semaphore_wait(barrier, devices - 1)
    items = 2 * chunks + 2
    routed = n_mp == 4 and chunks == 2 and n_dp % 4 == 0
    if routed:
        direct(1, part(1, 0))
        direct(2, part(0, 0))
        direct(1, part(0, 0))
        direct(2, part(1, 0))
    cos_copy = local(3, cos_hbm, cos)
    sin_copy = local(4, sin_hbm, sin)
    out_weight_copy = local(2, out_weight_hbm, obuf.at[0])
    dense_copy = local(5, dense_hbm, dense)
    if not routed:
        out_weight_copy.wait()
        for item in range(items):
            for target in range(1, n_mp):
                direct(target, item)

    hidden_copy.wait()
    tile = 128 if seq_span % 128 == 0 else 8

    def norm_rows(step, carry):
        rows = pl.ds(pl.multiple_of(step * tile, tile), tile)
        normed[rows, :] = (layer_norm(hidden[rows, :].astype(f32)) * gain_ref[...].reshape(1, feature)).astype(bf16)
        return carry

    lax.fori_loop(0, seq_span // tile, norm_rows, 0)
    masked_rows = jnp.dot(onehot_bf, normed[...], preferred_element_type=f32).astype(bf16)
    own_rows = jnp.dot(onehot_bf, hidden[...], preferred_element_type=f32)
    mixed[...] = own_rows
    cos_copy.wait()
    sin_copy.wait()
    exact = dict(preferred_element_type=f32, precision=lax.Precision.HIGHEST)
    query_cos = jnp.dot(onehot, cos[...], **exact)
    query_sin = jnp.dot(onehot, sin[...], **exact)
    lane = lax.broadcasted_iota(jnp.int32, (1, LANES), 1)
    first = lane % head_size < head_size // 2

    def rotate(inputs, cosine, sine):
        turned = jnp.where(
            first,
            pltpu.roll(inputs, LANES - head_size // 2, 1),
            pltpu.roll(inputs, head_size // 2, 1),
        )
        return inputs * cosine + turned * sine

    transposed = (((1,), (1,)), ((), ()))
    low = lane < head_size
    span = seq_span // 2 if seq_span % 32 == 0 else seq_span
    head_rows = 3 * head_size

    def attend(relation, chunk):
        weights = wbuf.at[relation, chunk]
        pairs = [
            weights[head * head_rows + head_size : (head + 1) * head_rows, :]
            for head in range(heads_in_chunk)
        ]
        pair_weights = pairs[0] if heads_in_chunk == 1 else jnp.concatenate(pairs, axis=0)

        def project(step, carry):
            rows = pl.ds(pl.multiple_of(step * span, 16), span)
            made = lax.dot_general(
                normed[rows, :], pair_weights, transposed, preferred_element_type=f32
            )
            for head in range(heads_in_chunk):
                block = made[:, head * LANES : (head + 1) * LANES]
                block = jnp.where(low, rotate(block, cos[rows, :], sin[rows, :]), block)
                pbuf[rows, head * LANES : (head + 1) * LANES] = block.astype(bf16)
            return carry

        lax.fori_loop(0, seq_span // span, project, 0)
        if heads_in_chunk == 1:
            query_weights = weights[: 2 * head_size, :]
        else:
            query_weights = jnp.concatenate(
                [weights[:head_size, :], weights[head_rows : head_rows + head_size, :]], axis=0
            )
        made = lax.dot_general(masked_rows, query_weights, transposed, preferred_element_type=f32)
        turned = rotate(made * head_size ** (-0.5), query_cos, query_sin)
        vectors = []
        for head in range(heads_in_chunk):
            query = turned if head == 0 else pltpu.roll(turned, head_size, 1)
            query = jnp.where(low, query, 0.0).astype(bf16)
            block = pbuf[:, head * LANES : (head + 1) * LANES]
            logits = lax.dot_general(query, block, transposed, preferred_element_type=f32)
            logits = jnp.where(alive, logits, -1e30)
            weight = jnp.exp(logits - jnp.max(logits, axis=-1, keepdims=True))
            probs = (weight / jnp.sum(weight, axis=-1, keepdims=True)).astype(bf16)
            vectors.append(jnp.dot(probs, block, preferred_element_type=f32))
        total = pltpu.roll(vectors[0], head_size, 1)
        if heads_in_chunk > 1:
            total = jnp.where(low, total, vectors[1])
        context[relation, chunk] = total[:, :chunk_heads].astype(bf16)

    def mix(relation):
        for chunk in range(chunks):
            rows = slice(chunk * chunk_heads, (chunk + 1) * chunk_heads)
            mixed[...] += jnp.dot(
                context[relation, chunk], obuf[relation, rows, :], preferred_element_type=f32
            )

    def fetch(*pairs):
        for pair in pairs:
            arrived(*pair)
            share(*pair)

    def attend_shared(relation, chunk):
        was_shared(relation, part(chunk, 0))
        was_shared(relation, part(chunk, 1))
        attend(relation, chunk)

    attend(0, 0)
    if routed:
        first_piece, second_piece = 2 * chunks, 2 * chunks + 1
        arrived(1, part(1, 0))
        relay(2, 1, part(1, 0))
        exchange(1, 1)
        share(1, part(1, 0))
        arrived(2, part(0, 0))
        relay(1, 2, part(0, 0))
        exchange(2, 0)
        share(2, part(0, 0))
        direct(1, part(0, 1))
        direct(2, part(1, 1))
        out_weight_copy.wait()
        direct(1, first_piece)
        direct(2, second_piece)
        direct(1, second_piece)
        direct(2, first_piece)
    for chunk in range(1, chunks):
        attend(0, chunk)
    mix(0)
    if routed:
        fetch((1, part(0, 0)), (2, part(1, 0)), (1, part(1, 1)))
        arrived(3, part(0, 0))
        exchange(3, 0)
        share(3, part(0, 0))
        arrived(3, part(1, 0))
        exchange(3, 1)
        share(3, part(1, 0))
        fetch((2, part(0, 1)))
        attend_shared(1, 1)
        attend_shared(2, 0)
        fetch((1, part(0, 1)), (2, part(1, 1)), (3, part(0, 1)))
        attend_shared(1, 0)
        arrived(1, first_piece)
        relay(2, 1, first_piece)
        share(1, first_piece)
        arrived(2, second_piece)
        relay(1, 2, second_piece)
        share(2, second_piece)
        attend_shared(2, 1)
        fetch((3, part(1, 1)))
        attend_shared(3, 0)
        fetch((1, second_piece), (2, first_piece))
        attend_shared(3, 1)
        for relation in (1, 2):
            was_shared(relation, first_piece)
            was_shared(relation, second_piece)
            mix(relation)
        fetch((3, first_piece), (3, second_piece))
        was_shared(3, first_piece)
        was_shared(3, second_piece)
        mix(3)
    else:
        for relation in range(1, n_mp):
            fetch(*[(relation, item) for item in range(items)])
        for relation in range(1, n_mp):
            for item in range(items):
                was_shared(relation, item)
            for chunk in range(chunks):
                attend(relation, chunk)
            mix(relation)

    normed_final = (layer_norm(mixed[...]) * final_gain_ref[...].reshape(1, feature)).astype(bf16)
    dense_copy.wait()
    dense_out = jnp.dot(normed_final, dense[...], preferred_element_type=f32)
    headed = layer_norm(0.5 * dense_out * (1.0 + lax.erf(dense_out * 0.5**0.5))).astype(bf16)
    logits = lax.dot_general(headed, decoder_ref[...], transposed, preferred_element_type=f32) + bias_ref[...]
    largest = jnp.max(logits, axis=-1, keepdims=True)
    scale = jnp.log(jnp.sum(jnp.exp(logits - largest), axis=-1, keepdims=True)) + largest
    vocabulary = lax.broadcasted_iota(jnp.int32, logits.shape, 1).astype(f32)
    picked = jnp.sum(jnp.where(vocabulary == targets, logits - scale, 0.0), axis=1, keepdims=True)
    row = jnp.sum(jnp.where(eye, picked, 0.0), axis=0, keepdims=True)
    padded = jnp.pad(row, ((0, 0), (0, LANES - masks)))
    scores[me] = jnp.broadcast_to(padded, scores.shape[1:])

    def score_copy(step):
        other = (me + step) % devices
        return pltpu.make_async_remote_copy(
            src_ref=scores.at[me, pl.ds(0, 1), :],
            dst_ref=scores.at[me, pl.ds(0, 1), :],
            send_sem=score_send_sem.at[step],
            recv_sem=score_sem.at[me],
            device_id=(other // n_mp, other % n_mp),
            device_id_type=MESH,
        )

    def send_scores(step, carry):
        score_copy(step).start()
        return carry

    lax.fori_loop(1, devices, send_scores, 0)
    for copy in sent:
        copy.wait_send()

    def wait_scores(step, carry):
        source = (me + step) % devices
        landing = scores.at[source, pl.ds(0, 1), :]
        pltpu.make_async_copy(landing, landing, score_sem.at[source]).wait()
        return carry

    lax.fori_loop(1, devices, wait_scores, 0)

    def wait_sends(step, carry):
        score_copy(step).wait_send()
        return carry

    lax.fori_loop(1, devices, wait_sends, 0)
    group = out_ref.shape[0]
    wanted = dp * group + lax.broadcasted_iota(jnp.int32, (group, owner_ref.shape[1]), 0)
    select = jnp.where(owner_ref[...] == wanted, 1.0, 0.0)
    out_ref[...] = jnp.dot(select, scores[:, 0, :], **exact)


ITEMS = {"K0": 0, "V0": 1, "K1": 2, "V1": 3, "Q0": 4, "Q1": 5, "O0": 6, "O1": 7}
FIRST_ROW = {"Q": 0, "K": 64, "V": 128}
ENDS = [('0V0.1>xy', '0V0.0>xy', '0K0.1>xy', '0O0.0>y', '0O0.1>x'),
 ('0K0.0>xy',
  '0R',
  '2V0.1>e',
  '1K0.1>e',
  '2O0.0>x',
  '0O0.1>y',
  '1V0.1>ey',
  '2K0.0>ex',
  '3V0.1',
  '0O1.0>xy',
  '1V0.0>ey'),
 ('1K0.0>e', '0O0.0>x'),
 ('1K1.1>y', '1O0.1', '1O1.0', '2K0.1>ex', '1K1.0>y'),
 ('1V1.0', '2O0.1>x'),
 ('2V1.0', '2V0.0>e'),
 ('2K1.0', '3K0.0>e', '3K0.1>e'),
 ('2G', '0O1.1>xy', '2V1.1', '1G', '3V0.0'),
 ('3O0.1>e', '3K1.1', '2K1.1', '1V1.1'),
 (),
 ('2O1.0', '3V1.1', '3K1.0'),
 ('3V1.0', '3O0.0>e'),
 ('2O1.1', '1O0.0'),
 ('3G', '1O1.1', '3O1.1'),
 ('3O1.0',)]
MIDS = [('0ox.1>y', '0V1.0>x', '0qx.1>y', '0K1.1>x', '0K1.0>x'),
 ('0V1.0>y',
  '0K1.0>y',
  '0qx.1>x',
  '0qx.0>x',
  '1V1.0>e',
  '2ox.1>m',
  '1K1.1>e',
  '0V1.1>y',
  '0qx.0>y',
  '2qx.1>m',
  '2V1.0>ex',
  '0V1.1>x',
  '0ox.0>x',
  '0ox.0>y'),
 ('9R', '1K1.0>e', '1qx.1>my', '1qx.0>my', '2oy.1', '2O1!1>x', '2K1.0>e', '2V1.1>ex'),
 (),
 ('2qx.0>m', '2ox.0>m', '1V1.1>e', '3V1.0>e', '2K0.0', '1V0.1', '0ox.1>x', '2qy.1', '0K1.1>y'),
 ('3qx.1>m',
  '1qy.1',
  '2V0.1',
  '1qy.0',
  'q1',
  '2qy.0',
  '1V0.0',
  '3qx.0>m',
  '1kx!1>y',
  'q2',
  '1kx!0>y',
  '2K1.1>e',
  '1ox.0>m'),
 ('3V1.1>e',),
 ('1K0.1', '3kx.1>m', '2oy.0', '2O1!0>x', '3O1.1>e', '3qy.0', '3qy.1'),
 ('q3', '3kx.0>m', '2V0.0', '1ox.1>m', '2K0.1', '1K0.0'),
 (),
 ('3O1.0>e', '3K0.0', '3ky.1'),
 ('3K0.1', '3ky.0', '1oy.0'),
 (),
 (),
 ('1oy.1', '3O0.0', '3O0.1')]


def split_kernel(
    sizes,
    sequence_ref,
    lengths_ref,
    codes_ref,
    tokens_ref,
    owner_ref,
    gain_ref,
    final_gain_ref,
    decoder_ref,
    bias_ref,
    hidden_hbm,
    weight_hbm,
    out_weight_hbm,
    dense_hbm,
    cos_hbm,
    sin_hbm,
    split_hbm,
    out_ref,
    hidden,
    normed,
    rows_buf,
    wbuf,
    obuf,
    dense,
    cos,
    sin,
    split,
    pbuf,
    context,
    qbuf,
    gbuf,
    mixed,
    inbox,
    scores,
    local_sem,
    send_sem,
    arrive_sem,
    query_sem,
    norm_send_sem,
    norm_sem,
    swap_send_sem,
    swap_sem,
    score_send_sem,
    score_sem,
    token_sem,
):
    n_dp, n_mp, head_size = sizes
    devices = n_dp * n_mp
    layers = n_dp // 2
    dp = lax.axis_index("dp")
    mp = lax.axis_index("mp")
    core = dp % 2
    layer = dp // 2
    partner = dp + 1 - 2 * core
    me = dp * n_mp + mp
    mate = partner * n_mp + mp
    parity = layer % 2
    pair = dp + 2 - 4 * parity
    twin = dp - 2 + 4 * parity
    middle = jnp.logical_and(layer > 0, layer < layers - 1)
    side = 1 - parity
    seq_span, feature = hidden.shape
    masks = codes_ref.shape[1]
    head_rows = 3 * head_size
    half_rows = head_size // 2
    where = {"x": (dp, flip(mp, 1)), "y": (dp, flip(mp, 2)), "e": (pair, mp), "m": (twin, mp), "d": (partner, mp)}

    barrier = pltpu.get_barrier_semaphore()

    def signal(semaphore, target):
        pl.semaphore_signal(semaphore, inc=1, device_id=target, device_id_type=MESH)

    for link in "dxye":
        signal(barrier, where[link])

    @pl.when(middle)
    def _():
        signal(barrier, where["m"])

    def local(index, source, target):
        copy = pltpu.make_async_copy(source, target, local_sem.at[index])
        copy.start()
        return copy

    weight_copy = local(1, weight_hbm.at[core], wbuf.at[0])
    out_start = pl.multiple_of(core * 2 * head_size, 2 * head_size)
    out_weight_copy = local(2, out_weight_hbm.at[pl.ds(out_start, 2 * head_size), :], obuf.at[0])
    hidden_copy = local(0, hidden_hbm, hidden)
    cos_copy = local(3, cos_hbm, cos)
    sin_copy = local(4, sin_hbm, sin)
    split_copy = local(6, split_hbm, split)
    dense_copy = local(5, dense_hbm, dense)

    def number(item):
        if item in ITEMS:
            return ITEMS[item]
        return {"qx": 4 + side, "qy": 5 - side, "ox": 6 + side, "oy": 7 - side, "kx": 2 - side, "ky": 1 + side}[item]

    def view(relation, item, half):
        if item in ITEMS:
            kind, head = item[0], int(item[1])
            start = head * head_size if kind == "O" else head * head_rows + FIRST_ROW[kind]
        elif item[0] == "k":
            kind = "K"
            start = 256 - 128 * side if item == "kx" else 128 + 128 * side
        else:
            kind = item[0].upper()
            start = (side if item[1] == "x" else 1 - side) * (head_rows if kind == "Q" else head_size)
        rows = pl.ds(pl.multiple_of(start + half * half_rows, half_rows), half_rows)
        return (obuf if kind == "O" else wbuf).at[relation, rows, :]

    flips = {"x": 1, "y": 2, "e": 0, "m": 0}

    def piece_copy(relation, item, half, link, index):
        target = relation ^ flips[link]
        return pltpu.make_async_remote_copy(
            src_ref=view(relation, item, half),
            dst_ref=view(target, item, half),
            send_sem=send_sem.at[index],
            recv_sem=arrive_sem.at[target, 2 * number(item) + half],
            device_id=where[link],
            device_id_type=MESH,
        )

    def rows_copy(source, target, link, index):
        return pltpu.make_async_remote_copy(
            src_ref=rows_buf.at[source],
            dst_ref=rows_buf.at[target],
            send_sem=swap_send_sem.at[index],
            recv_sem=swap_sem.at[index],
            device_id=where[link],
            device_id_type=MESH,
        )

    def query_copy(relation):
        return pltpu.make_async_remote_copy(
            src_ref=gbuf.at[relation],
            dst_ref=qbuf.at[relation],
            send_sem=query_sem.at[0, relation],
            recv_sem=query_sem.at[1, relation],
            device_id=where["e"],
            device_id_type=MESH,
        )

    sent = {True: [], False: []}

    def serve(words, in_middle):
        for word in words:
            if word in ("q1", "q2", "q3"):
                project_queries(int(word[1]))
                continue
            name, _, links = word.partition(">")
            relation, item = int(name[0]), name[1:3]
            if item == "R":
                if in_middle:
                    rows_copy(0, 2, "e", 1).wait_recv()
                    rows_copy(2, 3, "d", 2).start()
                else:
                    rows_copy(0, 2, "e", 1).start()
                continue
            if item == "G":
                query_copy(relation).wait_recv()
                continue
            half = int(name[4])
            if relation and name[3] != "!":
                landing = view(relation, item, half)
                pltpu.make_async_copy(
                    landing, landing, arrive_sem.at[relation, 2 * number(item) + half]
                ).wait()
            for link in links:
                index = len(sent[in_middle])
                sent[in_middle].append((relation, item, half, link, index))
                piece_copy(relation, item, half, link, index).start()

    def service(index):
        if MIDS[index]:

            @pl.when(middle)
            def _():
                serve(MIDS[index], True)

        if ENDS[index]:

            @pl.when(jnp.logical_not(middle))
            def _():
                serve(ENDS[index], False)

    weight_copy.wait()
    out_weight_copy.wait()
    pl.semaphore_wait(barrier, 4 + middle.astype(jnp.int32))
    service(0)
    signal(token_sem.at[0], (partner, mp))

    def tokens_step(step):
        if step == 0:
            pl.semaphore_wait(token_sem.at[0], 1)
            signal(token_sem.at[1], (dp, flip(mp, 1)))
        elif step == 1:
            pl.semaphore_wait(token_sem.at[1], 1)
            signal(token_sem.at[2], (dp, flip(mp, 2)))
        else:
            hop = step - 3
            if hop < 0:
                pl.semaphore_wait(token_sem.at[2], 1)
            else:

                @pl.when(layer == hop + 1)
                def _():
                    pl.semaphore_wait(token_sem.at[3], 1)

                @pl.when(layer == layers - 2 - hop)
                def _():
                    pl.semaphore_wait(token_sem.at[4], 1)

            if hop + 1 < layers - 1:

                @pl.when(layer == hop + 1)
                def _():
                    signal(token_sem.at[3], (dp + 2, mp))

                @pl.when(layer == layers - 2 - hop)
                def _():
                    signal(token_sem.at[4], (dp - 2, mp))

    eye = lax.broadcasted_iota(jnp.int32, (masks, masks), 0) == lax.broadcasted_iota(
        jnp.int32, (masks, masks), 1
    )
    places = lax.broadcasted_iota(jnp.int32, (masks, seq_span), 1).astype(f32)

    def locate(which):
        length = lengths_ref[sequence_ref[which]].astype(f32)
        codes = codes_ref[pl.ds(which, 1), :].astype(f32)
        quotient = jnp.floor(codes / length)
        spots = codes - quotient * length
        spots = jnp.where(spots < 0.0, spots + length, spots)
        spots = jnp.where(spots >= length, spots - length, spots)
        spots = jnp.sum(jnp.where(eye, spots, 0.0), axis=1, keepdims=True)
        live = lax.broadcasted_iota(jnp.int32, (1, seq_span), 1).astype(f32) < length
        return places == spots, live

    located = [locate(which) for which in (me, mate, pair * n_mp + mp, (pair + 1 - 2 * core) * n_mp + mp)]
    chosen = located[0][0]
    alive = [live for _, live in located]
    tokens = tokens_ref[pl.ds(sequence_ref[me], 1), :].astype(f32)
    targets = jnp.sum(jnp.where(chosen, tokens, 0.0), axis=1, keepdims=True)
    onehots = [jnp.where(spots, 1.0, 0.0).astype(bf16) for spots, _ in located]
    onehot = onehots[0]

    hidden_copy.wait()
    tile = 128

    def norm_copy(step):
        rows = pl.ds(pl.multiple_of(step * tile, tile), tile)
        return pltpu.make_async_remote_copy(
            src_ref=normed.at[0, rows, :],
            dst_ref=normed.at[1, rows, :],
            send_sem=norm_send_sem.at[step],
            recv_sem=norm_sem.at[step],
            device_id=(partner, mp),
            device_id_type=MESH,
        )

    def norm_rows(step, carry):
        rows = pl.ds(pl.multiple_of(step * tile, tile), tile)
        normed[0, rows, :] = (layer_norm(hidden[rows, :].astype(f32)) * gain_ref[...].reshape(1, feature)).astype(bf16)
        return carry

    lax.fori_loop(0, seq_span // tile, norm_rows, 0)
    rows_buf[0] = jnp.dot(onehot, normed[0], preferred_element_type=f32).astype(bf16)
    for step in range(seq_span // tile):
        norm_copy(step).start()
    mixed[:masks, :] = jnp.dot(onehot, hidden[...], preferred_element_type=f32)
    mixed[masks:, :] = jnp.zeros((masks, feature), f32)
    rows_copy(0, 1, "d", 0).start()
    split_copy.wait()
    table = jnp.dot(jnp.concatenate(onehots, axis=0), split[...], preferred_element_type=f32)
    query_cos = table[:, :LANES] + table[:, LANES : 2 * LANES]
    query_sin = table[:, 2 * LANES : 3 * LANES] + table[:, 3 * LANES :]
    lane = lax.broadcasted_iota(jnp.int32, (1, LANES), 1)
    first = lane % head_size < head_size // 2
    low = lane < head_size
    transposed = (((1,), (1,)), ((), ()))

    def rotate(inputs, cosine, sine):
        turned = jnp.where(
            first,
            pltpu.roll(inputs, LANES - head_size // 2, 1),
            pltpu.roll(inputs, head_size // 2, 1),
        )
        return inputs * cosine + turned * sine

    span = seq_span // 2

    def stack(refs):
        return jnp.concatenate([ref[...] for ref in refs], axis=0)

    def rows_of(start, count):
        return pl.ds(start if isinstance(start, int) else pl.multiple_of(start, head_size), count)

    def project(unit, buffer, slot):
        keys = stack(
            [wbuf.at[relation, rows_of(head * head_rows + head_size, 2 * head_size), :] for relation, head in unit]
        )

        def step_of(step, carry):
            rows = pl.ds(pl.multiple_of(step * span, 16), span)
            made = lax.dot_general(normed[slot, rows, :], keys, transposed, preferred_element_type=f32)
            for head in range(2):
                block = made[:, head * LANES : (head + 1) * LANES]
                block = jnp.where(low, rotate(block, cos[rows, :], sin[rows, :]), block)
                pbuf[buffer, slot, rows, head * LANES : (head + 1) * LANES] = block.astype(bf16)
            return carry

        lax.fori_loop(0, seq_span // span, step_of, 0)

    def queries(relation, low_slot, high_slot):
        weights = stack([wbuf.at[relation, head * head_rows : head * head_rows + head_size, :] for head in range(2)])
        rows = slice(low_slot * masks, high_slot * masks)
        source = rows_buf[low_slot:high_slot].reshape((high_slot - low_slot) * masks, feature)
        made = lax.dot_general(source, weights, transposed, preferred_element_type=f32)
        return rotate(made * head_size ** (-0.5), query_cos[rows], query_sin[rows]).astype(bf16)

    def project_queries(relation):
        if relation == 1:
            rows_copy(2, 3, "d", 2).wait_recv()
        made = queries(relation, 0, 4)
        gbuf[relation] = made[2 * masks :]
        qbuf[relation] = made[: 2 * masks]
        query_copy(relation).start()

    def of_head(query, head):
        query = query.astype(f32)
        if isinstance(head, int):
            return pltpu.roll(query, head_size, 1) if head else query
        return jnp.where(head == 1, pltpu.roll(query, head_size, 1), query)

    def attend(which, buffer, slot, near, far):
        empty = jnp.zeros((masks, LANES), bf16)
        near = jnp.where(low, near, 0.0).astype(bf16)
        far = jnp.where(low, far, 0.0).astype(bf16)
        both = jnp.concatenate(
            [jnp.concatenate([near, empty], axis=1), jnp.concatenate([empty, far], axis=1)], axis=0
        )
        block = pbuf[buffer, slot]
        logits = lax.dot_general(both, block, transposed, preferred_element_type=f32)
        logits = jnp.where(alive[slot], logits, -1e30)
        weight = jnp.exp(logits - jnp.max(logits, axis=-1, keepdims=True))
        probs = (weight / jnp.sum(weight, axis=-1, keepdims=True)).astype(bf16)
        vectors = jnp.dot(probs, block, preferred_element_type=f32)
        total = jnp.where(low, pltpu.roll(vectors[:masks, :LANES], head_size, 1), vectors[masks:, LANES:])
        context[slot * masks : (slot + 1) * masks, which * LANES : (which + 1) * LANES] = total.astype(bf16)

    def attend_both(which, unit, buffer):
        for slot in range(2):
            rows = slice(slot * masks, (slot + 1) * masks)
            near, far = [of_head(qbuf[relation, rows, :], head) for relation, head in unit]
            attend(which, buffer, slot, near, far)

    def mix(low_unit, *units):
        out_weights = stack([obuf.at[relation, rows_of(head * head_size, head_size), :] for unit in units for relation, head in unit])
        lanes = slice(low_unit * LANES, (low_unit + len(units)) * LANES)
        mixed[...] += jnp.dot(context[:, lanes], out_weights, preferred_element_type=f32)

    early = middle.astype(jnp.int32)
    own = ((0, 0), (0, 1))
    firsts = ((1, early), (2, early))
    seconds = ((1, 1 - early), (2, 1 - early))
    across = ((3, 0), (3, 1))

    cos_copy.wait()
    sin_copy.wait()
    service(1)
    project(own, 0, 0)
    service(2)
    query = queries(0, 0, 1)
    attend(0, 0, 0, of_head(query, 0), of_head(query, 1))
    tokens_step(0)
    service(3)
    for step in range(seq_span // tile):
        norm_copy(step).wait_recv()
    rows_copy(0, 1, "d", 0).wait_recv()
    project(own, 0, 1)
    service(4)
    query = queries(0, 1, 2)
    attend(0, 0, 1, of_head(query, 0), of_head(query, 1))
    mix(0, own)
    tokens_step(1)
    service(5)
    project(firsts, 1, 0)
    service(6)
    project(firsts, 1, 1)
    tokens_step(2)
    service(7)
    attend_both(1, firsts, 1)
    tokens_step(3)
    service(8)
    project(seconds, 0, 0)
    service(9)
    project(seconds, 0, 1)
    service(10)
    attend_both(2, seconds, 0)
    tokens_step(4)
    service(11)
    project(across, 1, 0)
    service(12)
    project(across, 1, 1)
    service(13)
    attend_both(3, across, 1)
    tokens_step(5)
    service(14)
    mix(1, firsts, seconds, across)
    inbox_copy = pltpu.make_async_remote_copy(
        src_ref=mixed.at[pl.ds(masks, masks), :],
        dst_ref=inbox,
        send_sem=swap_send_sem.at[3],
        recv_sem=swap_sem.at[3],
        device_id=(partner, mp),
        device_id_type=MESH,
    )
    inbox_copy.start()
    dense_copy.wait()
    for step in range(seq_span // tile):
        norm_copy(step).wait_send()
    rows_copy(0, 1, "d", 0).wait_send()

    @pl.when(middle)
    def _():
        for record in sent[True]:
            piece_copy(*record).wait_send()
        rows_copy(2, 3, "d", 2).wait_send()
        for relation in (1, 2, 3):
            query_copy(relation).wait_send()

    @pl.when(jnp.logical_not(middle))
    def _():
        for record in sent[False]:
            piece_copy(*record).wait_send()
        rows_copy(0, 2, "e", 1).wait_send()

    inbox_copy.wait_recv()
    residual = mixed[:masks, :] + inbox[...]
    normed_final = (layer_norm(residual) * final_gain_ref[...].reshape(1, feature)).astype(bf16)
    dense_out = jnp.dot(normed_final, dense[...], preferred_element_type=f32)
    headed = layer_norm(0.5 * dense_out * (1.0 + lax.erf(dense_out * 0.5**0.5))).astype(bf16)
    logits = lax.dot_general(headed, decoder_ref[...], transposed, preferred_element_type=f32) + bias_ref[...]
    largest = jnp.max(logits, axis=-1, keepdims=True)
    scale = jnp.log(jnp.sum(jnp.exp(logits - largest), axis=-1, keepdims=True)) + largest
    vocabulary = lax.broadcasted_iota(jnp.int32, logits.shape, 1).astype(f32)
    picked = jnp.sum(jnp.where(vocabulary == targets, logits - scale, 0.0), axis=1, keepdims=True)
    row = jnp.sum(jnp.where(eye, picked, 0.0), axis=0, keepdims=True)
    padded = jnp.pad(row, ((0, 0), (0, LANES - masks)))
    scores[me] = jnp.broadcast_to(padded, scores.shape[1:])

    def score_copy(step):
        other = (me + step) % devices
        return pltpu.make_async_remote_copy(
            src_ref=scores.at[me, pl.ds(0, 1), :],
            dst_ref=scores.at[me, pl.ds(0, 1), :],
            send_sem=score_send_sem.at[step],
            recv_sem=score_sem.at[me],
            device_id=(other // n_mp, other % n_mp),
            device_id_type=MESH,
        )

    def send_scores(step, carry):
        score_copy(step).start()
        return carry

    lax.fori_loop(1, devices, send_scores, 0)
    inbox_copy.wait_send()

    def wait_scores(step, carry):
        source = (me + step) % devices
        landing = scores.at[source, pl.ds(0, 1), :]
        pltpu.make_async_copy(landing, landing, score_sem.at[source]).wait()
        return carry

    lax.fori_loop(1, devices, wait_scores, 0)

    def wait_sends(step, carry):
        score_copy(step).wait_send()
        return carry

    lax.fori_loop(1, devices, wait_sends, 0)
    group = out_ref.shape[0]
    wanted = dp * group + lax.broadcasted_iota(jnp.int32, (group, owner_ref.shape[1]), 0)
    select = jnp.where(owner_ref[...] == wanted, 1.0, 0.0)
    out_ref[...] = jnp.dot(select, scores[:, 0, :], preferred_element_type=f32, precision=lax.Precision.HIGHEST)


def split_call(shape, inputs, weight, out_weight, hidden, dense_weight, cosine, sine, group, head_size):
    n_dp, n_mp = shape
    devices = n_dp * n_mp
    seq_span, feature = hidden.shape
    width = weight.shape[1]
    masks = inputs[2].shape[1]
    high = [t.astype(jnp.bfloat16).astype(np.float32) for t in (cosine, sine)]
    parts = [high[0], cosine - high[0], high[1], sine - high[1]]
    split = np.concatenate(parts, axis=1).astype(jnp.bfloat16)
    dma = pltpu.SemaphoreType.DMA
    vmem = pl.BlockSpec(memory_space=pltpu.VMEM)
    smem = pl.BlockSpec(memory_space=pltpu.SMEM)
    anywhere = pl.BlockSpec(memory_space=pl.ANY)
    tiles = seq_span // 128
    return pl.pallas_call(
        functools.partial(split_kernel, (n_dp, n_mp, head_size)),
        name="score_split",
        out_shape=jax.ShapeDtypeStruct((group, LANES), f32),
        in_specs=[smem] * 2 + [vmem] * 7 + [anywhere] * 7,
        out_specs=vmem,
        scratch_shapes=[
            pltpu.VMEM((seq_span, feature), bf16),
            pltpu.VMEM((2, seq_span, feature), bf16),
            pltpu.VMEM((4, masks, feature), bf16),
            pltpu.VMEM((n_mp, width, feature), bf16),
            pltpu.VMEM((n_mp, 2 * head_size, feature), bf16),
            pltpu.VMEM((feature, feature), bf16),
            pltpu.VMEM((seq_span, LANES), f32),
            pltpu.VMEM((seq_span, LANES), f32),
            pltpu.VMEM((seq_span, 4 * LANES), bf16),
            pltpu.VMEM((2, 2, seq_span, 2 * LANES), bf16),
            pltpu.VMEM((2 * masks, 4 * LANES), bf16),
            pltpu.VMEM((n_mp, 2 * masks, LANES), bf16),
            pltpu.VMEM((n_mp, 2 * masks, LANES), bf16),
            pltpu.VMEM((2 * masks, feature), f32),
            pltpu.VMEM((masks, feature), f32),
            pltpu.VMEM((devices, 8, LANES), f32),
            dma((7,)),
            dma((64,)),
            dma((n_mp, 16)),
            dma((2, n_mp)),
            dma((tiles,)),
            dma((tiles,)),
            dma((4,)),
            dma((4,)),
            dma((devices,)),
            dma((devices,)),
            pltpu.SemaphoreType.REGULAR((5,)),
        ],
        compiler_params=pltpu.CompilerParams(collective_id=1, has_side_effects=True),
    )(
        *inputs,
        hidden,
        weight,
        out_weight,
        dense_weight,
        jnp.asarray(cosine),
        jnp.asarray(sine),
        jnp.asarray(split),
    )


def on_device(
    shape,
    hidden_states,
    ln_attn_gain,
    w_qkv,
    output_weight,
    ln_final_gain,
    dense_weight,
    decoder_weight,
    decoder_bias,
    seq_tokens,
    seq_lengths,
    copy_sequence,
    mask_code,
    copy_owner,
):
    n_dp, n_mp = shape
    devices = n_dp * n_mp
    lane_copies, seq_span, feature = hidden_states.shape
    head_size, heads, _ = output_weight.shape
    copies, masks = mask_code.shape
    assert lane_copies == 1 and copies == devices and n_dp % 2 == 0
    assert 2 * head_size == LANES and masks <= LANES
    in_chunk = 2 if heads % 2 == 0 else 1
    chunks = heads // in_chunk
    width = in_chunk * 3 * head_size
    weight = jnp.transpose(w_qkv.reshape(feature, chunks, width), (1, 2, 0))
    out_weight = jnp.swapaxes(output_weight, 0, 1).reshape(heads * head_size, feature)
    cosine, sine = rotary_tables(seq_span, head_size)
    group = copies // n_dp
    items = 2 * chunks + 2
    dma = pltpu.SemaphoreType.DMA
    vmem = pl.BlockSpec(memory_space=pltpu.VMEM)
    smem = pl.BlockSpec(memory_space=pltpu.SMEM)
    anywhere = pl.BlockSpec(memory_space=pl.ANY)
    own = masks // n_mp
    inputs = (
        copy_sequence,
        seq_lengths,
        mask_code,
        seq_tokens,
        copy_owner.reshape(1, -1),
        ln_attn_gain,
        ln_final_gain,
        decoder_weight.T,
        decoder_bias.reshape(1, -1),
    )
    if n_mp == 4 and n_dp == 8 and heads == 4 and seq_span % 128 == 0:
        hidden = hidden_states.reshape(seq_span, feature)
        rows = split_call(shape, inputs, weight, out_weight, hidden, dense_weight, cosine, sine, group, head_size)
        return lax.dynamic_slice_in_dim(rows, lax.axis_index("mp") * own, own, 1)
    rows = pl.pallas_call(
        functools.partial(kernel, (n_dp, n_mp, head_size, in_chunk, chunks)),
        name="score_copies",
        out_shape=jax.ShapeDtypeStruct((group, LANES), f32),
        in_specs=[smem] * 2 + [vmem] * 7 + [anywhere] * 6,
        out_specs=vmem,
        scratch_shapes=[
            pltpu.VMEM((seq_span, feature), bf16),
            pltpu.VMEM((seq_span, feature), bf16),
            pltpu.VMEM((n_mp, chunks, width, feature), bf16),
            pltpu.VMEM((n_mp, heads * head_size, feature), bf16),
            pltpu.VMEM((feature, feature), bf16),
            pltpu.VMEM((seq_span, LANES), f32),
            pltpu.VMEM((seq_span, LANES), f32),
            pltpu.VMEM((seq_span, in_chunk * LANES), bf16),
            pltpu.VMEM((n_mp, chunks, masks, in_chunk * head_size), bf16),
            pltpu.VMEM((masks, feature), f32),
            pltpu.VMEM((devices, 8, LANES), f32),
            dma((6,)),
            dma((n_mp, items)),
            dma((items,)),
            dma((n_mp, chunks)),
            dma((n_mp, items)),
            dma((n_mp, items)),
            dma((n_mp, items)),
            dma((devices,)),
            dma((devices,)),
        ],
        compiler_params=pltpu.CompilerParams(collective_id=0, has_side_effects=True),
    )(
        copy_sequence,
        seq_lengths,
        mask_code,
        seq_tokens,
        copy_owner.reshape(1, -1),
        ln_attn_gain,
        ln_final_gain,
        decoder_weight.T,
        decoder_bias.reshape(1, -1),
        hidden_states.reshape(seq_span, feature),
        weight,
        out_weight,
        dense_weight,
        jnp.asarray(cosine),
        jnp.asarray(sine),
    )
    return lax.dynamic_slice_in_dim(rows, lax.axis_index("mp") * own, own, 1)


def solution(mesh):
    placed = (
        P(("dp", "mp"), None, None),
        P(),
        P(None, "mp", None),
        P(None, "mp", None),
        P(),
        P(),
        P(),
        P(),
        P(),
        P(),
        P(),
        P(),
        P(),
    )
    shape = (mesh.shape["dp"], mesh.shape["mp"])
    return jax.shard_map(
        functools.partial(on_device, shape),
        mesh=mesh,
        in_specs=placed,
        out_specs=P("dp", "mp"),
        check_vma=False,
    )
```

```python
import functools

import jax
import jax.numpy as jnp
import numpy as np
from jax import lax
from jax.experimental import pallas as pl
from jax.experimental.pallas import tpu as pltpu
from jax.sharding import PartitionSpec as P

epsilon = 1e-05
MESH = pl.DeviceIdType.MESH
f32 = jnp.float32
bf16 = jnp.bfloat16
LANES = 128


def layer_norm(inputs):
    average = jnp.mean(inputs, axis=-1, keepdims=True)
    centred = inputs - average
    variance = jnp.mean(centred * centred, axis=-1, keepdims=True)
    return centred * lax.rsqrt(variance + epsilon)


def rotary_tables(seq_span, head_size):
    half = head_size // 2
    frequency = (1.0 / 10000.0 ** (np.arange(half, dtype=np.float32) * (2.0 / head_size))).astype(
        np.float32
    )
    angles = np.arange(seq_span, dtype=np.float32)[:, None] * frequency[None, :]
    cosine, sine = np.cos(angles), np.sin(angles)
    times = LANES // head_size
    return (
        np.tile(np.concatenate([cosine, cosine], axis=1), (1, times)).astype(np.float32),
        np.tile(np.concatenate([-sine, sine], axis=1), (1, times)).astype(np.float32),
    )


def flip(index, mask):
    bit = 1
    out = index
    while bit <= mask:
        if mask & bit:
            out = out + bit * (1 - 2 * ((index // bit) % 2))
        bit *= 2
    return out


def kernel(
    sizes,
    sequence_ref,
    lengths_ref,
    codes_ref,
    tokens_ref,
    owner_ref,
    gain_ref,
    final_gain_ref,
    decoder_ref,
    bias_ref,
    hidden_hbm,
    weight_hbm,
    out_weight_hbm,
    dense_hbm,
    cos_hbm,
    sin_hbm,
    out_ref,
    hidden,
    normed,
    wbuf,
    obuf,
    dense,
    cos,
    sin,
    pbuf,
    context,
    mixed,
    scores,
    local_sem,
    direct_sem,
    relay_sem,
    exchange_sem,
    share_sem,
    arrive_sem,
    shared_sem,
    score_send_sem,
    score_sem,
):
    n_dp, n_mp, head_size, heads_in_chunk, chunks = sizes
    devices = n_dp * n_mp
    dp = lax.axis_index("dp")
    mp = lax.axis_index("mp")
    core = dp % 2
    partner = dp + 1 - 2 * core
    me = dp * n_mp + mp
    seq_span, feature = hidden.shape
    masks = codes_ref.shape[1]
    chunk_heads = heads_in_chunk * head_size
    out_rows = obuf.shape[1]
    piece_rows = out_rows // 4

    def local(index, source, target):
        copy = pltpu.make_async_copy(source, target, local_sem.at[index])
        copy.start()
        return copy

    weight_copy = local(1, weight_hbm, wbuf.at[0])
    hidden_copy = local(0, hidden_hbm, hidden)

    barrier = pltpu.get_barrier_semaphore()

    def greet(step, carry):
        other = (me + step) % devices
        pl.semaphore_signal(
            barrier, inc=1, device_id=(other // n_mp, other % n_mp), device_id_type=MESH
        )
        return carry

    lax.fori_loop(1, devices, greet, 0)

    parity = (dp // 2) % 2
    above = dp + 2 - 4 * parity
    part_rows = wbuf.shape[2] // 4

    def part(chunk, odd):
        return 2 * chunk + odd

    def place(relation, item, half):
        if item < 2 * chunks:
            chunk, odd = divmod(item, 2)
            which = 1 - parity if odd else parity
            start = (2 * half + which) * part_rows
            return wbuf.at[relation, chunk, pl.ds(pl.multiple_of(start, 16), part_rows), :]
        start = (2 * half + item - 2 * chunks) * piece_rows
        return obuf.at[relation, pl.ds(pl.multiple_of(start, 16), piece_rows), :]

    def view(relation, item):
        return place(relation, item, core)

    def partner_view(relation, item):
        return place(relation, item, 1 - core)

    sent = []

    def to_group(target, source_relation, relation, item, semaphore):
        copy = pltpu.make_async_remote_copy(
            src_ref=view(source_relation, item),
            dst_ref=view(relation, item),
            send_sem=semaphore,
            recv_sem=arrive_sem.at[relation, item],
            device_id=(dp, flip(mp, target)),
            device_id_type=MESH,
        )
        copy.start()
        sent.append(copy)

    def direct(target, item):
        to_group(target, 0, target, item, direct_sem.at[target, item])

    def relay(target, source_relation, item):
        to_group(target, source_relation, source_relation ^ target, item, relay_sem.at[item])

    def exchange(relation, chunk):
        copy = pltpu.make_async_remote_copy(
            src_ref=view(relation, part(chunk, 0)),
            dst_ref=view(relation, part(chunk, 0)),
            send_sem=exchange_sem.at[relation, chunk],
            recv_sem=arrive_sem.at[relation, part(chunk, 1)],
            device_id=(above, mp),
            device_id_type=MESH,
        )
        copy.start()
        sent.append(copy)

    def arrived(relation, item):
        landing = view(relation, item)
        pltpu.make_async_copy(landing, landing, arrive_sem.at[relation, item]).wait()

    def share(relation, item):
        copy = pltpu.make_async_remote_copy(
            src_ref=view(relation, item),
            dst_ref=view(relation, item),
            send_sem=share_sem.at[relation, item],
            recv_sem=shared_sem.at[relation, item],
            device_id=(partner, mp),
            device_id_type=MESH,
        )
        copy.start()
        sent.append(copy)

    def was_shared(relation, item):
        landing = partner_view(relation, item)
        pltpu.make_async_copy(landing, landing, shared_sem.at[relation, item]).wait()

    sequence = sequence_ref[me]
    length = lengths_ref[sequence].astype(f32)
    codes = codes_ref[pl.ds(me, 1), :].astype(f32)
    quotient = jnp.floor(codes / length)
    row_positions = codes - quotient * length
    row_positions = jnp.where(row_positions < 0.0, row_positions + length, row_positions)
    row_positions = jnp.where(row_positions >= length, row_positions - length, row_positions)
    eye = lax.broadcasted_iota(jnp.int32, (masks, masks), 0) == lax.broadcasted_iota(
        jnp.int32, (masks, masks), 1
    )
    positions = jnp.sum(jnp.where(eye, row_positions, 0.0), axis=1, keepdims=True)
    places = lax.broadcasted_iota(jnp.int32, (masks, seq_span), 1).astype(f32)
    chosen = places == positions
    onehot = jnp.where(chosen, 1.0, 0.0)
    onehot_bf = onehot.astype(bf16)
    tokens = tokens_ref[pl.ds(sequence, 1), :].astype(f32)
    targets = jnp.sum(jnp.where(chosen, tokens, 0.0), axis=1, keepdims=True)
    alive = lax.broadcasted_iota(jnp.int32, (1, seq_span), 1).astype(f32) < length

    weight_copy.wait()
    pl.semaphore_wait(barrier, devices - 1)
    items = 2 * chunks + 2
    routed = n_mp == 4 and chunks == 2 and n_dp % 4 == 0
    if routed:
        direct(1, part(1, 0))
        direct(2, part(0, 0))
        direct(1, part(0, 0))
        direct(2, part(1, 0))
    cos_copy = local(3, cos_hbm, cos)
    sin_copy = local(4, sin_hbm, sin)
    out_weight_copy = local(2, out_weight_hbm, obuf.at[0])
    dense_copy = local(5, dense_hbm, dense)
    if not routed:
        out_weight_copy.wait()
        for item in range(items):
            for target in range(1, n_mp):
                direct(target, item)

    hidden_copy.wait()
    tile = 128 if seq_span % 128 == 0 else 8

    def norm_rows(step, carry):
        rows = pl.ds(pl.multiple_of(step * tile, tile), tile)
        normed[rows, :] = (layer_norm(hidden[rows, :].astype(f32)) * gain_ref[...].reshape(1, feature)).astype(bf16)
        return carry

    lax.fori_loop(0, seq_span // tile, norm_rows, 0)
    masked_rows = jnp.dot(onehot_bf, normed[...], preferred_element_type=f32).astype(bf16)
    own_rows = jnp.dot(onehot_bf, hidden[...], preferred_element_type=f32)
    mixed[...] = own_rows
    cos_copy.wait()
    sin_copy.wait()
    exact = dict(preferred_element_type=f32, precision=lax.Precision.HIGHEST)
    query_cos = jnp.dot(onehot, cos[...], **exact)
    query_sin = jnp.dot(onehot, sin[...], **exact)
    lane = lax.broadcasted_iota(jnp.int32, (1, LANES), 1)
    first = lane % head_size < head_size // 2

    def rotate(inputs, cosine, sine):
        turned = jnp.where(
            first,
            pltpu.roll(inputs, LANES - head_size // 2, 1),
            pltpu.roll(inputs, head_size // 2, 1),
        )
        return inputs * cosine + turned * sine

    transposed = (((1,), (1,)), ((), ()))
    low = lane < head_size
    span = seq_span // 2 if seq_span % 32 == 0 else seq_span
    head_rows = 3 * head_size

    def attend(relation, chunk):
        weights = wbuf.at[relation, chunk]
        pairs = [
            weights[head * head_rows + head_size : (head + 1) * head_rows, :]
            for head in range(heads_in_chunk)
        ]
        pair_weights = pairs[0] if heads_in_chunk == 1 else jnp.concatenate(pairs, axis=0)

        def project(step, carry):
            rows = pl.ds(pl.multiple_of(step * span, 16), span)
            made = lax.dot_general(
                normed[rows, :], pair_weights, transposed, preferred_element_type=f32
            )
            for head in range(heads_in_chunk):
                block = made[:, head * LANES : (head + 1) * LANES]
                block = jnp.where(low, rotate(block, cos[rows, :], sin[rows, :]), block)
                pbuf[rows, head * LANES : (head + 1) * LANES] = block.astype(bf16)
            return carry

        lax.fori_loop(0, seq_span // span, project, 0)
        if heads_in_chunk == 1:
            query_weights = weights[: 2 * head_size, :]
        else:
            query_weights = jnp.concatenate(
                [weights[:head_size, :], weights[head_rows : head_rows + head_size, :]], axis=0
            )
        made = lax.dot_general(masked_rows, query_weights, transposed, preferred_element_type=f32)
        turned = rotate(made * head_size ** (-0.5), query_cos, query_sin)
        vectors = []
        for head in range(heads_in_chunk):
            query = turned if head == 0 else pltpu.roll(turned, head_size, 1)
            query = jnp.where(low, query, 0.0).astype(bf16)
            block = pbuf[:, head * LANES : (head + 1) * LANES]
            logits = lax.dot_general(query, block, transposed, preferred_element_type=f32)
            logits = jnp.where(alive, logits, -1e30)
            weight = jnp.exp(logits - jnp.max(logits, axis=-1, keepdims=True))
            probs = (weight / jnp.sum(weight, axis=-1, keepdims=True)).astype(bf16)
            vectors.append(jnp.dot(probs, block, preferred_element_type=f32))
        total = pltpu.roll(vectors[0], head_size, 1)
        if heads_in_chunk > 1:
            total = jnp.where(low, total, vectors[1])
        context[relation, chunk] = total[:, :chunk_heads].astype(bf16)

    def mix(relation):
        for chunk in range(chunks):
            rows = slice(chunk * chunk_heads, (chunk + 1) * chunk_heads)
            mixed[...] += jnp.dot(
                context[relation, chunk], obuf[relation, rows, :], preferred_element_type=f32
            )

    def fetch(*pairs):
        for pair in pairs:
            arrived(*pair)
            share(*pair)

    def attend_shared(relation, chunk):
        was_shared(relation, part(chunk, 0))
        was_shared(relation, part(chunk, 1))
        attend(relation, chunk)

    attend(0, 0)
    if routed:
        first_piece, second_piece = 2 * chunks, 2 * chunks + 1
        arrived(1, part(1, 0))
        relay(2, 1, part(1, 0))
        exchange(1, 1)
        share(1, part(1, 0))
        arrived(2, part(0, 0))
        relay(1, 2, part(0, 0))
        exchange(2, 0)
        share(2, part(0, 0))
        direct(1, part(0, 1))
        direct(2, part(1, 1))
        out_weight_copy.wait()
        direct(1, first_piece)
        direct(2, second_piece)
        direct(1, second_piece)
        direct(2, first_piece)
    for chunk in range(1, chunks):
        attend(0, chunk)
    mix(0)
    if routed:
        fetch((1, part(0, 0)), (2, part(1, 0)), (1, part(1, 1)))
        arrived(3, part(0, 0))
        exchange(3, 0)
        share(3, part(0, 0))
        arrived(3, part(1, 0))
        exchange(3, 1)
        share(3, part(1, 0))
        fetch((2, part(0, 1)))
        attend_shared(1, 1)
        attend_shared(2, 0)
        fetch((1, part(0, 1)), (2, part(1, 1)), (3, part(0, 1)))
        attend_shared(1, 0)
        arrived(1, first_piece)
        relay(2, 1, first_piece)
        share(1, first_piece)
        arrived(2, second_piece)
        relay(1, 2, second_piece)
        share(2, second_piece)
        attend_shared(2, 1)
        fetch((3, part(1, 1)))
        attend_shared(3, 0)
        fetch((1, second_piece), (2, first_piece))
        attend_shared(3, 1)
        for relation in (1, 2):
            was_shared(relation, first_piece)
            was_shared(relation, second_piece)
            mix(relation)
        fetch((3, first_piece), (3, second_piece))
        was_shared(3, first_piece)
        was_shared(3, second_piece)
        mix(3)
    else:
        for relation in range(1, n_mp):
            fetch(*[(relation, item) for item in range(items)])
        for relation in range(1, n_mp):
            for item in range(items):
                was_shared(relation, item)
            for chunk in range(chunks):
                attend(relation, chunk)
            mix(relation)

    normed_final = (layer_norm(mixed[...]) * final_gain_ref[...].reshape(1, feature)).astype(bf16)
    dense_copy.wait()
    dense_out = jnp.dot(normed_final, dense[...], preferred_element_type=f32)
    headed = layer_norm(0.5 * dense_out * (1.0 + lax.erf(dense_out * 0.5**0.5))).astype(bf16)
    logits = lax.dot_general(headed, decoder_ref[...], transposed, preferred_element_type=f32) + bias_ref[...]
    largest = jnp.max(logits, axis=-1, keepdims=True)
    scale = jnp.log(jnp.sum(jnp.exp(logits - largest), axis=-1, keepdims=True)) + largest
    vocabulary = lax.broadcasted_iota(jnp.int32, logits.shape, 1).astype(f32)
    picked = jnp.sum(jnp.where(vocabulary == targets, logits - scale, 0.0), axis=1, keepdims=True)
    row = jnp.sum(jnp.where(eye, picked, 0.0), axis=0, keepdims=True)
    padded = jnp.pad(row, ((0, 0), (0, LANES - masks)))
    scores[me] = jnp.broadcast_to(padded, scores.shape[1:])

    def score_copy(step):
        other = (me + step) % devices
        return pltpu.make_async_remote_copy(
            src_ref=scores.at[me, pl.ds(0, 1), :],
            dst_ref=scores.at[me, pl.ds(0, 1), :],
            send_sem=score_send_sem.at[step],
            recv_sem=score_sem.at[me],
            device_id=(other // n_mp, other % n_mp),
            device_id_type=MESH,
        )

    def send_scores(step, carry):
        score_copy(step).start()
        return carry

    lax.fori_loop(1, devices, send_scores, 0)
    for copy in sent:
        copy.wait_send()

    def wait_scores(step, carry):
        source = (me + step) % devices
        landing = scores.at[source, pl.ds(0, 1), :]
        pltpu.make_async_copy(landing, landing, score_sem.at[source]).wait()
        return carry

    lax.fori_loop(1, devices, wait_scores, 0)

    def wait_sends(step, carry):
        score_copy(step).wait_send()
        return carry

    lax.fori_loop(1, devices, wait_sends, 0)
    group = out_ref.shape[0]
    wanted = dp * group + lax.broadcasted_iota(jnp.int32, (group, owner_ref.shape[1]), 0)
    select = jnp.where(owner_ref[...] == wanted, 1.0, 0.0)
    out_ref[...] = jnp.dot(select, scores[:, 0, :], **exact)


ITEMS = {"K0": 0, "V0": 1, "K1": 2, "V1": 3, "Q0": 4, "Q1": 5, "O0": 6, "O1": 7}
FIRST_ROW = {"Q": 0, "K": 64, "V": 128}
ENDS = [('0V0.1>xy', '0V0.0>xy', '0K0.1>xy'),
 ('0O0.0>y',
  '0O0.1>x',
  '0K0.0>xy',
  '0R',
  '2V0.1>e',
  '1K0.1>e',
  '2O0.0>x',
  '0O0.1>y',
  '1V0.1>ey',
  '2K0.0>ex',
  '3V0.1',
  '0O1.0>xy',
  '1V0.0>ey'),
 ('1K0.0>e', '0O0.0>x'),
 ('1K1.1>y', '1O0.1', '1O1.0', '2K0.1>ex', '1K1.0>y'),
 ('1V1.0', '2O0.1>x'),
 ('2V1.0', '2V0.0>e'),
 ('2K1.0', '3K0.0>e', '3K0.1>e'),
 ('2G', '0O1.1>xy', '2V1.1', '1G', '3V0.0'),
 ('3O0.1>e', '3K1.1', '2K1.1', '1V1.1'),
 (),
 ('2O1.0', '3V1.1', '3K1.0'),
 ('3V1.0', '3O0.0>e'),
 ('2O1.1', '1O0.0'),
 ('3G', '1O1.1', '3O1.1'),
 ('3O1.0',)]
MIDS = [('0V1.0>x', '0qx.1>y', '0K1.1>x', '0K1.0>x'),
 ('0ox.1>y',
  '0V1.0>y',
  '0K1.0>y',
  '0qx.1>x',
  '0qx.0>x',
  '1V1.0>e',
  '2ox.1>m',
  '1K1.1>e',
  '0V1.1>y',
  '0qx.0>y',
  '2qx.1>m',
  '2V1.0>ex',
  '0V1.1>x',
  '0ox.0>x',
  '0ox.0>y'),
 ('9R', '1K1.0>e', '1qx.1>my', '1qx.0>my', '2oy.1', '2O1!1>x', '2K1.0>e', '2V1.1>ex'),
 (),
 ('2qx.0>m', '2ox.0>m', '1V1.1>e', '3V1.0>e', '2K0.0', '1V0.1', '0ox.1>x', '2qy.1', '0K1.1>y'),
 ('3qx.1>m',
  '1qy.1',
  '2V0.1',
  '1qy.0',
  'q1',
  '2qy.0',
  '1V0.0',
  '3qx.0>m',
  '1kx!1>y',
  'q2',
  '1kx!0>y',
  '2K1.1>e',
  '1ox.0>m'),
 ('3V1.1>e',),
 ('1K0.1', '3kx.1>m', '2oy.0', '2O1!0>x', '3O1.1>e', '3qy.0', '3qy.1'),
 ('q3', '3kx.0>m', '2V0.0', '1ox.1>m', '2K0.1', '1K0.0'),
 (),
 ('3O1.0>e', '3K0.0', '3ky.1'),
 ('3K0.1', '3ky.0', '1oy.0'),
 (),
 (),
 ('1oy.1', '3O0.0', '3O0.1')]


def split_kernel(
    sizes,
    sequence_hbm,
    lengths_hbm,
    codes_hbm,
    tokens_hbm,
    owner_hbm,
    gain_hbm,
    final_gain_hbm,
    decoder_hbm,
    bias_hbm,
    hidden_hbm,
    weight_hbm,
    out_weight_hbm,
    dense_hbm,
    cos_hbm,
    sin_hbm,
    split_hbm,
    out_ref,
    sequence_ref,
    lengths_ref,
    codes_ref,
    tokens_ref,
    owner_ref,
    gain_ref,
    final_gain_ref,
    decoder_ref,
    bias_ref,
    hidden,
    normed,
    rows_buf,
    wbuf,
    raw,
    obuf,
    dense,
    cos,
    sin,
    split,
    pbuf,
    context,
    qbuf,
    gbuf,
    mixed,
    inbox,
    scores,
    local_sem,
    send_sem,
    arrive_sem,
    query_sem,
    norm_send_sem,
    norm_sem,
    swap_send_sem,
    swap_sem,
    score_send_sem,
    score_sem,
    token_sem,
):
    n_dp, n_mp, head_size = sizes
    devices = n_dp * n_mp
    layers = n_dp // 2
    dp = lax.axis_index("dp")
    mp = lax.axis_index("mp")
    core = dp % 2
    layer = dp // 2
    partner = dp + 1 - 2 * core
    me = dp * n_mp + mp
    mate = partner * n_mp + mp
    parity = layer % 2
    pair = dp + 2 - 4 * parity
    twin = dp - 2 + 4 * parity
    middle = jnp.logical_and(layer > 0, layer < layers - 1)
    side = 1 - parity
    seq_span, feature = hidden.shape
    masks = codes_ref.shape[1]
    head_rows = 3 * head_size
    half_rows = head_size // 2
    where = {"x": (dp, flip(mp, 1)), "y": (dp, flip(mp, 2)), "e": (pair, mp), "m": (twin, mp), "d": (partner, mp)}

    barrier = pltpu.get_barrier_semaphore()

    def signal(semaphore, target):
        pl.semaphore_signal(semaphore, inc=1, device_id=target, device_id_type=MESH)

    for link in "dxye":
        signal(barrier, where[link])

    @pl.when(middle)
    def _():
        signal(barrier, where["m"])

    def local(index, source, target):
        copy = pltpu.make_async_copy(source, target, local_sem.at[index])
        copy.start()
        return copy

    weight_copy = local(1, weight_hbm.at[core], wbuf.at[0])
    hidden_copy = local(0, hidden_hbm, hidden)
    small_copies = [
        local(7 + place, source, target)
        for place, (source, target) in enumerate(
            (
                (sequence_hbm, sequence_ref),
                (lengths_hbm, lengths_ref),
                (codes_hbm, codes_ref),
                (tokens_hbm, tokens_ref),
                (gain_hbm, gain_ref),
            )
        )
    ]
    out_weight_copy = local(2, out_weight_hbm.at[:, pl.ds(pl.multiple_of(2 * core, 2), 2), :], raw)
    late_copies = [
        local(12 + place, source, target)
        for place, (source, target) in enumerate(
            (
                (owner_hbm, owner_ref),
                (final_gain_hbm, final_gain_ref),
                (decoder_hbm, decoder_ref),
                (bias_hbm, bias_ref),
            )
        )
    ]
    cos_copy = local(3, cos_hbm, cos)
    sin_copy = local(4, sin_hbm, sin)
    split_copy = local(6, split_hbm, split)
    dense_copy = local(5, dense_hbm, dense)

    def number(item):
        if item in ITEMS:
            return ITEMS[item]
        return {"qx": 4 + side, "qy": 5 - side, "ox": 6 + side, "oy": 7 - side, "kx": 2 - side, "ky": 1 + side}[item]

    def view(relation, item, half):
        if item in ITEMS:
            kind, head = item[0], int(item[1])
            start = head * head_size if kind == "O" else head * head_rows + FIRST_ROW[kind]
        elif item[0] == "k":
            kind = "K"
            start = 256 - 128 * side if item == "kx" else 128 + 128 * side
        else:
            kind = item[0].upper()
            start = (side if item[1] == "x" else 1 - side) * (head_rows if kind == "Q" else head_size)
        rows = pl.ds(pl.multiple_of(start + half * half_rows, half_rows), half_rows)
        return (obuf if kind == "O" else wbuf).at[relation, rows, :]

    flips = {"x": 1, "y": 2, "e": 0, "m": 0}

    def piece_copy(relation, item, half, link, index):
        target = relation ^ flips[link]
        return pltpu.make_async_remote_copy(
            src_ref=view(relation, item, half),
            dst_ref=view(target, item, half),
            send_sem=send_sem.at[index],
            recv_sem=arrive_sem.at[target, 2 * number(item) + half],
            device_id=where[link],
            device_id_type=MESH,
        )

    def rows_copy(source, target, link, index):
        return pltpu.make_async_remote_copy(
            src_ref=rows_buf.at[source],
            dst_ref=rows_buf.at[target],
            send_sem=swap_send_sem.at[index],
            recv_sem=swap_sem.at[index],
            device_id=where[link],
            device_id_type=MESH,
        )

    def query_copy(relation):
        return pltpu.make_async_remote_copy(
            src_ref=gbuf.at[relation],
            dst_ref=qbuf.at[relation],
            send_sem=query_sem.at[0, relation],
            recv_sem=query_sem.at[1, relation],
            device_id=where["e"],
            device_id_type=MESH,
        )

    sent = {True: [], False: []}

    def serve(words, in_middle):
        for word in words:
            if word in ("q1", "q2", "q3"):
                project_queries(int(word[1]))
                continue
            name, _, links = word.partition(">")
            relation, item = int(name[0]), name[1:3]
            if item == "R":
                if in_middle:
                    rows_copy(0, 2, "e", 1).wait_recv()
                    rows_copy(2, 3, "d", 2).start()
                else:
                    rows_copy(0, 2, "e", 1).start()
                continue
            if item == "G":
                query_copy(relation).wait_recv()
                continue
            half = int(name[4])
            if relation and name[3] != "!":
                landing = view(relation, item, half)
                pltpu.make_async_copy(
                    landing, landing, arrive_sem.at[relation, 2 * number(item) + half]
                ).wait()
            for link in links:
                index = len(sent[in_middle])
                sent[in_middle].append((relation, item, half, link, index))
                piece_copy(relation, item, half, link, index).start()

    def service(index):
        if MIDS[index]:

            @pl.when(middle)
            def _():
                serve(MIDS[index], True)

        if ENDS[index]:

            @pl.when(jnp.logical_not(middle))
            def _():
                serve(ENDS[index], False)

    weight_copy.wait()
    pl.semaphore_wait(barrier, 4 + middle.astype(jnp.int32))
    service(0)
    for copy in small_copies:
        copy.wait()
    out_weight_copy.wait()
    for head in range(2):
        obuf[0, head * head_size : (head + 1) * head_size, :] = raw[:, head, :]
    signal(token_sem.at[0], (partner, mp))

    def tokens_step(step):
        if step == 0:
            pl.semaphore_wait(token_sem.at[0], 1)
            signal(token_sem.at[1], (dp, flip(mp, 1)))
        elif step == 1:
            pl.semaphore_wait(token_sem.at[1], 1)
            signal(token_sem.at[2], (dp, flip(mp, 2)))
        else:
            hop = step - 3
            if hop < 0:
                pl.semaphore_wait(token_sem.at[2], 1)
            else:

                @pl.when(layer == hop + 1)
                def _():
                    pl.semaphore_wait(token_sem.at[3], 1)

                @pl.when(layer == layers - 2 - hop)
                def _():
                    pl.semaphore_wait(token_sem.at[4], 1)

            if hop + 1 < layers - 1:

                @pl.when(layer == hop + 1)
                def _():
                    signal(token_sem.at[3], (dp + 2, mp))

                @pl.when(layer == layers - 2 - hop)
                def _():
                    signal(token_sem.at[4], (dp - 2, mp))

    eye = lax.broadcasted_iota(jnp.int32, (masks, masks), 0) == lax.broadcasted_iota(
        jnp.int32, (masks, masks), 1
    )
    places = lax.broadcasted_iota(jnp.int32, (masks, seq_span), 1).astype(f32)

    def locate(which):
        length = lengths_ref[sequence_ref[which]].astype(f32)
        codes = codes_ref[pl.ds(which, 1), :].astype(f32)
        quotient = jnp.floor(codes / length)
        spots = codes - quotient * length
        spots = jnp.where(spots < 0.0, spots + length, spots)
        spots = jnp.where(spots >= length, spots - length, spots)
        spots = jnp.sum(jnp.where(eye, spots, 0.0), axis=1, keepdims=True)
        live = lax.broadcasted_iota(jnp.int32, (1, seq_span), 1).astype(f32) < length
        return places == spots, live

    located = [locate(which) for which in (me, mate, pair * n_mp + mp, (pair + 1 - 2 * core) * n_mp + mp)]
    chosen = located[0][0]
    alive = [live for _, live in located]
    tokens = tokens_ref[pl.ds(sequence_ref[me], 1), :].astype(f32)
    targets = jnp.sum(jnp.where(chosen, tokens, 0.0), axis=1, keepdims=True)
    onehots = [jnp.where(spots, 1.0, 0.0).astype(bf16) for spots, _ in located]
    onehot = onehots[0]

    hidden_copy.wait()
    tile = 128

    def norm_copy(step):
        rows = pl.ds(pl.multiple_of(step * tile, tile), tile)
        return pltpu.make_async_remote_copy(
            src_ref=normed.at[0, rows, :],
            dst_ref=normed.at[1, rows, :],
            send_sem=norm_send_sem.at[step],
            recv_sem=norm_sem.at[step],
            device_id=(partner, mp),
            device_id_type=MESH,
        )

    def norm_rows(step, carry):
        rows = pl.ds(pl.multiple_of(step * tile, tile), tile)
        normed[0, rows, :] = (layer_norm(hidden[rows, :].astype(f32)) * gain_ref[...].reshape(1, feature)).astype(bf16)
        return carry

    lax.fori_loop(0, seq_span // tile, norm_rows, 0)
    rows_buf[0] = jnp.dot(onehot, normed[0], preferred_element_type=f32).astype(bf16)
    for step in range(seq_span // tile):
        norm_copy(step).start()
    mixed[:masks, :] = jnp.dot(onehot, hidden[...], preferred_element_type=f32)
    mixed[masks:, :] = jnp.zeros((masks, feature), f32)
    rows_copy(0, 1, "d", 0).start()
    split_copy.wait()
    table = jnp.dot(jnp.concatenate(onehots, axis=0), split[...], preferred_element_type=f32)
    query_cos = table[:, :LANES] + table[:, LANES : 2 * LANES]
    query_sin = table[:, 2 * LANES : 3 * LANES] + table[:, 3 * LANES :]
    lane = lax.broadcasted_iota(jnp.int32, (1, LANES), 1)
    first = lane % head_size < head_size // 2
    low = lane < head_size
    transposed = (((1,), (1,)), ((), ()))

    def rotate(inputs, cosine, sine):
        turned = jnp.where(
            first,
            pltpu.roll(inputs, LANES - head_size // 2, 1),
            pltpu.roll(inputs, head_size // 2, 1),
        )
        return inputs * cosine + turned * sine

    span = seq_span // 2

    def stack(refs):
        return jnp.concatenate([ref[...] for ref in refs], axis=0)

    def rows_of(start, count):
        return pl.ds(start if isinstance(start, int) else pl.multiple_of(start, head_size), count)

    def project(unit, buffer, slot):
        keys = stack(
            [wbuf.at[relation, rows_of(head * head_rows + head_size, 2 * head_size), :] for relation, head in unit]
        )

        def step_of(step, carry):
            rows = pl.ds(pl.multiple_of(step * span, 16), span)
            made = lax.dot_general(normed[slot, rows, :], keys, transposed, preferred_element_type=f32)
            for head in range(2):
                block = made[:, head * LANES : (head + 1) * LANES]
                block = jnp.where(low, rotate(block, cos[rows, :], sin[rows, :]), block)
                pbuf[buffer, slot, rows, head * LANES : (head + 1) * LANES] = block.astype(bf16)
            return carry

        lax.fori_loop(0, seq_span // span, step_of, 0)

    def queries(relation, low_slot, high_slot):
        weights = stack([wbuf.at[relation, head * head_rows : head * head_rows + head_size, :] for head in range(2)])
        rows = slice(low_slot * masks, high_slot * masks)
        source = rows_buf[low_slot:high_slot].reshape((high_slot - low_slot) * masks, feature)
        made = lax.dot_general(source, weights, transposed, preferred_element_type=f32)
        return rotate(made * head_size ** (-0.5), query_cos[rows], query_sin[rows]).astype(bf16)

    def project_queries(relation):
        if relation == 1:
            rows_copy(2, 3, "d", 2).wait_recv()
        made = queries(relation, 0, 4)
        gbuf[relation] = made[2 * masks :]
        qbuf[relation] = made[: 2 * masks]
        query_copy(relation).start()

    def of_head(query, head):
        query = query.astype(f32)
        if isinstance(head, int):
            return pltpu.roll(query, head_size, 1) if head else query
        return jnp.where(head == 1, pltpu.roll(query, head_size, 1), query)

    def attend(which, buffer, slot, near, far):
        empty = jnp.zeros((masks, LANES), bf16)
        near = jnp.where(low, near, 0.0).astype(bf16)
        far = jnp.where(low, far, 0.0).astype(bf16)
        both = jnp.concatenate(
            [jnp.concatenate([near, empty], axis=1), jnp.concatenate([empty, far], axis=1)], axis=0
        )
        block = pbuf[buffer, slot]
        logits = lax.dot_general(both, block, transposed, preferred_element_type=f32)
        logits = jnp.where(alive[slot], logits, -1e30)
        weight = jnp.exp(logits - jnp.max(logits, axis=-1, keepdims=True))
        probs = (weight / jnp.sum(weight, axis=-1, keepdims=True)).astype(bf16)
        vectors = jnp.dot(probs, block, preferred_element_type=f32)
        total = jnp.where(low, pltpu.roll(vectors[:masks, :LANES], head_size, 1), vectors[masks:, LANES:])
        context[slot * masks : (slot + 1) * masks, which * LANES : (which + 1) * LANES] = total.astype(bf16)

    def attend_both(which, unit, buffer):
        for slot in range(2):
            rows = slice(slot * masks, (slot + 1) * masks)
            near, far = [of_head(qbuf[relation, rows, :], head) for relation, head in unit]
            attend(which, buffer, slot, near, far)

    def mix(low_unit, *units):
        out_weights = stack([obuf.at[relation, rows_of(head * head_size, head_size), :] for unit in units for relation, head in unit])
        lanes = slice(low_unit * LANES, (low_unit + len(units)) * LANES)
        mixed[...] += jnp.dot(context[:, lanes], out_weights, preferred_element_type=f32)

    early = middle.astype(jnp.int32)
    own = ((0, 0), (0, 1))
    firsts = ((1, early), (2, early))
    seconds = ((1, 1 - early), (2, 1 - early))
    across = ((3, 0), (3, 1))

    cos_copy.wait()
    sin_copy.wait()
    service(1)
    project(own, 0, 0)
    service(2)
    query = queries(0, 0, 1)
    attend(0, 0, 0, of_head(query, 0), of_head(query, 1))
    tokens_step(0)
    service(3)
    for step in range(seq_span // tile):
        norm_copy(step).wait_recv()
    rows_copy(0, 1, "d", 0).wait_recv()
    project(own, 0, 1)
    service(4)
    query = queries(0, 1, 2)
    attend(0, 0, 1, of_head(query, 0), of_head(query, 1))
    mix(0, own)
    tokens_step(1)
    service(5)
    project(firsts, 1, 0)
    service(6)
    project(firsts, 1, 1)
    tokens_step(2)
    service(7)
    attend_both(1, firsts, 1)
    tokens_step(3)
    service(8)
    project(seconds, 0, 0)
    service(9)
    project(seconds, 0, 1)
    service(10)
    attend_both(2, seconds, 0)
    tokens_step(4)
    service(11)
    project(across, 1, 0)
    service(12)
    project(across, 1, 1)
    service(13)
    attend_both(3, across, 1)
    tokens_step(5)
    service(14)
    mix(1, firsts, seconds, across)
    inbox_copy = pltpu.make_async_remote_copy(
        src_ref=mixed.at[pl.ds(masks, masks), :],
        dst_ref=inbox,
        send_sem=swap_send_sem.at[3],
        recv_sem=swap_sem.at[3],
        device_id=(partner, mp),
        device_id_type=MESH,
    )
    inbox_copy.start()
    dense_copy.wait()
    for copy in late_copies:
        copy.wait()
    for step in range(seq_span // tile):
        norm_copy(step).wait_send()
    rows_copy(0, 1, "d", 0).wait_send()

    @pl.when(middle)
    def _():
        for record in sent[True]:
            piece_copy(*record).wait_send()
        rows_copy(2, 3, "d", 2).wait_send()
        for relation in (1, 2, 3):
            query_copy(relation).wait_send()

    @pl.when(jnp.logical_not(middle))
    def _():
        for record in sent[False]:
            piece_copy(*record).wait_send()
        rows_copy(0, 2, "e", 1).wait_send()

    inbox_copy.wait_recv()
    residual = mixed[:masks, :] + inbox[...]
    normed_final = (layer_norm(residual) * final_gain_ref[...].reshape(1, feature)).astype(bf16)
    dense_out = jnp.dot(normed_final, dense[...], preferred_element_type=f32)
    headed = layer_norm(0.5 * dense_out * (1.0 + lax.erf(dense_out * 0.5**0.5))).astype(bf16)
    logits = lax.dot_general(headed, decoder_ref[...], transposed, preferred_element_type=f32) + bias_ref[...]
    largest = jnp.max(logits, axis=-1, keepdims=True)
    scale = jnp.log(jnp.sum(jnp.exp(logits - largest), axis=-1, keepdims=True)) + largest
    vocabulary = lax.broadcasted_iota(jnp.int32, logits.shape, 1).astype(f32)
    picked = jnp.sum(jnp.where(vocabulary == targets, logits - scale, 0.0), axis=1, keepdims=True)
    row = jnp.sum(jnp.where(eye, picked, 0.0), axis=0, keepdims=True)
    padded = jnp.pad(row, ((0, 0), (0, LANES - masks)))
    scores[me] = jnp.broadcast_to(padded, scores.shape[1:])

    def score_copy(step):
        other_dp, other_mp = flip(dp, step // n_mp), flip(mp, step % n_mp)
        return pltpu.make_async_remote_copy(
            src_ref=scores.at[me, pl.ds(0, 1), :],
            dst_ref=scores.at[me, pl.ds(0, 1), :],
            send_sem=score_send_sem.at[step],
            recv_sem=score_sem.at[step],
            device_id=(other_dp, other_mp),
            device_id_type=MESH,
        )

    for step in reversed(range(1, devices)):
        score_copy(step).start()
    inbox_copy.wait_send()
    for step in range(1, devices):
        source = flip(dp, step // n_mp) * n_mp + flip(mp, step % n_mp)
        landing = scores.at[source, pl.ds(0, 1), :]
        pltpu.make_async_copy(landing, landing, score_sem.at[step]).wait()
    for step in range(1, devices):
        score_copy(step).wait_send()
    group = out_ref.shape[0]
    wanted = dp * group + lax.broadcasted_iota(jnp.int32, (group, owner_ref.shape[1]), 0)
    select = jnp.where(owner_ref[...] == wanted, 1.0, 0.0)
    out_ref[...] = jnp.dot(select, scores[:, 0, :], preferred_element_type=f32, precision=lax.Precision.HIGHEST)


def split_call(shape, inputs, weight, out_weight, hidden, dense_weight, cosine, sine, group, head_size):
    n_dp, n_mp = shape
    devices = n_dp * n_mp
    seq_span, feature = hidden.shape
    width = weight.shape[1]
    masks = inputs[2].shape[1]
    high = [t.astype(jnp.bfloat16).astype(np.float32) for t in (cosine, sine)]
    parts = [high[0], cosine - high[0], high[1], sine - high[1]]
    split = np.concatenate(parts, axis=1).astype(jnp.bfloat16)
    dma = pltpu.SemaphoreType.DMA
    vmem = pl.BlockSpec(memory_space=pltpu.VMEM)
    anywhere = pl.BlockSpec(memory_space=pl.ANY)
    tiles = seq_span // 128
    return pl.pallas_call(
        functools.partial(split_kernel, (n_dp, n_mp, head_size)),
        name="score_split",
        out_shape=jax.ShapeDtypeStruct((group, LANES), f32),
        in_specs=[anywhere] * 16,
        out_specs=vmem,
        scratch_shapes=[(pltpu.SMEM if place < 2 else pltpu.VMEM)(x.shape, x.dtype) for place, x in enumerate(inputs)]
        + [
            pltpu.VMEM((seq_span, feature), bf16),
            pltpu.VMEM((2, seq_span, feature), bf16),
            pltpu.VMEM((4, masks, feature), bf16),
            pltpu.VMEM((n_mp, width, feature), bf16),
            pltpu.VMEM((head_size, 2, feature), bf16),
            pltpu.VMEM((n_mp, 2 * head_size, feature), bf16),
            pltpu.VMEM((feature, feature), bf16),
            pltpu.VMEM((seq_span, LANES), f32),
            pltpu.VMEM((seq_span, LANES), f32),
            pltpu.VMEM((seq_span, 4 * LANES), bf16),
            pltpu.VMEM((2, 2, seq_span, 2 * LANES), bf16),
            pltpu.VMEM((2 * masks, 4 * LANES), bf16),
            pltpu.VMEM((n_mp, 2 * masks, LANES), bf16),
            pltpu.VMEM((n_mp, 2 * masks, LANES), bf16),
            pltpu.VMEM((2 * masks, feature), f32),
            pltpu.VMEM((masks, feature), f32),
            pltpu.VMEM((devices, 8, LANES), f32),
            dma((16,)),
            dma((64,)),
            dma((n_mp, 16)),
            dma((2, n_mp)),
            dma((tiles,)),
            dma((tiles,)),
            dma((4,)),
            dma((4,)),
            dma((devices,)),
            dma((devices,)),
            pltpu.SemaphoreType.REGULAR((5,)),
        ],
        compiler_params=pltpu.CompilerParams(collective_id=1, has_side_effects=True),
    )(
        *inputs,
        hidden,
        weight,
        out_weight,
        dense_weight,
        jnp.asarray(cosine),
        jnp.asarray(sine),
        jnp.asarray(split),
    )


def on_device(
    shape,
    hidden_states,
    ln_attn_gain,
    w_qkv,
    output_weight,
    ln_final_gain,
    dense_weight,
    decoder_weight,
    decoder_bias,
    seq_tokens,
    seq_lengths,
    copy_sequence,
    mask_code,
    copy_owner,
):
    n_dp, n_mp = shape
    devices = n_dp * n_mp
    lane_copies, seq_span, feature = hidden_states.shape
    head_size, heads, _ = output_weight.shape
    copies, masks = mask_code.shape
    assert lane_copies == 1 and copies == devices and n_dp % 2 == 0
    assert 2 * head_size == LANES and masks <= LANES
    in_chunk = 2 if heads % 2 == 0 else 1
    chunks = heads // in_chunk
    width = in_chunk * 3 * head_size
    weight = jnp.transpose(w_qkv.reshape(feature, chunks, width), (1, 2, 0))
    cosine, sine = rotary_tables(seq_span, head_size)
    group = copies // n_dp
    items = 2 * chunks + 2
    dma = pltpu.SemaphoreType.DMA
    vmem = pl.BlockSpec(memory_space=pltpu.VMEM)
    smem = pl.BlockSpec(memory_space=pltpu.SMEM)
    anywhere = pl.BlockSpec(memory_space=pl.ANY)
    own = masks // n_mp
    inputs = (
        copy_sequence,
        seq_lengths,
        mask_code,
        seq_tokens,
        copy_owner.reshape(1, -1),
        ln_attn_gain,
        ln_final_gain,
        decoder_weight.T,
        decoder_bias.reshape(1, -1),
    )
    if n_mp == 4 and n_dp == 8 and heads == 4 and seq_span % 128 == 0:
        hidden = hidden_states.reshape(seq_span, feature)
        rows = split_call(shape, inputs, weight, output_weight, hidden, dense_weight, cosine, sine, group, head_size)
        return lax.dynamic_slice_in_dim(rows, lax.axis_index("mp") * own, own, 1)
    out_weight = jnp.swapaxes(output_weight, 0, 1).reshape(heads * head_size, feature)
    rows = pl.pallas_call(
        functools.partial(kernel, (n_dp, n_mp, head_size, in_chunk, chunks)),
        name="score_copies",
        out_shape=jax.ShapeDtypeStruct((group, LANES), f32),
        in_specs=[smem] * 2 + [vmem] * 7 + [anywhere] * 6,
        out_specs=vmem,
        scratch_shapes=[
            pltpu.VMEM((seq_span, feature), bf16),
            pltpu.VMEM((seq_span, feature), bf16),
            pltpu.VMEM((n_mp, chunks, width, feature), bf16),
            pltpu.VMEM((n_mp, heads * head_size, feature), bf16),
            pltpu.VMEM((feature, feature), bf16),
            pltpu.VMEM((seq_span, LANES), f32),
            pltpu.VMEM((seq_span, LANES), f32),
            pltpu.VMEM((seq_span, in_chunk * LANES), bf16),
            pltpu.VMEM((n_mp, chunks, masks, in_chunk * head_size), bf16),
            pltpu.VMEM((masks, feature), f32),
            pltpu.VMEM((devices, 8, LANES), f32),
            dma((6,)),
            dma((n_mp, items)),
            dma((items,)),
            dma((n_mp, chunks)),
            dma((n_mp, items)),
            dma((n_mp, items)),
            dma((n_mp, items)),
            dma((devices,)),
            dma((devices,)),
        ],
        compiler_params=pltpu.CompilerParams(collective_id=0, has_side_effects=True),
    )(
        copy_sequence,
        seq_lengths,
        mask_code,
        seq_tokens,
        copy_owner.reshape(1, -1),
        ln_attn_gain,
        ln_final_gain,
        decoder_weight.T,
        decoder_bias.reshape(1, -1),
        hidden_states.reshape(seq_span, feature),
        weight,
        out_weight,
        dense_weight,
        jnp.asarray(cosine),
        jnp.asarray(sine),
    )
    return lax.dynamic_slice_in_dim(rows, lax.axis_index("mp") * own, own, 1)


def solution(mesh):
    placed = (
        P(("dp", "mp"), None, None),
        P(),
        P(None, "mp", None),
        P(None, "mp", None),
        P(),
        P(),
        P(),
        P(),
        P(),
        P(),
        P(),
        P(),
        P(),
    )
    shape = (mesh.shape["dp"], mesh.shape["mp"])
    return jax.shard_map(
        functools.partial(on_device, shape),
        mesh=mesh,
        in_specs=placed,
        out_specs=P("dp", "mp"),
        check_vma=False,
    )
```

```python
import functools

import jax
import jax.numpy as jnp
import numpy as np
from jax import lax
from jax.experimental import pallas as pl
from jax.experimental.pallas import tpu as pltpu
from jax.sharding import PartitionSpec as P

epsilon = 1e-05
MESH = pl.DeviceIdType.MESH
f32 = jnp.float32
bf16 = jnp.bfloat16
LANES = 128


def layer_norm(inputs):
    average = jnp.mean(inputs, axis=-1, keepdims=True)
    centred = inputs - average
    variance = jnp.mean(centred * centred, axis=-1, keepdims=True)
    return centred * lax.rsqrt(variance + epsilon)


def rotary_tables(seq_span, head_size):
    half = head_size // 2
    frequency = (1.0 / 10000.0 ** (np.arange(half, dtype=np.float32) * (2.0 / head_size))).astype(
        np.float32
    )
    angles = np.arange(seq_span, dtype=np.float32)[:, None] * frequency[None, :]
    cosine, sine = np.cos(angles), np.sin(angles)
    times = LANES // head_size
    return (
        np.tile(np.concatenate([cosine, cosine], axis=1), (1, times)).astype(np.float32),
        np.tile(np.concatenate([-sine, sine], axis=1), (1, times)).astype(np.float32),
    )


def flip(index, mask):
    bit = 1
    out = index
    while bit <= mask:
        if mask & bit:
            out = out + bit * (1 - 2 * ((index // bit) % 2))
        bit *= 2
    return out


def kernel(
    sizes,
    sequence_ref,
    lengths_ref,
    codes_ref,
    tokens_ref,
    owner_ref,
    gain_ref,
    final_gain_ref,
    decoder_ref,
    bias_ref,
    hidden_hbm,
    weight_hbm,
    out_weight_hbm,
    dense_hbm,
    cos_hbm,
    sin_hbm,
    out_ref,
    hidden,
    normed,
    wbuf,
    obuf,
    dense,
    cos,
    sin,
    pbuf,
    context,
    mixed,
    scores,
    local_sem,
    direct_sem,
    relay_sem,
    exchange_sem,
    share_sem,
    arrive_sem,
    shared_sem,
    score_send_sem,
    score_sem,
):
    n_dp, n_mp, head_size, heads_in_chunk, chunks = sizes
    devices = n_dp * n_mp
    dp = lax.axis_index("dp")
    mp = lax.axis_index("mp")
    core = dp % 2
    partner = dp + 1 - 2 * core
    me = dp * n_mp + mp
    seq_span, feature = hidden.shape
    masks = codes_ref.shape[1]
    chunk_heads = heads_in_chunk * head_size
    out_rows = obuf.shape[1]
    piece_rows = out_rows // 4

    def local(index, source, target):
        copy = pltpu.make_async_copy(source, target, local_sem.at[index])
        copy.start()
        return copy

    weight_copy = local(1, weight_hbm, wbuf.at[0])
    hidden_copy = local(0, hidden_hbm, hidden)

    barrier = pltpu.get_barrier_semaphore()

    def greet(step, carry):
        other = (me + step) % devices
        pl.semaphore_signal(
            barrier, inc=1, device_id=(other // n_mp, other % n_mp), device_id_type=MESH
        )
        return carry

    lax.fori_loop(1, devices, greet, 0)

    parity = (dp // 2) % 2
    above = dp + 2 - 4 * parity
    part_rows = wbuf.shape[2] // 4

    def part(chunk, odd):
        return 2 * chunk + odd

    def place(relation, item, half):
        if item < 2 * chunks:
            chunk, odd = divmod(item, 2)
            which = 1 - parity if odd else parity
            start = (2 * half + which) * part_rows
            return wbuf.at[relation, chunk, pl.ds(pl.multiple_of(start, 16), part_rows), :]
        start = (2 * half + item - 2 * chunks) * piece_rows
        return obuf.at[relation, pl.ds(pl.multiple_of(start, 16), piece_rows), :]

    def view(relation, item):
        return place(relation, item, core)

    def partner_view(relation, item):
        return place(relation, item, 1 - core)

    sent = []

    def to_group(target, source_relation, relation, item, semaphore):
        copy = pltpu.make_async_remote_copy(
            src_ref=view(source_relation, item),
            dst_ref=view(relation, item),
            send_sem=semaphore,
            recv_sem=arrive_sem.at[relation, item],
            device_id=(dp, flip(mp, target)),
            device_id_type=MESH,
        )
        copy.start()
        sent.append(copy)

    def direct(target, item):
        to_group(target, 0, target, item, direct_sem.at[target, item])

    def relay(target, source_relation, item):
        to_group(target, source_relation, source_relation ^ target, item, relay_sem.at[item])

    def exchange(relation, chunk):
        copy = pltpu.make_async_remote_copy(
            src_ref=view(relation, part(chunk, 0)),
            dst_ref=view(relation, part(chunk, 0)),
            send_sem=exchange_sem.at[relation, chunk],
            recv_sem=arrive_sem.at[relation, part(chunk, 1)],
            device_id=(above, mp),
            device_id_type=MESH,
        )
        copy.start()
        sent.append(copy)

    def arrived(relation, item):
        landing = view(relation, item)
        pltpu.make_async_copy(landing, landing, arrive_sem.at[relation, item]).wait()

    def share(relation, item):
        copy = pltpu.make_async_remote_copy(
            src_ref=view(relation, item),
            dst_ref=view(relation, item),
            send_sem=share_sem.at[relation, item],
            recv_sem=shared_sem.at[relation, item],
            device_id=(partner, mp),
            device_id_type=MESH,
        )
        copy.start()
        sent.append(copy)

    def was_shared(relation, item):
        landing = partner_view(relation, item)
        pltpu.make_async_copy(landing, landing, shared_sem.at[relation, item]).wait()

    sequence = sequence_ref[me]
    length = lengths_ref[sequence].astype(f32)
    codes = codes_ref[pl.ds(me, 1), :].astype(f32)
    quotient = jnp.floor(codes / length)
    row_positions = codes - quotient * length
    row_positions = jnp.where(row_positions < 0.0, row_positions + length, row_positions)
    row_positions = jnp.where(row_positions >= length, row_positions - length, row_positions)
    eye = lax.broadcasted_iota(jnp.int32, (masks, masks), 0) == lax.broadcasted_iota(
        jnp.int32, (masks, masks), 1
    )
    positions = jnp.sum(jnp.where(eye, row_positions, 0.0), axis=1, keepdims=True)
    places = lax.broadcasted_iota(jnp.int32, (masks, seq_span), 1).astype(f32)
    chosen = places == positions
    onehot = jnp.where(chosen, 1.0, 0.0)
    onehot_bf = onehot.astype(bf16)
    tokens = tokens_ref[pl.ds(sequence, 1), :].astype(f32)
    targets = jnp.sum(jnp.where(chosen, tokens, 0.0), axis=1, keepdims=True)
    alive = lax.broadcasted_iota(jnp.int32, (1, seq_span), 1).astype(f32) < length

    weight_copy.wait()
    pl.semaphore_wait(barrier, devices - 1)
    items = 2 * chunks + 2
    routed = n_mp == 4 and chunks == 2 and n_dp % 4 == 0
    if routed:
        direct(1, part(1, 0))
        direct(2, part(0, 0))
        direct(1, part(0, 0))
        direct(2, part(1, 0))
    cos_copy = local(3, cos_hbm, cos)
    sin_copy = local(4, sin_hbm, sin)
    out_weight_copy = local(2, out_weight_hbm, obuf.at[0])
    dense_copy = local(5, dense_hbm, dense)
    if not routed:
        out_weight_copy.wait()
        for item in range(items):
            for target in range(1, n_mp):
                direct(target, item)

    hidden_copy.wait()
    tile = 128 if seq_span % 128 == 0 else 8

    def norm_rows(step, carry):
        rows = pl.ds(pl.multiple_of(step * tile, tile), tile)
        normed[rows, :] = (layer_norm(hidden[rows, :].astype(f32)) * gain_ref[...].reshape(1, feature)).astype(bf16)
        return carry

    lax.fori_loop(0, seq_span // tile, norm_rows, 0)
    masked_rows = jnp.dot(onehot_bf, normed[...], preferred_element_type=f32).astype(bf16)
    own_rows = jnp.dot(onehot_bf, hidden[...], preferred_element_type=f32)
    mixed[...] = own_rows
    cos_copy.wait()
    sin_copy.wait()
    exact = dict(preferred_element_type=f32, precision=lax.Precision.HIGHEST)
    query_cos = jnp.dot(onehot, cos[...], **exact)
    query_sin = jnp.dot(onehot, sin[...], **exact)
    lane = lax.broadcasted_iota(jnp.int32, (1, LANES), 1)
    first = lane % head_size < head_size // 2

    def rotate(inputs, cosine, sine):
        turned = jnp.where(
            first,
            pltpu.roll(inputs, LANES - head_size // 2, 1),
            pltpu.roll(inputs, head_size // 2, 1),
        )
        return inputs * cosine + turned * sine

    transposed = (((1,), (1,)), ((), ()))
    low = lane < head_size
    span = seq_span // 2 if seq_span % 32 == 0 else seq_span
    head_rows = 3 * head_size

    def attend(relation, chunk):
        weights = wbuf.at[relation, chunk]
        pairs = [
            weights[head * head_rows + head_size : (head + 1) * head_rows, :]
            for head in range(heads_in_chunk)
        ]
        pair_weights = pairs[0] if heads_in_chunk == 1 else jnp.concatenate(pairs, axis=0)

        def project(step, carry):
            rows = pl.ds(pl.multiple_of(step * span, 16), span)
            made = lax.dot_general(
                normed[rows, :], pair_weights, transposed, preferred_element_type=f32
            )
            for head in range(heads_in_chunk):
                block = made[:, head * LANES : (head + 1) * LANES]
                block = jnp.where(low, rotate(block, cos[rows, :], sin[rows, :]), block)
                pbuf[rows, head * LANES : (head + 1) * LANES] = block.astype(bf16)
            return carry

        lax.fori_loop(0, seq_span // span, project, 0)
        if heads_in_chunk == 1:
            query_weights = weights[: 2 * head_size, :]
        else:
            query_weights = jnp.concatenate(
                [weights[:head_size, :], weights[head_rows : head_rows + head_size, :]], axis=0
            )
        made = lax.dot_general(masked_rows, query_weights, transposed, preferred_element_type=f32)
        turned = rotate(made * head_size ** (-0.5), query_cos, query_sin)
        vectors = []
        for head in range(heads_in_chunk):
            query = turned if head == 0 else pltpu.roll(turned, head_size, 1)
            query = jnp.where(low, query, 0.0).astype(bf16)
            block = pbuf[:, head * LANES : (head + 1) * LANES]
            logits = lax.dot_general(query, block, transposed, preferred_element_type=f32)
            logits = jnp.where(alive, logits, -1e30)
            weight = jnp.exp(logits - jnp.max(logits, axis=-1, keepdims=True))
            probs = (weight / jnp.sum(weight, axis=-1, keepdims=True)).astype(bf16)
            vectors.append(jnp.dot(probs, block, preferred_element_type=f32))
        total = pltpu.roll(vectors[0], head_size, 1)
        if heads_in_chunk > 1:
            total = jnp.where(low, total, vectors[1])
        context[relation, chunk] = total[:, :chunk_heads].astype(bf16)

    def mix(relation):
        for chunk in range(chunks):
            rows = slice(chunk * chunk_heads, (chunk + 1) * chunk_heads)
            mixed[...] += jnp.dot(
                context[relation, chunk], obuf[relation, rows, :], preferred_element_type=f32
            )

    def fetch(*pairs):
        for pair in pairs:
            arrived(*pair)
            share(*pair)

    def attend_shared(relation, chunk):
        was_shared(relation, part(chunk, 0))
        was_shared(relation, part(chunk, 1))
        attend(relation, chunk)

    attend(0, 0)
    if routed:
        first_piece, second_piece = 2 * chunks, 2 * chunks + 1
        arrived(1, part(1, 0))
        relay(2, 1, part(1, 0))
        exchange(1, 1)
        share(1, part(1, 0))
        arrived(2, part(0, 0))
        relay(1, 2, part(0, 0))
        exchange(2, 0)
        share(2, part(0, 0))
        direct(1, part(0, 1))
        direct(2, part(1, 1))
        out_weight_copy.wait()
        direct(1, first_piece)
        direct(2, second_piece)
        direct(1, second_piece)
        direct(2, first_piece)
    for chunk in range(1, chunks):
        attend(0, chunk)
    mix(0)
    if routed:
        fetch((1, part(0, 0)), (2, part(1, 0)), (1, part(1, 1)))
        arrived(3, part(0, 0))
        exchange(3, 0)
        share(3, part(0, 0))
        arrived(3, part(1, 0))
        exchange(3, 1)
        share(3, part(1, 0))
        fetch((2, part(0, 1)))
        attend_shared(1, 1)
        attend_shared(2, 0)
        fetch((1, part(0, 1)), (2, part(1, 1)), (3, part(0, 1)))
        attend_shared(1, 0)
        arrived(1, first_piece)
        relay(2, 1, first_piece)
        share(1, first_piece)
        arrived(2, second_piece)
        relay(1, 2, second_piece)
        share(2, second_piece)
        attend_shared(2, 1)
        fetch((3, part(1, 1)))
        attend_shared(3, 0)
        fetch((1, second_piece), (2, first_piece))
        attend_shared(3, 1)
        for relation in (1, 2):
            was_shared(relation, first_piece)
            was_shared(relation, second_piece)
            mix(relation)
        fetch((3, first_piece), (3, second_piece))
        was_shared(3, first_piece)
        was_shared(3, second_piece)
        mix(3)
    else:
        for relation in range(1, n_mp):
            fetch(*[(relation, item) for item in range(items)])
        for relation in range(1, n_mp):
            for item in range(items):
                was_shared(relation, item)
            for chunk in range(chunks):
                attend(relation, chunk)
            mix(relation)

    normed_final = (layer_norm(mixed[...]) * final_gain_ref[...].reshape(1, feature)).astype(bf16)
    dense_copy.wait()
    dense_out = jnp.dot(normed_final, dense[...], preferred_element_type=f32)
    headed = layer_norm(0.5 * dense_out * (1.0 + lax.erf(dense_out * 0.5**0.5))).astype(bf16)
    logits = lax.dot_general(headed, decoder_ref[...], transposed, preferred_element_type=f32) + bias_ref[...]
    largest = jnp.max(logits, axis=-1, keepdims=True)
    scale = jnp.log(jnp.sum(jnp.exp(logits - largest), axis=-1, keepdims=True)) + largest
    vocabulary = lax.broadcasted_iota(jnp.int32, logits.shape, 1).astype(f32)
    picked = jnp.sum(jnp.where(vocabulary == targets, logits - scale, 0.0), axis=1, keepdims=True)
    row = jnp.sum(jnp.where(eye, picked, 0.0), axis=0, keepdims=True)
    padded = jnp.pad(row, ((0, 0), (0, LANES - masks)))
    scores[me] = jnp.broadcast_to(padded, scores.shape[1:])

    def score_copy(step):
        other = (me + step) % devices
        return pltpu.make_async_remote_copy(
            src_ref=scores.at[me, pl.ds(0, 1), :],
            dst_ref=scores.at[me, pl.ds(0, 1), :],
            send_sem=score_send_sem.at[step],
            recv_sem=score_sem.at[me],
            device_id=(other // n_mp, other % n_mp),
            device_id_type=MESH,
        )

    def send_scores(step, carry):
        score_copy(step).start()
        return carry

    lax.fori_loop(1, devices, send_scores, 0)
    for copy in sent:
        copy.wait_send()

    def wait_scores(step, carry):
        source = (me + step) % devices
        landing = scores.at[source, pl.ds(0, 1), :]
        pltpu.make_async_copy(landing, landing, score_sem.at[source]).wait()
        return carry

    lax.fori_loop(1, devices, wait_scores, 0)

    def wait_sends(step, carry):
        score_copy(step).wait_send()
        return carry

    lax.fori_loop(1, devices, wait_sends, 0)
    group = out_ref.shape[0]
    wanted = dp * group + lax.broadcasted_iota(jnp.int32, (group, owner_ref.shape[1]), 0)
    select = jnp.where(owner_ref[...] == wanted, 1.0, 0.0)
    out_ref[...] = jnp.dot(select, scores[:, 0, :], **exact)


FIRST_ROW = (1, 2, 4, 5, 0, 3, 0, 1)
WAIT, ROWS, QUERY = 1024, 2048, 2052
PLANS = (((133, 194, 128, 69), (79, 1058, 140, 68, 1301, 70), (2048, 142, 290),
  (131, 1061, 64, 1068, 1044, 1057, 293, 1055, 77, 108, 148, 143, 159), (),
  (98, 287, 1059, 1084, 1076, 1326, 1040, 110, 316, 134, 1047, 1043, 1056, 1071, 144, 1041, 1053, 145, 300,
   76, 151, 1062, 1046, 102, 1042, 285),
  (), (308, 2050, 1074, 99, 1072, 1060, 149, 2049, 157, 1052), (1063,), (), (1079, 1069, 1086, 284, 1078),
  (1073, 1077, 1075), (), (1087, 2051, 1054), (1085,)),
 ((129, 71, 68, 137, 135, 132), (1057, 1047, 141, 535, 73, 67), (72, 134, 65, 1044, 1065, 66, 553, 801),
  (1060, 1045, 1049, 292, 128, 537, 1063, 1043), (1064, 533, 275, 131),
  (279, 74, 103, 1041, 105, 273, 147, 807, 548, 531, 1069, 145, 1046, 1125, 1075, 1050, 2048, 1058, 1051,
   1067, 1048, 563, 1168, 1079, 1066, 2053, 106, 1056, 155, 1055, 2054, 301, 1073, 98, 1042, 1062, 530, 102),
  (), (1059,), (1080, 1071, 1054), (1580, 1084, 1083, 1082, 1081, 1072, 1077, 1053, 557, 111, 414, 2055),
  (1070,), (1076, 1074, 1078, 1085), (), (1086, 1087, 1052), ()),
 ((128, 70, 136, 68), (75, 1302, 138, 77, 74, 534, 1064, 139, 1044, 104, 143, 552, 1040, 148, 528),
  (1051, 1067, 72, 555, 1053, 134, 276, 150, 1066, 285, 78, 539, 1047), (1065, 279, 554), (1076, 1057),
  (1592, 106, 1050, 289, 151, 1071, 157, 79, 1058, 2048, 303, 155, 1062, 559, 1063, 1054, 1048, 144, 1041,
   1049, 2053, 2054, 105, 1173, 1061, 1060, 542, 1082, 286),
  (308,), (1043,), (1042, 1085, 1059, 1055, 1081, 573, 1075, 97, 1070, 1083, 2055, 1056),
  (110, 159, 1072, 1074, 1079), (), (1073, 1078, 1077), (), (1086, 1052, 1084, 1068), (1069, 1087)),
 ((131, 64, 130, 67),
  (128, 1040, 133, 76, 272, 65, 1058, 1059, 142, 1056, 99, 134, 98, 1046, 66, 141, 2048, 132, 79, 290, 1061,
   1041),
  (1052, 273), (293,), (1070, 156, 135), (101, 96, 1042, 1074, 1053, 140, 302, 291, 1043, 69, 1084, 1057),
  (1071, 150, 1044, 110, 306, 1047), (1060, 1062, 2050, 284, 97, 2049, 151), (1045, 1075, 1063), (),
  (1077, 1072, 1069, 157, 111, 316), (2051, 1055, 1079, 1078, 1073, 1076), (), (),
  (1068, 1054, 1087, 1085, 1086)))


def split_kernel(
    sizes,
    sequence_hbm,
    lengths_hbm,
    codes_hbm,
    tokens_hbm,
    owner_hbm,
    gain_hbm,
    final_gain_hbm,
    decoder_hbm,
    bias_hbm,
    hidden_hbm,
    weight_hbm,
    out_weight_hbm,
    dense_hbm,
    cos_hbm,
    sin_hbm,
    split_hbm,
    out_ref,
    sequence_ref,
    lengths_ref,
    codes_ref,
    tokens_ref,
    owner_ref,
    gain_ref,
    final_gain_ref,
    decoder_ref,
    bias_ref,
    hidden,
    normed,
    rows_buf,
    wbuf,
    raw,
    obuf,
    dense,
    cos,
    sin,
    split,
    pbuf,
    context,
    qbuf,
    gbuf,
    mixed,
    inbox,
    scores,
    local_sem,
    send_sem,
    arrive_sem,
    query_sem,
    norm_sem,
    swap_send_sem,
    swap_sem,
    score_sem,
    token_sem,
):
    n_dp, n_mp, head_size = sizes
    devices = n_dp * n_mp
    layers = n_dp // 2
    dp = lax.axis_index("dp")
    mp = lax.axis_index("mp")
    core = dp % 2
    layer = dp // 2
    partner = dp + 1 - 2 * core
    me = dp * n_mp + mp
    mate = partner * n_mp + mp
    parity = layer % 2
    pair = dp + 2 - 4 * parity
    twin = dp - 2 + 4 * parity
    middle = jnp.logical_and(layer > 0, layer < layers - 1)
    seq_span, feature = hidden.shape
    masks = codes_ref.shape[1]
    head_rows = 3 * head_size
    half_rows = head_size // 2
    where = {"x": (dp, flip(mp, 1)), "y": (dp, flip(mp, 2)), "e": (pair, mp), "m": (twin, mp), "d": (partner, mp)}

    barrier = pltpu.get_barrier_semaphore()

    def signal(semaphore, target):
        pl.semaphore_signal(semaphore, inc=1, device_id=target, device_id_type=MESH)

    for link in "dxye":
        signal(barrier, where[link])

    @pl.when(middle)
    def _():
        signal(barrier, where["m"])

    def local(index, source, target):
        copy = pltpu.make_async_copy(source, target, local_sem.at[index])
        copy.start()
        return copy

    weight_copy = local(1, weight_hbm.at[core], wbuf.at[0])
    hidden_copy = local(0, hidden_hbm, hidden)
    small_copies = [
        local(7 + place, source, target)
        for place, (source, target) in enumerate(
            (
                (sequence_hbm, sequence_ref),
                (lengths_hbm, lengths_ref),
                (codes_hbm, codes_ref),
                (tokens_hbm, tokens_ref),
                (gain_hbm, gain_ref),
            )
        )
    ]
    out_weight_copy = local(2, out_weight_hbm.at[:, pl.ds(pl.multiple_of(2 * core, 2), 2), :], raw)
    late_copies = [
        local(12 + place, source, target)
        for place, (source, target) in enumerate(
            (
                (owner_hbm, owner_ref),
                (final_gain_hbm, final_gain_ref),
                (decoder_hbm, decoder_ref),
                (bias_hbm, bias_ref),
            )
        )
    ]
    cos_copy = local(3, cos_hbm, cos)
    sin_copy = local(4, sin_hbm, sin)
    split_copy = local(6, split_hbm, split)
    dense_copy = local(5, dense_hbm, dense)

    def view(relation, item, half):
        start = FIRST_ROW[item] * head_size
        return (obuf if item > 5 else wbuf).at[relation, pl.ds(start + half * half_rows, half_rows), :]

    flips = {"x": 1, "y": 2, "e": 0, "m": 0}

    def piece_copy(relation, item, half, link, index):
        target = relation ^ flips[link]
        return pltpu.make_async_remote_copy(
            src_ref=view(relation, item, half),
            dst_ref=view(target, item, half),
            send_sem=send_sem.at[index // 12],
            recv_sem=arrive_sem.at[target - 1, 2 * item + half],
            device_id=where[link],
            device_id_type=MESH,
        )

    def rows_copy(source, target, link, index):
        return pltpu.make_async_remote_copy(
            src_ref=rows_buf.at[source],
            dst_ref=rows_buf.at[target],
            send_sem=swap_send_sem.at[index],
            recv_sem=swap_sem.at[index],
            device_id=where[link],
            device_id_type=MESH,
        )

    def query_copy(relation):
        return pltpu.make_async_remote_copy(
            src_ref=gbuf.at[relation],
            dst_ref=qbuf.at[relation],
            send_sem=query_sem.at[0, relation - 1],
            recv_sem=query_sem.at[1, relation - 1],
            device_id=where["e"],
            device_id_type=MESH,
        )

    sent = [[] for _ in range(layers)]

    def serve(words, place):
        inner = 0 < place < layers - 1
        for word in words:
            if word > QUERY:
                project_queries(word - QUERY)
            elif word > ROWS:
                query_copy(word - ROWS).wait_recv()
            elif word == ROWS and inner:
                rows_copy(0, 2, "e", 1).wait_recv()
                rows_copy(2, 3, "d", 2).start()
            elif word == ROWS:
                rows_copy(0, 2, "e", 1).start()
            else:
                relation, item, half = word // 16 % 4, word // 2 % 8, word % 2
                if word >= WAIT:
                    landing = view(relation, item, half)
                    pltpu.make_async_copy(landing, landing, arrive_sem.at[relation - 1, 2 * item + half]).wait()
                for place_of, link in enumerate("xyem"):
                    if word // 64 % 16 & (1 << place_of):
                        record = (relation, item, half, link, len(sent[place]))
                        sent[place].append(record)
                        piece_copy(*record).start()

    def service(index):
        for place in range(layers):
            if PLANS[place][index]:

                @pl.when(layer == place)
                def _():
                    serve(PLANS[place][index], place)

    weight_copy.wait()
    pl.semaphore_wait(barrier, 4 + middle.astype(jnp.int32))
    service(0)
    for copy in small_copies:
        copy.wait()
    out_weight_copy.wait()
    for head in range(2):
        obuf[0, head * head_size : (head + 1) * head_size, :] = raw[:, head, :]
    signal(token_sem.at[0], (partner, mp))

    def tokens_step(step):
        if step == 0:
            pl.semaphore_wait(token_sem.at[0], 1)
            signal(token_sem.at[1], (dp, flip(mp, 1)))
        elif step == 1:
            pl.semaphore_wait(token_sem.at[1], 1)
            signal(token_sem.at[2], (dp, flip(mp, 2)))
        else:
            hop = step - 3
            if hop < 0:
                pl.semaphore_wait(token_sem.at[2], 1)
            else:

                @pl.when(layer == hop + 1)
                def _():
                    pl.semaphore_wait(token_sem.at[3], 1)

                @pl.when(layer == layers - 2 - hop)
                def _():
                    pl.semaphore_wait(token_sem.at[4], 1)

            if hop + 1 < layers - 1:

                @pl.when(layer == hop + 1)
                def _():
                    signal(token_sem.at[3], (dp + 2, mp))

                @pl.when(layer == layers - 2 - hop)
                def _():
                    signal(token_sem.at[4], (dp - 2, mp))

    eye = lax.broadcasted_iota(jnp.int32, (masks, masks), 0) == lax.broadcasted_iota(
        jnp.int32, (masks, masks), 1
    )
    places = lax.broadcasted_iota(jnp.int32, (masks, seq_span), 1).astype(f32)

    def locate(which):
        length = lengths_ref[sequence_ref[which]].astype(f32)
        codes = codes_ref[pl.ds(which, 1), :].astype(f32)
        quotient = jnp.floor(codes / length)
        spots = codes - quotient * length
        spots = jnp.where(spots < 0.0, spots + length, spots)
        spots = jnp.where(spots >= length, spots - length, spots)
        spots = jnp.sum(jnp.where(eye, spots, 0.0), axis=1, keepdims=True)
        live = lax.broadcasted_iota(jnp.int32, (1, seq_span), 1).astype(f32) < length
        return places == spots, live

    located = [locate(which) for which in (me, mate, pair * n_mp + mp, (pair + 1 - 2 * core) * n_mp + mp)]
    chosen = located[0][0]
    alive = [live for _, live in located]
    tokens = tokens_ref[pl.ds(sequence_ref[me], 1), :].astype(f32)
    targets = jnp.sum(jnp.where(chosen, tokens, 0.0), axis=1, keepdims=True)
    onehots = [jnp.where(spots, 1.0, 0.0).astype(bf16) for spots, _ in located]
    onehot = onehots[0]

    hidden_copy.wait()
    tile = 128

    norm_copy = pltpu.make_async_remote_copy(
        src_ref=normed.at[0],
        dst_ref=normed.at[1],
        send_sem=norm_sem.at[0],
        recv_sem=norm_sem.at[1],
        device_id=(partner, mp),
        device_id_type=MESH,
    )

    def norm_rows(step, carry):
        rows = pl.ds(pl.multiple_of(step * tile, tile), tile)
        normed[0, rows, :] = (layer_norm(hidden[rows, :].astype(f32)) * gain_ref[...].reshape(1, feature)).astype(bf16)
        return carry

    lax.fori_loop(0, seq_span // tile, norm_rows, 0)
    rows_buf[0] = jnp.dot(onehot, normed[0], preferred_element_type=f32).astype(bf16)
    norm_copy.start()
    mixed[:masks, :] = jnp.dot(onehot, hidden[...], preferred_element_type=f32)
    mixed[masks:, :] = jnp.zeros((masks, feature), f32)
    rows_copy(0, 1, "d", 0).start()
    split_copy.wait()
    table = jnp.dot(jnp.concatenate(onehots, axis=0), split[...], preferred_element_type=f32)
    query_cos = table[:, :LANES] + table[:, LANES : 2 * LANES]
    query_sin = table[:, 2 * LANES : 3 * LANES] + table[:, 3 * LANES :]
    lane = lax.broadcasted_iota(jnp.int32, (1, LANES), 1)
    first = lane % head_size < head_size // 2
    low = lane < head_size
    transposed = (((1,), (1,)), ((), ()))

    def rotate(inputs, cosine, sine):
        turned = jnp.where(
            first,
            pltpu.roll(inputs, LANES - head_size // 2, 1),
            pltpu.roll(inputs, head_size // 2, 1),
        )
        return inputs * cosine + turned * sine

    span = seq_span

    def stack(refs):
        return jnp.concatenate([ref[...] for ref in refs], axis=0)

    def rows_of(start, count):
        return pl.ds(start if isinstance(start, int) else pl.multiple_of(start, head_size), count)

    def project(unit, buffer, slot):
        keys = stack(
            [wbuf.at[relation, rows_of(head * head_rows + head_size, 2 * head_size), :] for relation, head in unit]
        )

        def step_of(step, carry):
            rows = pl.ds(pl.multiple_of(step * span, 16), span)
            made = lax.dot_general(normed[slot, rows, :], keys, transposed, preferred_element_type=f32)
            for head in range(2):
                block = made[:, head * LANES : (head + 1) * LANES]
                block = jnp.where(low, rotate(block, cos[rows, :], sin[rows, :]), block)
                pbuf[buffer, slot, rows, head * LANES : (head + 1) * LANES] = block.astype(bf16)
            return carry

        lax.fori_loop(0, seq_span // span, step_of, 0)

    def queries(relation, low_slot, high_slot):
        weights = stack([wbuf.at[relation, head * head_rows : head * head_rows + head_size, :] for head in range(2)])
        rows = slice(low_slot * masks, high_slot * masks)
        source = rows_buf[low_slot:high_slot].reshape((high_slot - low_slot) * masks, feature)
        made = lax.dot_general(source, weights, transposed, preferred_element_type=f32)
        return rotate(made * head_size ** (-0.5), query_cos[rows], query_sin[rows]).astype(bf16)

    def project_queries(relation):
        if relation == 1:
            rows_copy(2, 3, "d", 2).wait_recv()
        made = queries(relation, 0, 4)
        gbuf[relation] = made[2 * masks :]
        qbuf[relation] = made[: 2 * masks]
        query_copy(relation).start()

    def of_head(query, head):
        query = query.astype(f32)
        if isinstance(head, int):
            return pltpu.roll(query, head_size, 1) if head else query
        return jnp.where(head == 1, pltpu.roll(query, head_size, 1), query)

    def attend(which, buffer, slot, near, far):
        empty = jnp.zeros((masks, LANES), bf16)
        near = jnp.where(low, near, 0.0).astype(bf16)
        far = jnp.where(low, far, 0.0).astype(bf16)
        both = jnp.concatenate(
            [jnp.concatenate([near, empty], axis=1), jnp.concatenate([empty, far], axis=1)], axis=0
        )
        block = pbuf[buffer, slot]
        logits = lax.dot_general(both, block, transposed, preferred_element_type=f32)
        logits = jnp.where(alive[slot], logits, -1e30)
        weight = jnp.exp(logits - jnp.max(logits, axis=-1, keepdims=True))
        probs = (weight / jnp.sum(weight, axis=-1, keepdims=True)).astype(bf16)
        vectors = jnp.dot(probs, block, preferred_element_type=f32)
        total = jnp.where(low, pltpu.roll(vectors[:masks, :LANES], head_size, 1), vectors[masks:, LANES:])
        context[slot * masks : (slot + 1) * masks, which * LANES : (which + 1) * LANES] = total.astype(bf16)

    def attend_both(which, unit, buffer):
        for slot in range(2):
            rows = slice(slot * masks, (slot + 1) * masks)
            near, far = [of_head(qbuf[relation, rows, :], head) for relation, head in unit]
            attend(which, buffer, slot, near, far)

    def mix(low_unit, *units):
        out_weights = stack([obuf.at[relation, rows_of(head * head_size, head_size), :] for unit in units for relation, head in unit])
        lanes = slice(low_unit * LANES, (low_unit + len(units)) * LANES)
        mixed[...] += jnp.dot(context[:, lanes], out_weights, preferred_element_type=f32)

    early = middle.astype(jnp.int32)
    own = ((0, 0), (0, 1))
    firsts = ((1, early), (2, early))
    seconds = ((1, 1 - early), (2, 1 - early))
    across = ((3, 0), (3, 1))

    cos_copy.wait()
    sin_copy.wait()
    service(1)
    project(own, 0, 0)
    service(2)
    query = queries(0, 0, 1)
    attend(0, 0, 0, of_head(query, 0), of_head(query, 1))
    tokens_step(0)
    service(3)
    norm_copy.wait_recv()
    rows_copy(0, 1, "d", 0).wait_recv()
    project(own, 0, 1)
    service(4)
    query = queries(0, 1, 2)
    attend(0, 0, 1, of_head(query, 0), of_head(query, 1))
    mix(0, own)
    tokens_step(1)
    service(5)
    project(firsts, 1, 0)
    service(6)
    project(firsts, 1, 1)
    tokens_step(2)
    service(7)
    attend_both(1, firsts, 1)
    tokens_step(3)
    service(8)
    project(seconds, 0, 0)
    service(9)
    project(seconds, 0, 1)
    service(10)
    attend_both(2, seconds, 0)
    tokens_step(4)
    service(11)
    project(across, 1, 0)
    service(12)
    project(across, 1, 1)
    service(13)
    attend_both(3, across, 1)
    tokens_step(5)
    service(14)
    mix(1, firsts, seconds, across)
    inbox_copy = pltpu.make_async_remote_copy(
        src_ref=mixed.at[pl.ds(masks, masks), :],
        dst_ref=inbox,
        send_sem=swap_send_sem.at[3],
        recv_sem=swap_sem.at[3],
        device_id=(partner, mp),
        device_id_type=MESH,
    )
    inbox_copy.start()
    dense_copy.wait()
    for copy in late_copies:
        copy.wait()
    inbox_copy.wait_recv()
    residual = mixed[:masks, :] + inbox[...]
    normed_final = (layer_norm(residual) * final_gain_ref[...].reshape(1, feature)).astype(bf16)
    dense_out = jnp.dot(normed_final, dense[...], preferred_element_type=f32)
    headed = layer_norm(0.5 * dense_out * (1.0 + lax.erf(dense_out * 0.5**0.5))).astype(bf16)
    logits = lax.dot_general(headed, decoder_ref[...], transposed, preferred_element_type=f32) + bias_ref[...]
    largest = jnp.max(logits, axis=-1, keepdims=True)
    scale = jnp.log(jnp.sum(jnp.exp(logits - largest), axis=-1, keepdims=True)) + largest
    vocabulary = lax.broadcasted_iota(jnp.int32, logits.shape, 1).astype(f32)
    picked = jnp.sum(jnp.where(vocabulary == targets, logits - scale, 0.0), axis=1, keepdims=True)
    row = jnp.sum(jnp.where(eye, picked, 0.0), axis=0, keepdims=True)
    padded = jnp.concatenate([row] * (LANES // masks), axis=1)
    scores[me] = padded

    def score_copy(step):
        other_dp, other_mp = flip(dp, step // n_mp), flip(mp, step % n_mp)
        return pltpu.make_async_remote_copy(
            src_ref=scores.at[me],
            dst_ref=scores.at[me],
            send_sem=score_sem.at[0],
            recv_sem=score_sem.at[1],
            device_id=(other_dp, other_mp),
            device_id_type=MESH,
        )

    for step in reversed(range(1, devices)):
        score_copy(step).start()
    inbox_copy.wait_send()
    norm_copy.wait_send()
    rows_copy(0, 1, "d", 0).wait_send()

    for place in range(layers):

        @pl.when(layer == place)
        def _():
            for group in range(0, len(sent[place]), 12):
                count = min(12, len(sent[place]) - group)
                bulk = wbuf.at[0, pl.ds(0, count * half_rows), :]
                pltpu.make_async_copy(bulk, bulk, send_sem.at[group // 12]).wait()
            if 0 < place < layers - 1:
                rows_copy(2, 3, "d", 2).wait_send()
                for relation in (1, 2, 3):
                    query_copy(relation).wait_send()
            else:
                rows_copy(0, 2, "e", 1).wait_send()

    group = out_ref.shape[0]
    square = lax.broadcasted_iota(jnp.int32, (devices, devices), 0) == lax.broadcasted_iota(
        jnp.int32, (devices, devices), 1
    )
    owners = jnp.sum(jnp.where(square, owner_ref[...].astype(f32), 0.0), axis=1, keepdims=True)
    selects = [jnp.where(owners == (dp * group + place).astype(f32), 1.0, 0.0) for place in range(group)]
    everyone = scores.at[pl.ds(0, devices - 1)]
    pltpu.make_async_copy(everyone, everyone, score_sem.at[1]).wait()
    pltpu.make_async_copy(everyone, everyone, score_sem.at[0]).wait()
    gathered = scores[...].reshape(devices, LANES)
    result = jnp.concatenate([jnp.sum(gathered * select, axis=0, keepdims=True) for select in selects], axis=0)
    out_ref[...] = pltpu.roll(result, LANES - mp * out_ref.shape[1], 1)[:, : out_ref.shape[1]]


def split_call(shape, inputs, weight, out_weight, hidden, dense_weight, cosine, sine, group, head_size):
    n_dp, n_mp = shape
    devices = n_dp * n_mp
    seq_span, feature = hidden.shape
    width = weight.shape[1]
    masks = inputs[2].shape[1]
    high = [t.astype(jnp.bfloat16).astype(np.float32) for t in (cosine, sine)]
    parts = [high[0], cosine - high[0], high[1], sine - high[1]]
    split = np.concatenate(parts, axis=1).astype(jnp.bfloat16)
    dma = pltpu.SemaphoreType.DMA
    vmem = pl.BlockSpec(memory_space=pltpu.VMEM)
    anywhere = pl.BlockSpec(memory_space=pl.ANY)
    return pl.pallas_call(
        functools.partial(split_kernel, (n_dp, n_mp, head_size)),
        name="score_split",
        out_shape=jax.ShapeDtypeStruct((group, masks // n_mp), f32),
        in_specs=[anywhere] * 16,
        out_specs=vmem,
        scratch_shapes=[(pltpu.SMEM if place < 2 else pltpu.VMEM)(x.shape, x.dtype) for place, x in enumerate(inputs)]
        + [
            pltpu.VMEM((seq_span, feature), bf16),
            pltpu.VMEM((2, seq_span, feature), bf16),
            pltpu.VMEM((4, masks, feature), bf16),
            pltpu.VMEM((n_mp, width, feature), bf16),
            pltpu.VMEM((head_size, 2, feature), bf16),
            pltpu.VMEM((n_mp, 2 * head_size, feature), bf16),
            pltpu.VMEM((feature, feature), bf16),
            pltpu.VMEM((seq_span, LANES), f32),
            pltpu.VMEM((seq_span, LANES), f32),
            pltpu.VMEM((seq_span, 4 * LANES), bf16),
            pltpu.VMEM((2, 2, seq_span, 2 * LANES), bf16),
            pltpu.VMEM((2 * masks, 4 * LANES), bf16),
            pltpu.VMEM((n_mp, 2 * masks, LANES), bf16),
            pltpu.VMEM((n_mp, 2 * masks, LANES), bf16),
            pltpu.VMEM((2 * masks, feature), f32),
            pltpu.VMEM((masks, feature), f32),
            pltpu.VMEM((devices, 1, LANES), f32),
            dma((16,)),
            dma((6,)),
            dma((n_mp - 1, 16)),
            dma((2, n_mp - 1)),
            dma((2,)),
            dma((4,)),
            dma((4,)),
            dma((2,)),
            pltpu.SemaphoreType.REGULAR((5,)),
        ],
        compiler_params=pltpu.CompilerParams(collective_id=1, has_side_effects=True),
    )(
        *inputs,
        hidden,
        weight,
        out_weight,
        dense_weight,
        jnp.asarray(cosine),
        jnp.asarray(sine),
        jnp.asarray(split),
    )


def on_device(
    shape,
    hidden_states,
    ln_attn_gain,
    w_qkv,
    output_weight,
    ln_final_gain,
    dense_weight,
    decoder_weight,
    decoder_bias,
    seq_tokens,
    seq_lengths,
    copy_sequence,
    mask_code,
    copy_owner,
):
    n_dp, n_mp = shape
    devices = n_dp * n_mp
    lane_copies, seq_span, feature = hidden_states.shape
    head_size, heads, _ = output_weight.shape
    copies, masks = mask_code.shape
    assert lane_copies == 1 and copies == devices and n_dp % 2 == 0
    assert 2 * head_size == LANES and masks <= LANES
    in_chunk = 2 if heads % 2 == 0 else 1
    chunks = heads // in_chunk
    width = in_chunk * 3 * head_size
    weight = jnp.transpose(w_qkv.reshape(feature, chunks, width), (1, 2, 0))
    cosine, sine = rotary_tables(seq_span, head_size)
    group = copies // n_dp
    items = 2 * chunks + 2
    dma = pltpu.SemaphoreType.DMA
    vmem = pl.BlockSpec(memory_space=pltpu.VMEM)
    smem = pl.BlockSpec(memory_space=pltpu.SMEM)
    anywhere = pl.BlockSpec(memory_space=pl.ANY)
    own = masks // n_mp
    inputs = (
        copy_sequence,
        seq_lengths,
        mask_code,
        seq_tokens,
        copy_owner.reshape(1, -1),
        ln_attn_gain,
        ln_final_gain,
        decoder_weight.T,
        decoder_bias.reshape(1, -1),
    )
    if n_mp == 4 and n_dp == 8 and heads == 4 and seq_span % 128 == 0:
        hidden = hidden_states.reshape(seq_span, feature)
        return split_call(shape, inputs, weight, output_weight, hidden, dense_weight, cosine, sine, group, head_size)
    out_weight = jnp.swapaxes(output_weight, 0, 1).reshape(heads * head_size, feature)
    rows = pl.pallas_call(
        functools.partial(kernel, (n_dp, n_mp, head_size, in_chunk, chunks)),
        name="score_copies",
        out_shape=jax.ShapeDtypeStruct((group, LANES), f32),
        in_specs=[smem] * 2 + [vmem] * 7 + [anywhere] * 6,
        out_specs=vmem,
        scratch_shapes=[
            pltpu.VMEM((seq_span, feature), bf16),
            pltpu.VMEM((seq_span, feature), bf16),
            pltpu.VMEM((n_mp, chunks, width, feature), bf16),
            pltpu.VMEM((n_mp, heads * head_size, feature), bf16),
            pltpu.VMEM((feature, feature), bf16),
            pltpu.VMEM((seq_span, LANES), f32),
            pltpu.VMEM((seq_span, LANES), f32),
            pltpu.VMEM((seq_span, in_chunk * LANES), bf16),
            pltpu.VMEM((n_mp, chunks, masks, in_chunk * head_size), bf16),
            pltpu.VMEM((masks, feature), f32),
            pltpu.VMEM((devices, 8, LANES), f32),
            dma((6,)),
            dma((n_mp, items)),
            dma((items,)),
            dma((n_mp, chunks)),
            dma((n_mp, items)),
            dma((n_mp, items)),
            dma((n_mp, items)),
            dma((devices,)),
            dma((devices,)),
        ],
        compiler_params=pltpu.CompilerParams(collective_id=0, has_side_effects=True),
    )(
        copy_sequence,
        seq_lengths,
        mask_code,
        seq_tokens,
        copy_owner.reshape(1, -1),
        ln_attn_gain,
        ln_final_gain,
        decoder_weight.T,
        decoder_bias.reshape(1, -1),
        hidden_states.reshape(seq_span, feature),
        weight,
        out_weight,
        dense_weight,
        jnp.asarray(cosine),
        jnp.asarray(sine),
    )
    return lax.dynamic_slice_in_dim(rows, lax.axis_index("mp") * own, own, 1)


def solution(mesh):
    placed = (
        P(("dp", "mp"), None, None),
        P(),
        P(None, "mp", None),
        P(None, "mp", None),
        P(),
        P(),
        P(),
        P(),
        P(),
        P(),
        P(),
        P(),
        P(),
    )
    shape = (mesh.shape["dp"], mesh.shape["mp"])
    return jax.shard_map(
        functools.partial(on_device, shape),
        mesh=mesh,
        in_specs=placed,
        out_specs=P("dp", "mp"),
        check_vma=False,
    )
```

```python
import functools

import jax
import jax.numpy as jnp
import numpy as np
from jax import lax
from jax.experimental import pallas as pl
from jax.experimental.pallas import tpu as pltpu
from jax.sharding import PartitionSpec as P

epsilon = 1e-05
MESH = pl.DeviceIdType.MESH
f32 = jnp.float32
bf16 = jnp.bfloat16
LANES = 128


def layer_norm(inputs):
    average = jnp.mean(inputs, axis=-1, keepdims=True)
    centred = inputs - average
    variance = jnp.mean(centred * centred, axis=-1, keepdims=True)
    return centred * lax.rsqrt(variance + epsilon)


def rotary_tables(seq_span, head_size):
    half = head_size // 2
    frequency = (1.0 / 10000.0 ** (np.arange(half, dtype=np.float32) * (2.0 / head_size))).astype(
        np.float32
    )
    angles = np.arange(seq_span, dtype=np.float32)[:, None] * frequency[None, :]
    cosine, sine = np.cos(angles), np.sin(angles)
    times = LANES // head_size
    return (
        np.tile(np.concatenate([cosine, cosine], axis=1), (1, times)).astype(np.float32),
        np.tile(np.concatenate([-sine, sine], axis=1), (1, times)).astype(np.float32),
    )


def flip(index, mask):
    bit = 1
    out = index
    while bit <= mask:
        if mask & bit:
            out = out + bit * (1 - 2 * ((index // bit) % 2))
        bit *= 2
    return out


def kernel(
    sizes,
    sequence_ref,
    lengths_ref,
    codes_ref,
    tokens_ref,
    owner_ref,
    gain_ref,
    final_gain_ref,
    decoder_ref,
    bias_ref,
    hidden_hbm,
    weight_hbm,
    out_weight_hbm,
    dense_hbm,
    cos_hbm,
    sin_hbm,
    out_ref,
    hidden,
    normed,
    wbuf,
    obuf,
    dense,
    cos,
    sin,
    pbuf,
    context,
    mixed,
    scores,
    local_sem,
    direct_sem,
    relay_sem,
    exchange_sem,
    share_sem,
    arrive_sem,
    shared_sem,
    score_send_sem,
    score_sem,
):
    n_dp, n_mp, head_size, heads_in_chunk, chunks = sizes
    devices = n_dp * n_mp
    dp = lax.axis_index("dp")
    mp = lax.axis_index("mp")
    core = dp % 2
    partner = dp + 1 - 2 * core
    me = dp * n_mp + mp
    seq_span, feature = hidden.shape
    masks = codes_ref.shape[1]
    chunk_heads = heads_in_chunk * head_size
    out_rows = obuf.shape[1]
    piece_rows = out_rows // 4

    def local(index, source, target):
        copy = pltpu.make_async_copy(source, target, local_sem.at[index])
        copy.start()
        return copy

    weight_copy = local(1, weight_hbm, wbuf.at[0])
    hidden_copy = local(0, hidden_hbm, hidden)

    barrier = pltpu.get_barrier_semaphore()

    def greet(step, carry):
        other = (me + step) % devices
        pl.semaphore_signal(
            barrier, inc=1, device_id=(other // n_mp, other % n_mp), device_id_type=MESH
        )
        return carry

    lax.fori_loop(1, devices, greet, 0)

    parity = (dp // 2) % 2
    above = dp + 2 - 4 * parity
    part_rows = wbuf.shape[2] // 4

    def part(chunk, odd):
        return 2 * chunk + odd

    def place(relation, item, half):
        if item < 2 * chunks:
            chunk, odd = divmod(item, 2)
            which = 1 - parity if odd else parity
            start = (2 * half + which) * part_rows
            return wbuf.at[relation, chunk, pl.ds(pl.multiple_of(start, 16), part_rows), :]
        start = (2 * half + item - 2 * chunks) * piece_rows
        return obuf.at[relation, pl.ds(pl.multiple_of(start, 16), piece_rows), :]

    def view(relation, item):
        return place(relation, item, core)

    def partner_view(relation, item):
        return place(relation, item, 1 - core)

    sent = []

    def to_group(target, source_relation, relation, item, semaphore):
        copy = pltpu.make_async_remote_copy(
            src_ref=view(source_relation, item),
            dst_ref=view(relation, item),
            send_sem=semaphore,
            recv_sem=arrive_sem.at[relation, item],
            device_id=(dp, flip(mp, target)),
            device_id_type=MESH,
        )
        copy.start()
        sent.append(copy)

    def direct(target, item):
        to_group(target, 0, target, item, direct_sem.at[target, item])

    def relay(target, source_relation, item):
        to_group(target, source_relation, source_relation ^ target, item, relay_sem.at[item])

    def exchange(relation, chunk):
        copy = pltpu.make_async_remote_copy(
            src_ref=view(relation, part(chunk, 0)),
            dst_ref=view(relation, part(chunk, 0)),
            send_sem=exchange_sem.at[relation, chunk],
            recv_sem=arrive_sem.at[relation, part(chunk, 1)],
            device_id=(above, mp),
            device_id_type=MESH,
        )
        copy.start()
        sent.append(copy)

    def arrived(relation, item):
        landing = view(relation, item)
        pltpu.make_async_copy(landing, landing, arrive_sem.at[relation, item]).wait()

    def share(relation, item):
        copy = pltpu.make_async_remote_copy(
            src_ref=view(relation, item),
            dst_ref=view(relation, item),
            send_sem=share_sem.at[relation, item],
            recv_sem=shared_sem.at[relation, item],
            device_id=(partner, mp),
            device_id_type=MESH,
        )
        copy.start()
        sent.append(copy)

    def was_shared(relation, item):
        landing = partner_view(relation, item)
        pltpu.make_async_copy(landing, landing, shared_sem.at[relation, item]).wait()

    sequence = sequence_ref[me]
    length = lengths_ref[sequence].astype(f32)
    codes = codes_ref[pl.ds(me, 1), :].astype(f32)
    quotient = jnp.floor(codes / length)
    row_positions = codes - quotient * length
    row_positions = jnp.where(row_positions < 0.0, row_positions + length, row_positions)
    row_positions = jnp.where(row_positions >= length, row_positions - length, row_positions)
    eye = lax.broadcasted_iota(jnp.int32, (masks, masks), 0) == lax.broadcasted_iota(
        jnp.int32, (masks, masks), 1
    )
    positions = jnp.sum(jnp.where(eye, row_positions, 0.0), axis=1, keepdims=True)
    places = lax.broadcasted_iota(jnp.int32, (masks, seq_span), 1).astype(f32)
    chosen = places == positions
    onehot = jnp.where(chosen, 1.0, 0.0)
    onehot_bf = onehot.astype(bf16)
    tokens = tokens_ref[pl.ds(sequence, 1), :].astype(f32)
    targets = jnp.sum(jnp.where(chosen, tokens, 0.0), axis=1, keepdims=True)
    alive = lax.broadcasted_iota(jnp.int32, (1, seq_span), 1).astype(f32) < length

    weight_copy.wait()
    pl.semaphore_wait(barrier, devices - 1)
    items = 2 * chunks + 2
    routed = n_mp == 4 and chunks == 2 and n_dp % 4 == 0
    if routed:
        direct(1, part(1, 0))
        direct(2, part(0, 0))
        direct(1, part(0, 0))
        direct(2, part(1, 0))
    cos_copy = local(3, cos_hbm, cos)
    sin_copy = local(4, sin_hbm, sin)
    out_weight_copy = local(2, out_weight_hbm, obuf.at[0])
    dense_copy = local(5, dense_hbm, dense)
    if not routed:
        out_weight_copy.wait()
        for item in range(items):
            for target in range(1, n_mp):
                direct(target, item)

    hidden_copy.wait()
    tile = 128 if seq_span % 128 == 0 else 8

    def norm_rows(step, carry):
        rows = pl.ds(pl.multiple_of(step * tile, tile), tile)
        normed[rows, :] = (layer_norm(hidden[rows, :].astype(f32)) * gain_ref[...].reshape(1, feature)).astype(bf16)
        return carry

    lax.fori_loop(0, seq_span // tile, norm_rows, 0)
    masked_rows = jnp.dot(onehot_bf, normed[...], preferred_element_type=f32).astype(bf16)
    own_rows = jnp.dot(onehot_bf, hidden[...], preferred_element_type=f32)
    mixed[...] = own_rows
    cos_copy.wait()
    sin_copy.wait()
    exact = dict(preferred_element_type=f32, precision=lax.Precision.HIGHEST)
    query_cos = jnp.dot(onehot, cos[...], **exact)
    query_sin = jnp.dot(onehot, sin[...], **exact)
    lane = lax.broadcasted_iota(jnp.int32, (1, LANES), 1)
    first = lane % head_size < head_size // 2

    def rotate(inputs, cosine, sine):
        turned = jnp.where(
            first,
            pltpu.roll(inputs, LANES - head_size // 2, 1),
            pltpu.roll(inputs, head_size // 2, 1),
        )
        return inputs * cosine + turned * sine

    transposed = (((1,), (1,)), ((), ()))
    low = lane < head_size
    span = seq_span // 2 if seq_span % 32 == 0 else seq_span
    head_rows = 3 * head_size

    def attend(relation, chunk):
        weights = wbuf.at[relation, chunk]
        pairs = [
            weights[head * head_rows + head_size : (head + 1) * head_rows, :]
            for head in range(heads_in_chunk)
        ]
        pair_weights = pairs[0] if heads_in_chunk == 1 else jnp.concatenate(pairs, axis=0)

        def project(step, carry):
            rows = pl.ds(pl.multiple_of(step * span, 16), span)
            made = lax.dot_general(
                normed[rows, :], pair_weights, transposed, preferred_element_type=f32
            )
            for head in range(heads_in_chunk):
                block = made[:, head * LANES : (head + 1) * LANES]
                block = jnp.where(low, rotate(block, cos[rows, :], sin[rows, :]), block)
                pbuf[rows, head * LANES : (head + 1) * LANES] = block.astype(bf16)
            return carry

        lax.fori_loop(0, seq_span // span, project, 0)
        if heads_in_chunk == 1:
            query_weights = weights[: 2 * head_size, :]
        else:
            query_weights = jnp.concatenate(
                [weights[:head_size, :], weights[head_rows : head_rows + head_size, :]], axis=0
            )
        made = lax.dot_general(masked_rows, query_weights, transposed, preferred_element_type=f32)
        turned = rotate(made * head_size ** (-0.5), query_cos, query_sin)
        vectors = []
        for head in range(heads_in_chunk):
            query = turned if head == 0 else pltpu.roll(turned, head_size, 1)
            query = jnp.where(low, query, 0.0).astype(bf16)
            block = pbuf[:, head * LANES : (head + 1) * LANES]
            logits = lax.dot_general(query, block, transposed, preferred_element_type=f32)
            logits = jnp.where(alive, logits, -1e30)
            weight = jnp.exp(logits - jnp.max(logits, axis=-1, keepdims=True))
            probs = (weight / jnp.sum(weight, axis=-1, keepdims=True)).astype(bf16)
            vectors.append(jnp.dot(probs, block, preferred_element_type=f32))
        total = pltpu.roll(vectors[0], head_size, 1)
        if heads_in_chunk > 1:
            total = jnp.where(low, total, vectors[1])
        context[relation, chunk] = total[:, :chunk_heads].astype(bf16)

    def mix(relation):
        for chunk in range(chunks):
            rows = slice(chunk * chunk_heads, (chunk + 1) * chunk_heads)
            mixed[...] += jnp.dot(
                context[relation, chunk], obuf[relation, rows, :], preferred_element_type=f32
            )

    def fetch(*pairs):
        for pair in pairs:
            arrived(*pair)
            share(*pair)

    def attend_shared(relation, chunk):
        was_shared(relation, part(chunk, 0))
        was_shared(relation, part(chunk, 1))
        attend(relation, chunk)

    attend(0, 0)
    if routed:
        first_piece, second_piece = 2 * chunks, 2 * chunks + 1
        arrived(1, part(1, 0))
        relay(2, 1, part(1, 0))
        exchange(1, 1)
        share(1, part(1, 0))
        arrived(2, part(0, 0))
        relay(1, 2, part(0, 0))
        exchange(2, 0)
        share(2, part(0, 0))
        direct(1, part(0, 1))
        direct(2, part(1, 1))
        out_weight_copy.wait()
        direct(1, first_piece)
        direct(2, second_piece)
        direct(1, second_piece)
        direct(2, first_piece)
    for chunk in range(1, chunks):
        attend(0, chunk)
    mix(0)
    if routed:
        fetch((1, part(0, 0)), (2, part(1, 0)), (1, part(1, 1)))
        arrived(3, part(0, 0))
        exchange(3, 0)
        share(3, part(0, 0))
        arrived(3, part(1, 0))
        exchange(3, 1)
        share(3, part(1, 0))
        fetch((2, part(0, 1)))
        attend_shared(1, 1)
        attend_shared(2, 0)
        fetch((1, part(0, 1)), (2, part(1, 1)), (3, part(0, 1)))
        attend_shared(1, 0)
        arrived(1, first_piece)
        relay(2, 1, first_piece)
        share(1, first_piece)
        arrived(2, second_piece)
        relay(1, 2, second_piece)
        share(2, second_piece)
        attend_shared(2, 1)
        fetch((3, part(1, 1)))
        attend_shared(3, 0)
        fetch((1, second_piece), (2, first_piece))
        attend_shared(3, 1)
        for relation in (1, 2):
            was_shared(relation, first_piece)
            was_shared(relation, second_piece)
            mix(relation)
        fetch((3, first_piece), (3, second_piece))
        was_shared(3, first_piece)
        was_shared(3, second_piece)
        mix(3)
    else:
        for relation in range(1, n_mp):
            fetch(*[(relation, item) for item in range(items)])
        for relation in range(1, n_mp):
            for item in range(items):
                was_shared(relation, item)
            for chunk in range(chunks):
                attend(relation, chunk)
            mix(relation)

    normed_final = (layer_norm(mixed[...]) * final_gain_ref[...].reshape(1, feature)).astype(bf16)
    dense_copy.wait()
    dense_out = jnp.dot(normed_final, dense[...], preferred_element_type=f32)
    headed = layer_norm(0.5 * dense_out * (1.0 + lax.erf(dense_out * 0.5**0.5))).astype(bf16)
    logits = lax.dot_general(headed, decoder_ref[...], transposed, preferred_element_type=f32) + bias_ref[...]
    largest = jnp.max(logits, axis=-1, keepdims=True)
    scale = jnp.log(jnp.sum(jnp.exp(logits - largest), axis=-1, keepdims=True)) + largest
    vocabulary = lax.broadcasted_iota(jnp.int32, logits.shape, 1).astype(f32)
    picked = jnp.sum(jnp.where(vocabulary == targets, logits - scale, 0.0), axis=1, keepdims=True)
    row = jnp.sum(jnp.where(eye, picked, 0.0), axis=0, keepdims=True)
    padded = jnp.pad(row, ((0, 0), (0, LANES - masks)))
    scores[me] = jnp.broadcast_to(padded, scores.shape[1:])

    def score_copy(step):
        other = (me + step) % devices
        return pltpu.make_async_remote_copy(
            src_ref=scores.at[me, pl.ds(0, 1), :],
            dst_ref=scores.at[me, pl.ds(0, 1), :],
            send_sem=score_send_sem.at[step],
            recv_sem=score_sem.at[me],
            device_id=(other // n_mp, other % n_mp),
            device_id_type=MESH,
        )

    def send_scores(step, carry):
        score_copy(step).start()
        return carry

    lax.fori_loop(1, devices, send_scores, 0)
    for copy in sent:
        copy.wait_send()

    def wait_scores(step, carry):
        source = (me + step) % devices
        landing = scores.at[source, pl.ds(0, 1), :]
        pltpu.make_async_copy(landing, landing, score_sem.at[source]).wait()
        return carry

    lax.fori_loop(1, devices, wait_scores, 0)

    def wait_sends(step, carry):
        score_copy(step).wait_send()
        return carry

    lax.fori_loop(1, devices, wait_sends, 0)
    group = out_ref.shape[0]
    wanted = dp * group + lax.broadcasted_iota(jnp.int32, (group, owner_ref.shape[1]), 0)
    select = jnp.where(owner_ref[...] == wanted, 1.0, 0.0)
    out_ref[...] = jnp.dot(select, scores[:, 0, :], **exact)


FIRST_ROW = (1, 2, 4, 5, 0, 3, 0, 1)
WAIT, ROWS, QUERY = 1024, 2048, 2052
PLANS = (((128, 70, 131, 69), (194, 143, 76, 2048, 1315, 1045, 67, 135), (142, 65),
  (1046, 134, 1314, 1043, 98, 1071, 149, 1042, 99, 303, 1056), (406, 78),
  (1052, 1063, 1041, 1134, 156, 1060, 1044, 273, 1040, 275, 1057, 133),
  (111, 144, 1062, 1330, 1047, 103, 79, 1333), (2049, 140, 2050), (1054, 1084, 141, 1061, 1078, 77, 1075), (),
  (1079, 1073, 1342), (1076, 1068, 1072), (), (1085, 1053, 2051, 1087, 1069, 1055), ()),
 ((132, 64, 68, 202, 139), (), (1060, 71, 141, 66, 548, 135, 1040, 140, 272, 69, 292, 73, 1300, 532),
  (1066, 1579, 1057, 1048, 1559, 554, 528, 1069, 353, 152, 134),
  (1045, 1058, 279, 109, 136, 1080, 148, 568, 106, 1071),
  (1049, 1061, 1050, 1063, 1132, 78, 1062, 1051, 1073, 2048, 556, 1046, 1065, 305, 557, 105, 561, 155, 2053),
  (1064, 2054, 151, 76), (77, 1076, 1056, 1043), (1085, 147, 1041, 308, 1059, 1042), (1082,), (1083, 317),
  (1054, 1084, 1081, 559, 142, 1077, 1079, 1075, 1078, 1074, 1072, 2055), (), (),
  (1053, 1087, 1052, 1070, 1055, 1086)),
 ((72, 129, 74, 133, 75, 137, 1048, 69, 1057, 65, 135, 536, 134, 801),
  (1050, 1051, 1061, 73, 1065, 805, 131, 553, 539, 1056, 79, 1045, 142, 277), (136, 155, 1297, 1044, 1062),
  (1060, 102, 544, 1049, 1063, 96, 153, 2048, 276, 292), (100,),
  (1047, 1067, 1070, 2053, 1066, 1055, 1042, 1064, 110, 1046, 2054),
  (1083, 302, 1059, 106, 1040, 99, 1058, 159), (1078, 1072, 566, 1076, 287, 1080, 308, 1043, 149), (560,),
  (1087,), (1069, 543, 1082, 109),
  (1081, 1052, 1086, 1074, 1077, 2055, 1068, 156, 575, 1079, 300, 1053, 1075, 1073), (), (1085,),
  (1054, 1071, 1084)),
 ((66, 70, 128, 130), (199, 143, 131, 1056, 1042, 288, 67, 76, 146, 77, 2048, 1058, 141, 1046, 1047),
  (64, 274, 278, 1057, 290), (1043,), (150, 151, 134, 1061, 1063, 275, 78, 1059, 1074),
  (97, 306, 99, 1180, 1045, 284, 1040, 1053, 101, 144, 1041),
  (1135, 1079, 2049, 311, 1054, 1060, 1078, 158, 285, 286), (2050,), (157, 1062, 1044, 1073, 1075), (),
  (1072, 1077), (1076, 1086, 1070), (), (2051,), (1084, 1085, 1055, 1069, 1068, 1087)))


def split_kernel(
    sizes,
    sequence_hbm,
    lengths_hbm,
    codes_hbm,
    tokens_hbm,
    owner_hbm,
    gain_hbm,
    final_gain_hbm,
    decoder_hbm,
    bias_hbm,
    hidden_hbm,
    weight_hbm,
    out_weight_hbm,
    dense_hbm,
    cos_hbm,
    sin_hbm,
    split_hbm,
    out_ref,
    sequence_ref,
    lengths_ref,
    codes_ref,
    tokens_ref,
    owner_ref,
    gain_ref,
    final_gain_ref,
    decoder_ref,
    bias_ref,
    hidden,
    normed,
    rows_buf,
    wbuf,
    raw,
    obuf,
    dense,
    cos,
    sin,
    split,
    pbuf,
    context,
    qbuf,
    gbuf,
    mixed,
    inbox,
    scores,
    local_sem,
    send_sem,
    arrive_sem,
    query_sem,
    norm_sem,
    swap_send_sem,
    swap_sem,
    score_sem,
    token_sem,
):
    n_dp, n_mp, head_size = sizes
    devices = n_dp * n_mp
    layers = n_dp // 2
    dp = lax.axis_index("dp")
    mp = lax.axis_index("mp")
    core = dp % 2
    layer = dp // 2
    partner = dp + 1 - 2 * core
    me = dp * n_mp + mp
    mate = partner * n_mp + mp
    parity = layer % 2
    pair = dp + 2 - 4 * parity
    twin = dp - 2 + 4 * parity
    middle = jnp.logical_and(layer > 0, layer < layers - 1)
    seq_span, feature = hidden.shape
    masks = codes_ref.shape[1]
    head_rows = 3 * head_size
    half_rows = head_size // 2
    where = {"x": (dp, flip(mp, 1)), "y": (dp, flip(mp, 2)), "e": (pair, mp), "m": (twin, mp), "d": (partner, mp)}

    barrier = pltpu.get_barrier_semaphore()

    def signal(semaphore, target):
        pl.semaphore_signal(semaphore, inc=1, device_id=target, device_id_type=MESH)

    for link in "dxye":
        signal(barrier, where[link])

    @pl.when(middle)
    def _():
        signal(barrier, where["m"])

    def local(index, source, target):
        copy = pltpu.make_async_copy(source, target, local_sem.at[index])
        copy.start()
        return copy

    weight_copy = local(1, weight_hbm.at[core], wbuf.at[0])
    hidden_copy = local(0, hidden_hbm, hidden)
    small_copies = [
        local(7 + place, source, target)
        for place, (source, target) in enumerate(
            (
                (sequence_hbm, sequence_ref),
                (lengths_hbm, lengths_ref),
                (codes_hbm, codes_ref),
                (tokens_hbm, tokens_ref),
                (gain_hbm, gain_ref),
            )
        )
    ]
    out_weight_copy = local(2, out_weight_hbm.at[:, pl.ds(pl.multiple_of(2 * core, 2), 2), :], raw)
    late_copies = [
        local(12 + place, source, target)
        for place, (source, target) in enumerate(
            (
                (owner_hbm, owner_ref),
                (final_gain_hbm, final_gain_ref),
                (decoder_hbm, decoder_ref),
                (bias_hbm, bias_ref),
            )
        )
    ]
    cos_copy = local(3, cos_hbm, cos)
    sin_copy = local(4, sin_hbm, sin)
    split_copy = local(6, split_hbm, split)
    dense_copy = local(5, dense_hbm, dense)

    def view(relation, item, half):
        start = FIRST_ROW[item] * head_size
        return (obuf if item > 5 else wbuf).at[relation, pl.ds(start + half * half_rows, half_rows), :]

    flips = {"x": 1, "y": 2, "e": 0, "m": 0}

    def piece_copy(relation, item, half, link, index):
        target = relation ^ flips[link]
        return pltpu.make_async_remote_copy(
            src_ref=view(relation, item, half),
            dst_ref=view(target, item, half),
            send_sem=send_sem.at[index // 12],
            recv_sem=arrive_sem.at[target - 1, 2 * item + half],
            device_id=where[link],
            device_id_type=MESH,
        )

    def rows_copy(source, target, link, index):
        return pltpu.make_async_remote_copy(
            src_ref=rows_buf.at[source],
            dst_ref=rows_buf.at[target],
            send_sem=swap_send_sem.at[index],
            recv_sem=swap_sem.at[index],
            device_id=where[link],
            device_id_type=MESH,
        )

    def query_copy(relation):
        return pltpu.make_async_remote_copy(
            src_ref=gbuf.at[relation],
            dst_ref=qbuf.at[relation],
            send_sem=query_sem.at[0, relation - 1],
            recv_sem=query_sem.at[1, relation - 1],
            device_id=where["e"],
            device_id_type=MESH,
        )

    sent = [[] for _ in range(layers)]

    def serve(words, place):
        inner = 0 < place < layers - 1
        for word in words:
            if word > QUERY:
                project_queries(word - QUERY)
            elif word > ROWS:
                query_copy(word - ROWS).wait_recv()
            elif word == ROWS and inner:
                rows_copy(0, 2, "e", 1).wait_recv()
                rows_copy(2, 3, "d", 2).start()
            elif word == ROWS:
                rows_copy(0, 2, "e", 1).start()
            else:
                relation, item, half = word // 16 % 4, word // 2 % 8, word % 2
                if word >= WAIT:
                    landing = view(relation, item, half)
                    pltpu.make_async_copy(landing, landing, arrive_sem.at[relation - 1, 2 * item + half]).wait()
                for place_of, link in enumerate("xyem"):
                    if word // 64 % 16 & (1 << place_of):
                        record = (relation, item, half, link, len(sent[place]))
                        sent[place].append(record)
                        piece_copy(*record).start()

    def service(index):
        for place in range(layers):
            if PLANS[place][index]:

                @pl.when(layer == place)
                def _():
                    serve(PLANS[place][index], place)

    weight_copy.wait()
    pl.semaphore_wait(barrier, 4 + middle.astype(jnp.int32))
    service(0)
    for copy in small_copies:
        copy.wait()
    out_weight_copy.wait()
    for head in range(2):
        obuf[0, head * head_size : (head + 1) * head_size, :] = raw[:, head, :]
    signal(token_sem.at[0], (partner, mp))

    def tokens_step(step):
        if step == 0:
            pl.semaphore_wait(token_sem.at[0], 1)
            signal(token_sem.at[1], (dp, flip(mp, 1)))
        elif step == 1:
            pl.semaphore_wait(token_sem.at[1], 1)
            signal(token_sem.at[2], (dp, flip(mp, 2)))
        else:
            hop = step - 3
            if hop < 0:
                pl.semaphore_wait(token_sem.at[2], 1)
            else:

                @pl.when(layer == hop + 1)
                def _():
                    pl.semaphore_wait(token_sem.at[3], 1)

                @pl.when(layer == layers - 2 - hop)
                def _():
                    pl.semaphore_wait(token_sem.at[4], 1)

            if hop + 1 < layers - 1:

                @pl.when(layer == hop + 1)
                def _():
                    signal(token_sem.at[3], (dp + 2, mp))

                @pl.when(layer == layers - 2 - hop)
                def _():
                    signal(token_sem.at[4], (dp - 2, mp))

    eye = lax.broadcasted_iota(jnp.int32, (masks, masks), 0) == lax.broadcasted_iota(
        jnp.int32, (masks, masks), 1
    )
    places = lax.broadcasted_iota(jnp.int32, (masks, seq_span), 1).astype(f32)

    def locate(which):
        length = lengths_ref[sequence_ref[which]].astype(f32)
        codes = codes_ref[pl.ds(which, 1), :].astype(f32)
        quotient = jnp.floor(codes / length)
        spots = codes - quotient * length
        spots = jnp.where(spots < 0.0, spots + length, spots)
        spots = jnp.where(spots >= length, spots - length, spots)
        spots = jnp.sum(jnp.where(eye, spots, 0.0), axis=1, keepdims=True)
        live = lax.broadcasted_iota(jnp.int32, (1, seq_span), 1).astype(f32) < length
        return places == spots, live

    located = [locate(which) for which in (me, mate, pair * n_mp + mp, (pair + 1 - 2 * core) * n_mp + mp)]
    chosen = located[0][0]
    alive = [live for _, live in located]
    tokens = tokens_ref[pl.ds(sequence_ref[me], 1), :].astype(f32)
    targets = jnp.sum(jnp.where(chosen, tokens, 0.0), axis=1, keepdims=True)
    onehots = [jnp.where(spots, 1.0, 0.0).astype(bf16) for spots, _ in located]
    onehot = onehots[0]

    hidden_copy.wait()
    tile = 128

    norm_copy = pltpu.make_async_remote_copy(
        src_ref=normed.at[0],
        dst_ref=normed.at[1],
        send_sem=norm_sem.at[0],
        recv_sem=norm_sem.at[1],
        device_id=(partner, mp),
        device_id_type=MESH,
    )

    def norm_rows(step, carry):
        rows = pl.ds(pl.multiple_of(step * tile, tile), tile)
        normed[0, rows, :] = (layer_norm(hidden[rows, :].astype(f32)) * gain_ref[...].reshape(1, feature)).astype(bf16)
        return carry

    lax.fori_loop(0, seq_span // tile, norm_rows, 0)
    rows_buf[0] = jnp.dot(onehot, normed[0], preferred_element_type=f32).astype(bf16)
    norm_copy.start()
    mixed[:masks, :] = jnp.dot(onehot, hidden[...], preferred_element_type=f32)
    mixed[masks:, :] = jnp.zeros((masks, feature), f32)
    rows_copy(0, 1, "d", 0).start()
    split_copy.wait()
    table = jnp.dot(jnp.concatenate(onehots, axis=0), split[...], preferred_element_type=f32)
    query_cos = table[:, :LANES] + table[:, LANES : 2 * LANES]
    query_sin = table[:, 2 * LANES : 3 * LANES] + table[:, 3 * LANES :]
    lane = lax.broadcasted_iota(jnp.int32, (1, LANES), 1)
    first = lane % head_size < head_size // 2
    low = lane < head_size
    transposed = (((1,), (1,)), ((), ()))

    def rotate(inputs, cosine, sine):
        turned = jnp.where(
            first,
            pltpu.roll(inputs, LANES - head_size // 2, 1),
            pltpu.roll(inputs, head_size // 2, 1),
        )
        return inputs * cosine + turned * sine

    span = seq_span

    def stack(refs):
        return jnp.concatenate([ref[...] for ref in refs], axis=0)

    def rows_of(start, count):
        return pl.ds(start if isinstance(start, int) else pl.multiple_of(start, head_size), count)

    def project(unit, buffer, slot):
        straight, turned = [], []
        for relation, head in unit:
            start = head * head_rows + head_size
            straight.append(wbuf[relation, rows_of(start, 2 * head_size), :])
            for offset, count in ((half_rows, half_rows), (0, half_rows), (head_size, head_size)):
                place = start + offset
                place = place if isinstance(place, int) else pl.multiple_of(place, half_rows)
                turned.append(wbuf[relation, pl.ds(place, count), :])
        keys = jnp.concatenate(straight + turned, axis=0)

        def step_of(step, carry):
            rows = pl.ds(pl.multiple_of(step * span, 16), span)
            made = lax.dot_general(normed[slot, rows, :], keys, transposed, preferred_element_type=f32)
            for head in range(2):
                block = made[:, head * LANES : (head + 1) * LANES] * cos[rows, :]
                block += made[:, (head + 2) * LANES : (head + 3) * LANES] * sin[rows, :]
                pbuf[buffer, slot, rows, head * LANES : (head + 1) * LANES] = block.astype(bf16)
            return carry

        lax.fori_loop(0, seq_span // span, step_of, 0)

    def queries(relation, low_slot, high_slot):
        weights = stack([wbuf.at[relation, head * head_rows : head * head_rows + head_size, :] for head in range(2)])
        rows = slice(low_slot * masks, high_slot * masks)
        source = rows_buf[low_slot:high_slot].reshape((high_slot - low_slot) * masks, feature)
        made = lax.dot_general(source, weights, transposed, preferred_element_type=f32)
        return rotate(made * head_size ** (-0.5), query_cos[rows], query_sin[rows]).astype(bf16)

    def project_queries(relation):
        if relation == 1:
            rows_copy(2, 3, "d", 2).wait_recv()
        made = queries(relation, 0, 4)
        gbuf[relation] = made[2 * masks :]
        qbuf[relation] = made[: 2 * masks]
        query_copy(relation).start()

    def of_head(query, head):
        query = query.astype(f32)
        if isinstance(head, int):
            return pltpu.roll(query, head_size, 1) if head else query
        return jnp.where(head == 1, pltpu.roll(query, head_size, 1), query)

    def attend(which, buffer, slot, near, far):
        empty = jnp.zeros((masks, LANES), bf16)
        near = jnp.where(low, near, 0.0).astype(bf16)
        far = jnp.where(low, far, 0.0).astype(bf16)
        both = jnp.concatenate(
            [jnp.concatenate([near, empty], axis=1), jnp.concatenate([empty, far], axis=1)], axis=0
        )
        block = pbuf[buffer, slot]
        logits = lax.dot_general(both, block, transposed, preferred_element_type=f32)
        logits = jnp.where(alive[slot], logits, -1e30)
        weight = jnp.exp(logits - jnp.max(logits, axis=-1, keepdims=True))
        probs = (weight / jnp.sum(weight, axis=-1, keepdims=True)).astype(bf16)
        vectors = jnp.dot(probs, block, preferred_element_type=f32)
        total = jnp.where(low, pltpu.roll(vectors[:masks, :LANES], head_size, 1), vectors[masks:, LANES:])
        context[slot * masks : (slot + 1) * masks, which * LANES : (which + 1) * LANES] = total.astype(bf16)

    def attend_both(which, unit, buffer):
        for slot in range(2):
            rows = slice(slot * masks, (slot + 1) * masks)
            near, far = [of_head(qbuf[relation, rows, :], head) for relation, head in unit]
            attend(which, buffer, slot, near, far)

    def mix(low_unit, *units):
        out_weights = stack([obuf.at[relation, rows_of(head * head_size, head_size), :] for unit in units for relation, head in unit])
        lanes = slice(low_unit * LANES, (low_unit + len(units)) * LANES)
        mixed[...] += jnp.dot(context[:, lanes], out_weights, preferred_element_type=f32)

    early = middle.astype(jnp.int32)
    own = ((0, 0), (0, 1))
    firsts = ((1, early), (2, early))
    seconds = ((1, 1 - early), (2, 1 - early))
    across = ((3, 0), (3, 1))

    cos_copy.wait()
    sin_copy.wait()
    service(1)
    project(own, 0, 0)
    service(2)
    query = queries(0, 0, 1)
    attend(0, 0, 0, of_head(query, 0), of_head(query, 1))
    tokens_step(0)
    service(3)
    norm_copy.wait_recv()
    rows_copy(0, 1, "d", 0).wait_recv()
    project(own, 0, 1)
    service(4)
    query = queries(0, 1, 2)
    attend(0, 0, 1, of_head(query, 0), of_head(query, 1))
    mix(0, own)
    tokens_step(1)
    service(5)
    project(firsts, 1, 0)
    service(6)
    project(firsts, 1, 1)
    tokens_step(2)
    service(7)
    attend_both(1, firsts, 1)
    tokens_step(3)
    service(8)
    project(seconds, 0, 0)
    service(9)
    project(seconds, 0, 1)
    service(10)
    attend_both(2, seconds, 0)
    tokens_step(4)
    service(11)
    project(across, 1, 0)
    service(12)
    project(across, 1, 1)
    service(13)
    attend_both(3, across, 1)
    tokens_step(5)
    service(14)
    mix(1, firsts, seconds, across)
    inbox_copy = pltpu.make_async_remote_copy(
        src_ref=mixed.at[pl.ds(masks, masks), :],
        dst_ref=inbox,
        send_sem=swap_send_sem.at[3],
        recv_sem=swap_sem.at[3],
        device_id=(partner, mp),
        device_id_type=MESH,
    )
    inbox_copy.start()
    dense_copy.wait()
    for copy in late_copies:
        copy.wait()
    inbox_copy.wait_recv()
    residual = mixed[:masks, :] + inbox[...]
    normed_final = (layer_norm(residual) * final_gain_ref[...].reshape(1, feature)).astype(bf16)
    dense_out = jnp.dot(normed_final, dense[...], preferred_element_type=f32)
    headed = layer_norm(0.5 * dense_out * (1.0 + lax.erf(dense_out * 0.5**0.5))).astype(bf16)
    logits = lax.dot_general(headed, decoder_ref[...], transposed, preferred_element_type=f32) + bias_ref[...]
    largest = jnp.max(logits, axis=-1, keepdims=True)
    scale = jnp.log(jnp.sum(jnp.exp(logits - largest), axis=-1, keepdims=True)) + largest
    vocabulary = lax.broadcasted_iota(jnp.int32, logits.shape, 1).astype(f32)
    picked = jnp.sum(jnp.where(vocabulary == targets, logits - scale, 0.0), axis=1, keepdims=True)
    row = jnp.sum(jnp.where(eye, picked, 0.0), axis=0, keepdims=True)
    padded = jnp.concatenate([row] * (LANES // masks), axis=1)
    scores[me] = padded

    def score_copy(step):
        other_dp, other_mp = flip(dp, step // n_mp), flip(mp, step % n_mp)
        return pltpu.make_async_remote_copy(
            src_ref=scores.at[me],
            dst_ref=scores.at[me],
            send_sem=score_sem.at[0],
            recv_sem=score_sem.at[1],
            device_id=(other_dp, other_mp),
            device_id_type=MESH,
        )

    for step in reversed(range(1, devices)):
        score_copy(step).start()
    inbox_copy.wait_send()
    norm_copy.wait_send()
    rows_copy(0, 1, "d", 0).wait_send()

    for place in range(layers):

        @pl.when(layer == place)
        def _():
            for group in range(0, len(sent[place]), 12):
                count = min(12, len(sent[place]) - group)
                bulk = wbuf.at[0, pl.ds(0, count * half_rows), :]
                pltpu.make_async_copy(bulk, bulk, send_sem.at[group // 12]).wait()
            if 0 < place < layers - 1:
                rows_copy(2, 3, "d", 2).wait_send()
                for relation in (1, 2, 3):
                    query_copy(relation).wait_send()
            else:
                rows_copy(0, 2, "e", 1).wait_send()

    group = out_ref.shape[0]
    square = lax.broadcasted_iota(jnp.int32, (devices, devices), 0) == lax.broadcasted_iota(
        jnp.int32, (devices, devices), 1
    )
    owners = jnp.sum(jnp.where(square, owner_ref[...].astype(f32), 0.0), axis=1, keepdims=True)
    selects = [jnp.where(owners == (dp * group + place).astype(f32), 1.0, 0.0) for place in range(group)]
    everyone = scores.at[pl.ds(0, devices - 1)]
    pltpu.make_async_copy(everyone, everyone, score_sem.at[1]).wait()
    pltpu.make_async_copy(everyone, everyone, score_sem.at[0]).wait()
    gathered = scores[...].reshape(devices, LANES)
    result = jnp.concatenate([jnp.sum(gathered * select, axis=0, keepdims=True) for select in selects], axis=0)
    out_ref[...] = pltpu.roll(result, LANES - mp * out_ref.shape[1], 1)[:, : out_ref.shape[1]]


def split_call(shape, inputs, weight, out_weight, hidden, dense_weight, cosine, sine, group, head_size):
    n_dp, n_mp = shape
    devices = n_dp * n_mp
    seq_span, feature = hidden.shape
    width = weight.shape[1]
    masks = inputs[2].shape[1]
    high = [t.astype(jnp.bfloat16).astype(np.float32) for t in (cosine, sine)]
    parts = [high[0], cosine - high[0], high[1], sine - high[1]]
    split = np.concatenate(parts, axis=1).astype(jnp.bfloat16)
    dma = pltpu.SemaphoreType.DMA
    vmem = pl.BlockSpec(memory_space=pltpu.VMEM)
    anywhere = pl.BlockSpec(memory_space=pl.ANY)
    return pl.pallas_call(
        functools.partial(split_kernel, (n_dp, n_mp, head_size)),
        name="score_split",
        out_shape=jax.ShapeDtypeStruct((group, masks // n_mp), f32),
        in_specs=[anywhere] * 16,
        out_specs=vmem,
        scratch_shapes=[(pltpu.SMEM if place < 2 else pltpu.VMEM)(x.shape, x.dtype) for place, x in enumerate(inputs)]
        + [
            pltpu.VMEM((seq_span, feature), bf16),
            pltpu.VMEM((2, seq_span, feature), bf16),
            pltpu.VMEM((4, masks, feature), bf16),
            pltpu.VMEM((n_mp, width, feature), bf16),
            pltpu.VMEM((head_size, 2, feature), bf16),
            pltpu.VMEM((n_mp, 2 * head_size, feature), bf16),
            pltpu.VMEM((feature, feature), bf16),
            pltpu.VMEM((seq_span, LANES), f32),
            pltpu.VMEM((seq_span, LANES), f32),
            pltpu.VMEM((seq_span, 4 * LANES), bf16),
            pltpu.VMEM((2, 2, seq_span, 2 * LANES), bf16),
            pltpu.VMEM((2 * masks, 4 * LANES), bf16),
            pltpu.VMEM((n_mp, 2 * masks, LANES), bf16),
            pltpu.VMEM((n_mp, 2 * masks, LANES), bf16),
            pltpu.VMEM((2 * masks, feature), f32),
            pltpu.VMEM((masks, feature), f32),
            pltpu.VMEM((devices, 1, LANES), f32),
            dma((16,)),
            dma((6,)),
            dma((n_mp - 1, 16)),
            dma((2, n_mp - 1)),
            dma((2,)),
            dma((4,)),
            dma((4,)),
            dma((2,)),
            pltpu.SemaphoreType.REGULAR((5,)),
        ],
        compiler_params=pltpu.CompilerParams(collective_id=1, has_side_effects=True),
    )(
        *inputs,
        hidden,
        weight,
        out_weight,
        dense_weight,
        jnp.asarray(np.where(np.arange(LANES) < head_size, cosine, np.float32(1))),
        jnp.asarray(np.where(np.arange(LANES) < head_size, sine, np.float32(0))),
        jnp.asarray(split),
    )


def on_device(
    shape,
    hidden_states,
    ln_attn_gain,
    w_qkv,
    output_weight,
    ln_final_gain,
    dense_weight,
    decoder_weight,
    decoder_bias,
    seq_tokens,
    seq_lengths,
    copy_sequence,
    mask_code,
    copy_owner,
):
    n_dp, n_mp = shape
    devices = n_dp * n_mp
    lane_copies, seq_span, feature = hidden_states.shape
    head_size, heads, _ = output_weight.shape
    copies, masks = mask_code.shape
    assert lane_copies == 1 and copies == devices and n_dp % 2 == 0
    assert 2 * head_size == LANES and masks <= LANES
    in_chunk = 2 if heads % 2 == 0 else 1
    chunks = heads // in_chunk
    width = in_chunk * 3 * head_size
    weight = jnp.transpose(w_qkv.reshape(feature, chunks, width), (1, 2, 0))
    cosine, sine = rotary_tables(seq_span, head_size)
    group = copies // n_dp
    items = 2 * chunks + 2
    dma = pltpu.SemaphoreType.DMA
    vmem = pl.BlockSpec(memory_space=pltpu.VMEM)
    smem = pl.BlockSpec(memory_space=pltpu.SMEM)
    anywhere = pl.BlockSpec(memory_space=pl.ANY)
    own = masks // n_mp
    inputs = (
        copy_sequence,
        seq_lengths,
        mask_code,
        seq_tokens,
        copy_owner.reshape(1, -1),
        ln_attn_gain,
        ln_final_gain,
        decoder_weight.T,
        decoder_bias.reshape(1, -1),
    )
    if n_mp == 4 and n_dp == 8 and heads == 4 and seq_span % 128 == 0:
        hidden = hidden_states.reshape(seq_span, feature)
        return split_call(shape, inputs, weight, output_weight, hidden, dense_weight, cosine, sine, group, head_size)
    out_weight = jnp.swapaxes(output_weight, 0, 1).reshape(heads * head_size, feature)
    rows = pl.pallas_call(
        functools.partial(kernel, (n_dp, n_mp, head_size, in_chunk, chunks)),
        name="score_copies",
        out_shape=jax.ShapeDtypeStruct((group, LANES), f32),
        in_specs=[smem] * 2 + [vmem] * 7 + [anywhere] * 6,
        out_specs=vmem,
        scratch_shapes=[
            pltpu.VMEM((seq_span, feature), bf16),
            pltpu.VMEM((seq_span, feature), bf16),
            pltpu.VMEM((n_mp, chunks, width, feature), bf16),
            pltpu.VMEM((n_mp, heads * head_size, feature), bf16),
            pltpu.VMEM((feature, feature), bf16),
            pltpu.VMEM((seq_span, LANES), f32),
            pltpu.VMEM((seq_span, LANES), f32),
            pltpu.VMEM((seq_span, in_chunk * LANES), bf16),
            pltpu.VMEM((n_mp, chunks, masks, in_chunk * head_size), bf16),
            pltpu.VMEM((masks, feature), f32),
            pltpu.VMEM((devices, 8, LANES), f32),
            dma((6,)),
            dma((n_mp, items)),
            dma((items,)),
            dma((n_mp, chunks)),
            dma((n_mp, items)),
            dma((n_mp, items)),
            dma((n_mp, items)),
            dma((devices,)),
            dma((devices,)),
        ],
        compiler_params=pltpu.CompilerParams(collective_id=0, has_side_effects=True),
    )(
        copy_sequence,
        seq_lengths,
        mask_code,
        seq_tokens,
        copy_owner.reshape(1, -1),
        ln_attn_gain,
        ln_final_gain,
        decoder_weight.T,
        decoder_bias.reshape(1, -1),
        hidden_states.reshape(seq_span, feature),
        weight,
        out_weight,
        dense_weight,
        jnp.asarray(cosine),
        jnp.asarray(sine),
    )
    return lax.dynamic_slice_in_dim(rows, lax.axis_index("mp") * own, own, 1)


def solution(mesh):
    placed = (
        P(("dp", "mp"), None, None),
        P(),
        P(None, "mp", None),
        P(None, "mp", None),
        P(),
        P(),
        P(),
        P(),
        P(),
        P(),
        P(),
        P(),
        P(),
    )
    shape = (mesh.shape["dp"], mesh.shape["mp"])
    return jax.shard_map(
        functools.partial(on_device, shape),
        mesh=mesh,
        in_specs=placed,
        out_specs=P("dp", "mp"),
        check_vma=False,
    )
```

```python
import functools

import jax
import jax.numpy as jnp
import numpy as np
from jax import lax
from jax.experimental import pallas as pl
from jax.experimental.pallas import tpu as pltpu
from jax.sharding import PartitionSpec as P

epsilon = 1e-05
MESH = pl.DeviceIdType.MESH
f32 = jnp.float32
bf16 = jnp.bfloat16
LANES = 128


def layer_norm(inputs):
    average = jnp.mean(inputs, axis=-1, keepdims=True)
    centred = inputs - average
    variance = jnp.mean(centred * centred, axis=-1, keepdims=True)
    return centred * lax.rsqrt(variance + epsilon)


def rotary_tables(seq_span, head_size):
    half = head_size // 2
    frequency = (1.0 / 10000.0 ** (np.arange(half, dtype=np.float32) * (2.0 / head_size))).astype(
        np.float32
    )
    angles = np.arange(seq_span, dtype=np.float32)[:, None] * frequency[None, :]
    cosine, sine = np.cos(angles), np.sin(angles)
    times = LANES // head_size
    return (
        np.tile(np.concatenate([cosine, cosine], axis=1), (1, times)).astype(np.float32),
        np.tile(np.concatenate([-sine, sine], axis=1), (1, times)).astype(np.float32),
    )


def flip(index, mask):
    bit = 1
    out = index
    while bit <= mask:
        if mask & bit:
            out = out + bit * (1 - 2 * ((index // bit) % 2))
        bit *= 2
    return out


def kernel(
    sizes,
    sequence_ref,
    lengths_ref,
    codes_ref,
    tokens_ref,
    owner_ref,
    gain_ref,
    final_gain_ref,
    decoder_ref,
    bias_ref,
    hidden_hbm,
    weight_hbm,
    out_weight_hbm,
    dense_hbm,
    cos_hbm,
    sin_hbm,
    out_ref,
    hidden,
    normed,
    wbuf,
    obuf,
    dense,
    cos,
    sin,
    pbuf,
    context,
    mixed,
    scores,
    local_sem,
    direct_sem,
    relay_sem,
    exchange_sem,
    share_sem,
    arrive_sem,
    shared_sem,
    score_send_sem,
    score_sem,
):
    n_dp, n_mp, head_size, heads_in_chunk, chunks = sizes
    devices = n_dp * n_mp
    dp = lax.axis_index("dp")
    mp = lax.axis_index("mp")
    core = dp % 2
    partner = dp + 1 - 2 * core
    me = dp * n_mp + mp
    seq_span, feature = hidden.shape
    masks = codes_ref.shape[1]
    chunk_heads = heads_in_chunk * head_size
    out_rows = obuf.shape[1]
    piece_rows = out_rows // 4

    def local(index, source, target):
        copy = pltpu.make_async_copy(source, target, local_sem.at[index])
        copy.start()
        return copy

    weight_copy = local(1, weight_hbm, wbuf.at[0])
    hidden_copy = local(0, hidden_hbm, hidden)

    barrier = pltpu.get_barrier_semaphore()

    def greet(step, carry):
        other = (me + step) % devices
        pl.semaphore_signal(
            barrier, inc=1, device_id=(other // n_mp, other % n_mp), device_id_type=MESH
        )
        return carry

    lax.fori_loop(1, devices, greet, 0)

    parity = (dp // 2) % 2
    above = dp + 2 - 4 * parity
    part_rows = wbuf.shape[2] // 4

    def part(chunk, odd):
        return 2 * chunk + odd

    def place(relation, item, half):
        if item < 2 * chunks:
            chunk, odd = divmod(item, 2)
            which = 1 - parity if odd else parity
            start = (2 * half + which) * part_rows
            return wbuf.at[relation, chunk, pl.ds(pl.multiple_of(start, 16), part_rows), :]
        start = (2 * half + item - 2 * chunks) * piece_rows
        return obuf.at[relation, pl.ds(pl.multiple_of(start, 16), piece_rows), :]

    def view(relation, item):
        return place(relation, item, core)

    def partner_view(relation, item):
        return place(relation, item, 1 - core)

    sent = []

    def to_group(target, source_relation, relation, item, semaphore):
        copy = pltpu.make_async_remote_copy(
            src_ref=view(source_relation, item),
            dst_ref=view(relation, item),
            send_sem=semaphore,
            recv_sem=arrive_sem.at[relation, item],
            device_id=(dp, flip(mp, target)),
            device_id_type=MESH,
        )
        copy.start()
        sent.append(copy)

    def direct(target, item):
        to_group(target, 0, target, item, direct_sem.at[target, item])

    def relay(target, source_relation, item):
        to_group(target, source_relation, source_relation ^ target, item, relay_sem.at[item])

    def exchange(relation, chunk):
        copy = pltpu.make_async_remote_copy(
            src_ref=view(relation, part(chunk, 0)),
            dst_ref=view(relation, part(chunk, 0)),
            send_sem=exchange_sem.at[relation, chunk],
            recv_sem=arrive_sem.at[relation, part(chunk, 1)],
            device_id=(above, mp),
            device_id_type=MESH,
        )
        copy.start()
        sent.append(copy)

    def arrived(relation, item):
        landing = view(relation, item)
        pltpu.make_async_copy(landing, landing, arrive_sem.at[relation, item]).wait()

    def share(relation, item):
        copy = pltpu.make_async_remote_copy(
            src_ref=view(relation, item),
            dst_ref=view(relation, item),
            send_sem=share_sem.at[relation, item],
            recv_sem=shared_sem.at[relation, item],
            device_id=(partner, mp),
            device_id_type=MESH,
        )
        copy.start()
        sent.append(copy)

    def was_shared(relation, item):
        landing = partner_view(relation, item)
        pltpu.make_async_copy(landing, landing, shared_sem.at[relation, item]).wait()

    sequence = sequence_ref[me]
    length = lengths_ref[sequence].astype(f32)
    codes = codes_ref[pl.ds(me, 1), :].astype(f32)
    quotient = jnp.floor(codes / length)
    row_positions = codes - quotient * length
    row_positions = jnp.where(row_positions < 0.0, row_positions + length, row_positions)
    row_positions = jnp.where(row_positions >= length, row_positions - length, row_positions)
    eye = lax.broadcasted_iota(jnp.int32, (masks, masks), 0) == lax.broadcasted_iota(
        jnp.int32, (masks, masks), 1
    )
    positions = jnp.sum(jnp.where(eye, row_positions, 0.0), axis=1, keepdims=True)
    places = lax.broadcasted_iota(jnp.int32, (masks, seq_span), 1).astype(f32)
    chosen = places == positions
    onehot = jnp.where(chosen, 1.0, 0.0)
    onehot_bf = onehot.astype(bf16)
    tokens = tokens_ref[pl.ds(sequence, 1), :].astype(f32)
    targets = jnp.sum(jnp.where(chosen, tokens, 0.0), axis=1, keepdims=True)
    alive = lax.broadcasted_iota(jnp.int32, (1, seq_span), 1).astype(f32) < length

    weight_copy.wait()
    pl.semaphore_wait(barrier, devices - 1)
    items = 2 * chunks + 2
    routed = n_mp == 4 and chunks == 2 and n_dp % 4 == 0
    if routed:
        direct(1, part(1, 0))
        direct(2, part(0, 0))
        direct(1, part(0, 0))
        direct(2, part(1, 0))
    cos_copy = local(3, cos_hbm, cos)
    sin_copy = local(4, sin_hbm, sin)
    out_weight_copy = local(2, out_weight_hbm, obuf.at[0])
    dense_copy = local(5, dense_hbm, dense)
    if not routed:
        out_weight_copy.wait()
        for item in range(items):
            for target in range(1, n_mp):
                direct(target, item)

    hidden_copy.wait()
    tile = 128 if seq_span % 128 == 0 else 8

    def norm_rows(step, carry):
        rows = pl.ds(pl.multiple_of(step * tile, tile), tile)
        normed[rows, :] = (layer_norm(hidden[rows, :].astype(f32)) * gain_ref[...].reshape(1, feature)).astype(bf16)
        return carry

    lax.fori_loop(0, seq_span // tile, norm_rows, 0)
    masked_rows = jnp.dot(onehot_bf, normed[...], preferred_element_type=f32).astype(bf16)
    own_rows = jnp.dot(onehot_bf, hidden[...], preferred_element_type=f32)
    mixed[...] = own_rows
    cos_copy.wait()
    sin_copy.wait()
    exact = dict(preferred_element_type=f32, precision=lax.Precision.HIGHEST)
    query_cos = jnp.dot(onehot, cos[...], **exact)
    query_sin = jnp.dot(onehot, sin[...], **exact)
    lane = lax.broadcasted_iota(jnp.int32, (1, LANES), 1)
    first = lane % head_size < head_size // 2

    def rotate(inputs, cosine, sine):
        turned = jnp.where(
            first,
            pltpu.roll(inputs, LANES - head_size // 2, 1),
            pltpu.roll(inputs, head_size // 2, 1),
        )
        return inputs * cosine + turned * sine

    transposed = (((1,), (1,)), ((), ()))
    low = lane < head_size
    span = seq_span // 2 if seq_span % 32 == 0 else seq_span
    head_rows = 3 * head_size

    def attend(relation, chunk):
        weights = wbuf.at[relation, chunk]
        pairs = [
            weights[head * head_rows + head_size : (head + 1) * head_rows, :]
            for head in range(heads_in_chunk)
        ]
        pair_weights = pairs[0] if heads_in_chunk == 1 else jnp.concatenate(pairs, axis=0)

        def project(step, carry):
            rows = pl.ds(pl.multiple_of(step * span, 16), span)
            made = lax.dot_general(
                normed[rows, :], pair_weights, transposed, preferred_element_type=f32
            )
            for head in range(heads_in_chunk):
                block = made[:, head * LANES : (head + 1) * LANES]
                block = jnp.where(low, rotate(block, cos[rows, :], sin[rows, :]), block)
                pbuf[rows, head * LANES : (head + 1) * LANES] = block.astype(bf16)
            return carry

        lax.fori_loop(0, seq_span // span, project, 0)
        if heads_in_chunk == 1:
            query_weights = weights[: 2 * head_size, :]
        else:
            query_weights = jnp.concatenate(
                [weights[:head_size, :], weights[head_rows : head_rows + head_size, :]], axis=0
            )
        made = lax.dot_general(masked_rows, query_weights, transposed, preferred_element_type=f32)
        turned = rotate(made * head_size ** (-0.5), query_cos, query_sin)
        vectors = []
        for head in range(heads_in_chunk):
            query = turned if head == 0 else pltpu.roll(turned, head_size, 1)
            query = jnp.where(low, query, 0.0).astype(bf16)
            block = pbuf[:, head * LANES : (head + 1) * LANES]
            logits = lax.dot_general(query, block, transposed, preferred_element_type=f32)
            logits = jnp.where(alive, logits, -1e30)
            weight = jnp.exp(logits - jnp.max(logits, axis=-1, keepdims=True))
            probs = (weight / jnp.sum(weight, axis=-1, keepdims=True)).astype(bf16)
            vectors.append(jnp.dot(probs, block, preferred_element_type=f32))
        total = pltpu.roll(vectors[0], head_size, 1)
        if heads_in_chunk > 1:
            total = jnp.where(low, total, vectors[1])
        context[relation, chunk] = total[:, :chunk_heads].astype(bf16)

    def mix(relation):
        for chunk in range(chunks):
            rows = slice(chunk * chunk_heads, (chunk + 1) * chunk_heads)
            mixed[...] += jnp.dot(
                context[relation, chunk], obuf[relation, rows, :], preferred_element_type=f32
            )

    def fetch(*pairs):
        for pair in pairs:
            arrived(*pair)
            share(*pair)

    def attend_shared(relation, chunk):
        was_shared(relation, part(chunk, 0))
        was_shared(relation, part(chunk, 1))
        attend(relation, chunk)

    attend(0, 0)
    if routed:
        first_piece, second_piece = 2 * chunks, 2 * chunks + 1
        arrived(1, part(1, 0))
        relay(2, 1, part(1, 0))
        exchange(1, 1)
        share(1, part(1, 0))
        arrived(2, part(0, 0))
        relay(1, 2, part(0, 0))
        exchange(2, 0)
        share(2, part(0, 0))
        direct(1, part(0, 1))
        direct(2, part(1, 1))
        out_weight_copy.wait()
        direct(1, first_piece)
        direct(2, second_piece)
        direct(1, second_piece)
        direct(2, first_piece)
    for chunk in range(1, chunks):
        attend(0, chunk)
    mix(0)
    if routed:
        fetch((1, part(0, 0)), (2, part(1, 0)), (1, part(1, 1)))
        arrived(3, part(0, 0))
        exchange(3, 0)
        share(3, part(0, 0))
        arrived(3, part(1, 0))
        exchange(3, 1)
        share(3, part(1, 0))
        fetch((2, part(0, 1)))
        attend_shared(1, 1)
        attend_shared(2, 0)
        fetch((1, part(0, 1)), (2, part(1, 1)), (3, part(0, 1)))
        attend_shared(1, 0)
        arrived(1, first_piece)
        relay(2, 1, first_piece)
        share(1, first_piece)
        arrived(2, second_piece)
        relay(1, 2, second_piece)
        share(2, second_piece)
        attend_shared(2, 1)
        fetch((3, part(1, 1)))
        attend_shared(3, 0)
        fetch((1, second_piece), (2, first_piece))
        attend_shared(3, 1)
        for relation in (1, 2):
            was_shared(relation, first_piece)
            was_shared(relation, second_piece)
            mix(relation)
        fetch((3, first_piece), (3, second_piece))
        was_shared(3, first_piece)
        was_shared(3, second_piece)
        mix(3)
    else:
        for relation in range(1, n_mp):
            fetch(*[(relation, item) for item in range(items)])
        for relation in range(1, n_mp):
            for item in range(items):
                was_shared(relation, item)
            for chunk in range(chunks):
                attend(relation, chunk)
            mix(relation)

    normed_final = (layer_norm(mixed[...]) * final_gain_ref[...].reshape(1, feature)).astype(bf16)
    dense_copy.wait()
    dense_out = jnp.dot(normed_final, dense[...], preferred_element_type=f32)
    headed = layer_norm(0.5 * dense_out * (1.0 + lax.erf(dense_out * 0.5**0.5))).astype(bf16)
    logits = lax.dot_general(headed, decoder_ref[...], transposed, preferred_element_type=f32) + bias_ref[...]
    largest = jnp.max(logits, axis=-1, keepdims=True)
    scale = jnp.log(jnp.sum(jnp.exp(logits - largest), axis=-1, keepdims=True)) + largest
    vocabulary = lax.broadcasted_iota(jnp.int32, logits.shape, 1).astype(f32)
    picked = jnp.sum(jnp.where(vocabulary == targets, logits - scale, 0.0), axis=1, keepdims=True)
    row = jnp.sum(jnp.where(eye, picked, 0.0), axis=0, keepdims=True)
    padded = jnp.pad(row, ((0, 0), (0, LANES - masks)))
    scores[me] = jnp.broadcast_to(padded, scores.shape[1:])

    def score_copy(step):
        other = (me + step) % devices
        return pltpu.make_async_remote_copy(
            src_ref=scores.at[me, pl.ds(0, 1), :],
            dst_ref=scores.at[me, pl.ds(0, 1), :],
            send_sem=score_send_sem.at[step],
            recv_sem=score_sem.at[me],
            device_id=(other // n_mp, other % n_mp),
            device_id_type=MESH,
        )

    def send_scores(step, carry):
        score_copy(step).start()
        return carry

    lax.fori_loop(1, devices, send_scores, 0)
    for copy in sent:
        copy.wait_send()

    def wait_scores(step, carry):
        source = (me + step) % devices
        landing = scores.at[source, pl.ds(0, 1), :]
        pltpu.make_async_copy(landing, landing, score_sem.at[source]).wait()
        return carry

    lax.fori_loop(1, devices, wait_scores, 0)

    def wait_sends(step, carry):
        score_copy(step).wait_send()
        return carry

    lax.fori_loop(1, devices, wait_sends, 0)
    group = out_ref.shape[0]
    wanted = dp * group + lax.broadcasted_iota(jnp.int32, (group, owner_ref.shape[1]), 0)
    select = jnp.where(owner_ref[...] == wanted, 1.0, 0.0)
    out_ref[...] = jnp.dot(select, scores[:, 0, :], **exact)


FIRST_ROW = (1, 2, 4, 5, 0, 3, 0, 1)
WAIT, ROWS, QUERY = 1024, 2048, 2052
PLANS = (((128, 70, 131, 69), (194, 143, 76, 2048, 1315, 1045, 67, 135), (142, 65),
  (1046, 134, 1314, 1043, 98, 1071, 149, 1042, 99, 303, 1056), (406, 78),
  (1052, 1063, 1041, 1134, 156, 1060, 1044, 273, 1040, 275, 1057, 133),
  (111, 144, 1062, 1330, 1047, 103, 79, 1333), (2049, 140, 2050), (1054, 1084, 141, 1061, 1078, 77, 1075), (),
  (1079, 1073, 1342), (1076, 1068, 1072), (), (1085, 1053, 2051, 1087, 1069, 1055), ()),
 ((132, 64, 68, 202, 139), (), (1060, 71, 141, 66, 548, 135, 1040, 140, 272, 69, 292, 73, 1300, 532),
  (1066, 1579, 1057, 1048, 1559, 554, 528, 1069, 353, 152, 134),
  (1045, 1058, 279, 109, 136, 1080, 148, 568, 106, 1071),
  (1049, 1061, 1050, 1063, 1132, 78, 1062, 1051, 1073, 2048, 556, 1046, 1065, 305, 557, 105, 561, 155, 2053),
  (1064, 2054, 151, 76), (77, 1076, 1056, 1043), (1085, 147, 1041, 308, 1059, 1042), (1082,), (1083, 317),
  (1054, 1084, 1081, 559, 142, 1077, 1079, 1075, 1078, 1074, 1072, 2055), (), (),
  (1053, 1087, 1052, 1070, 1055, 1086)),
 ((72, 129, 74, 133, 75, 137, 1048, 69, 1057, 65, 135, 536, 134, 801),
  (1050, 1051, 1061, 73, 1065, 805, 131, 553, 539, 1056, 79, 1045, 142, 277), (136, 155, 1297, 1044, 1062),
  (1060, 102, 544, 1049, 1063, 96, 153, 2048, 276, 292), (100,),
  (1047, 1067, 1070, 2053, 1066, 1055, 1042, 1064, 110, 1046, 2054),
  (1083, 302, 1059, 106, 1040, 99, 1058, 159), (1078, 1072, 566, 1076, 287, 1080, 308, 1043, 149), (560,),
  (1087,), (1069, 543, 1082, 109),
  (1081, 1052, 1086, 1074, 1077, 2055, 1068, 156, 575, 1079, 300, 1053, 1075, 1073), (), (1085,),
  (1054, 1071, 1084)),
 ((66, 70, 128, 130), (199, 143, 131, 1056, 1042, 288, 67, 76, 146, 77, 2048, 1058, 141, 1046, 1047),
  (64, 274, 278, 1057, 290), (1043,), (150, 151, 134, 1061, 1063, 275, 78, 1059, 1074),
  (97, 306, 99, 1180, 1045, 284, 1040, 1053, 101, 144, 1041),
  (1135, 1079, 2049, 311, 1054, 1060, 1078, 158, 285, 286), (2050,), (157, 1062, 1044, 1073, 1075), (),
  (1072, 1077), (1076, 1086, 1070), (), (2051,), (1084, 1085, 1055, 1069, 1068, 1087)))


def split_kernel(
    sizes,
    sequence_hbm,
    lengths_hbm,
    codes_hbm,
    tokens_hbm,
    owner_hbm,
    gain_hbm,
    final_gain_hbm,
    decoder_hbm,
    bias_hbm,
    hidden_hbm,
    weight_hbm,
    out_weight_hbm,
    dense_hbm,
    cos_hbm,
    sin_hbm,
    split_hbm,
    out_ref,
    sequence_ref,
    lengths_ref,
    codes_ref,
    tokens_ref,
    owner_ref,
    gain_ref,
    final_gain_ref,
    decoder_ref,
    bias_ref,
    hidden,
    normed,
    rows_buf,
    wbuf,
    raw,
    obuf,
    dense,
    cos,
    sin,
    split,
    pbuf,
    context,
    qbuf,
    gbuf,
    mixed,
    inbox,
    scores,
    local_sem,
    send_sem,
    arrive_sem,
    query_sem,
    norm_sem,
    swap_send_sem,
    swap_sem,
    score_sem,
    token_sem,
):
    n_dp, n_mp, head_size = sizes
    devices = n_dp * n_mp
    layers = n_dp // 2
    dp = lax.axis_index("dp")
    mp = lax.axis_index("mp")
    core = dp % 2
    layer = dp // 2
    partner = dp + 1 - 2 * core
    me = dp * n_mp + mp
    mate = partner * n_mp + mp
    parity = layer % 2
    pair = dp + 2 - 4 * parity
    twin = dp - 2 + 4 * parity
    middle = jnp.logical_and(layer > 0, layer < layers - 1)
    seq_span, feature = hidden.shape
    masks = codes_ref.shape[1]
    head_rows = 3 * head_size
    half_rows = head_size // 2
    where = {"x": (dp, flip(mp, 1)), "y": (dp, flip(mp, 2)), "e": (pair, mp), "m": (twin, mp), "d": (partner, mp)}

    barrier = pltpu.get_barrier_semaphore()

    def signal(semaphore, target):
        pl.semaphore_signal(semaphore, inc=1, device_id=target, device_id_type=MESH)

    def local(index, source, target):
        copy = pltpu.make_async_copy(source, target, local_sem.at[index])
        copy.start()
        return copy

    weight_copy = local(1, weight_hbm.at[core], wbuf.at[0])
    for link in "dxye":
        signal(barrier, where[link])

    @pl.when(middle)
    def _():
        signal(barrier, where["m"])

    hidden_copy = local(0, hidden_hbm, hidden)
    small_copies = [
        local(7 + place, source, target)
        for place, (source, target) in enumerate(
            (
                (sequence_hbm, sequence_ref),
                (lengths_hbm, lengths_ref),
                (codes_hbm, codes_ref),
                (tokens_hbm, tokens_ref),
                (gain_hbm, gain_ref),
            )
        )
    ]
    out_weight_copy = local(2, out_weight_hbm.at[:, pl.ds(pl.multiple_of(2 * core, 2), 2), :], raw)
    late_copies = [
        local(12 + place, source, target)
        for place, (source, target) in enumerate(
            (
                (owner_hbm, owner_ref),
                (final_gain_hbm, final_gain_ref),
                (decoder_hbm, decoder_ref),
                (bias_hbm, bias_ref),
            )
        )
    ]
    cos_copy = local(3, cos_hbm, cos)
    sin_copy = local(4, sin_hbm, sin)
    split_copy = local(6, split_hbm, split)
    dense_copy = local(5, dense_hbm, dense)

    def view(relation, item, half):
        start = FIRST_ROW[item] * head_size
        return (obuf if item > 5 else wbuf).at[relation, pl.ds(start + half * half_rows, half_rows), :]

    flips = {"x": 1, "y": 2, "e": 0, "m": 0}

    def piece_copy(relation, item, half, link, index):
        target = relation ^ flips[link]
        return pltpu.make_async_remote_copy(
            src_ref=view(relation, item, half),
            dst_ref=view(target, item, half),
            send_sem=send_sem.at[index // 12],
            recv_sem=arrive_sem.at[target - 1, 2 * item + half],
            device_id=where[link],
            device_id_type=MESH,
        )

    def rows_copy(source, target, link, index):
        return pltpu.make_async_remote_copy(
            src_ref=rows_buf.at[source],
            dst_ref=rows_buf.at[target],
            send_sem=swap_send_sem.at[index],
            recv_sem=swap_sem.at[index],
            device_id=where[link],
            device_id_type=MESH,
        )

    def query_copy(relation):
        return pltpu.make_async_remote_copy(
            src_ref=gbuf.at[relation],
            dst_ref=qbuf.at[relation],
            send_sem=query_sem.at[0, relation - 1],
            recv_sem=query_sem.at[1, relation - 1],
            device_id=where["e"],
            device_id_type=MESH,
        )

    sent = [[] for _ in range(layers)]

    def serve(words, place):
        inner = 0 < place < layers - 1
        for word in words:
            if word > QUERY:
                project_queries(word - QUERY)
            elif word > ROWS:
                query_copy(word - ROWS).wait_recv()
            elif word == ROWS and inner:
                rows_copy(0, 2, "e", 1).wait_recv()
                rows_copy(2, 3, "d", 2).start()
            elif word == ROWS:
                rows_copy(0, 2, "e", 1).start()
            else:
                relation, item, half = word // 16 % 4, word // 2 % 8, word % 2
                if word >= WAIT:
                    landing = view(relation, item, half)
                    pltpu.make_async_copy(landing, landing, arrive_sem.at[relation - 1, 2 * item + half]).wait()
                for place_of, link in enumerate("xyem"):
                    if word // 64 % 16 & (1 << place_of):
                        record = (relation, item, half, link, len(sent[place]))
                        sent[place].append(record)
                        piece_copy(*record).start()

    def service(index):
        for place in range(layers):
            if PLANS[place][index]:

                @pl.when(layer == place)
                def _():
                    serve(PLANS[place][index], place)

    weight_copy.wait()
    pl.semaphore_wait(barrier, 4 + middle.astype(jnp.int32))
    service(0)
    for copy in small_copies:
        copy.wait()
    out_weight_copy.wait()
    for head in range(2):
        obuf[0, head * head_size : (head + 1) * head_size, :] = raw[:, head, :]
    signal(token_sem.at[0], (partner, mp))

    def tokens_step(step):
        if step == 0:
            pl.semaphore_wait(token_sem.at[0], 1)
            signal(token_sem.at[1], (dp, flip(mp, 1)))
        elif step == 1:
            pl.semaphore_wait(token_sem.at[1], 1)
            signal(token_sem.at[2], (dp, flip(mp, 2)))
        else:
            hop = step - 3
            if hop < 0:
                pl.semaphore_wait(token_sem.at[2], 1)
            else:

                @pl.when(layer == hop + 1)
                def _():
                    pl.semaphore_wait(token_sem.at[3], 1)

                @pl.when(layer == layers - 2 - hop)
                def _():
                    pl.semaphore_wait(token_sem.at[4], 1)

            if hop + 1 < layers - 1:

                @pl.when(layer == hop + 1)
                def _():
                    signal(token_sem.at[3], (dp + 2, mp))

                @pl.when(layer == layers - 2 - hop)
                def _():
                    signal(token_sem.at[4], (dp - 2, mp))

    eye = lax.broadcasted_iota(jnp.int32, (masks, masks), 0) == lax.broadcasted_iota(
        jnp.int32, (masks, masks), 1
    )
    places = lax.broadcasted_iota(jnp.int32, (masks, seq_span), 1).astype(f32)

    def locate(which):
        length = lengths_ref[sequence_ref[which]].astype(f32)
        codes = codes_ref[pl.ds(which, 1), :].astype(f32)
        quotient = jnp.floor(codes / length)
        spots = codes - quotient * length
        spots = jnp.where(spots < 0.0, spots + length, spots)
        spots = jnp.where(spots >= length, spots - length, spots)
        spots = jnp.sum(jnp.where(eye, spots, 0.0), axis=1, keepdims=True)
        live = lax.broadcasted_iota(jnp.int32, (1, seq_span), 1).astype(f32) < length
        return places == spots, live

    located = [locate(which) for which in (me, mate, pair * n_mp + mp, (pair + 1 - 2 * core) * n_mp + mp)]
    chosen = located[0][0]
    alive = [live for _, live in located]
    tokens = tokens_ref[pl.ds(sequence_ref[me], 1), :].astype(f32)
    targets = jnp.sum(jnp.where(chosen, tokens, 0.0), axis=1, keepdims=True)
    onehots = [jnp.where(spots, 1.0, 0.0).astype(bf16) for spots, _ in located]
    onehot = onehots[0]

    hidden_copy.wait()
    tile = 128

    norm_copy = pltpu.make_async_remote_copy(
        src_ref=normed.at[0],
        dst_ref=normed.at[1],
        send_sem=norm_sem.at[0],
        recv_sem=norm_sem.at[1],
        device_id=(partner, mp),
        device_id_type=MESH,
    )

    def norm_rows(step, carry):
        rows = pl.ds(pl.multiple_of(step * tile, tile), tile)
        normed[0, rows, :] = (layer_norm(hidden[rows, :].astype(f32)) * gain_ref[...].reshape(1, feature)).astype(bf16)
        return carry

    lax.fori_loop(0, seq_span // tile, norm_rows, 0)
    rows_buf[0] = jnp.dot(onehot, normed[0], preferred_element_type=f32).astype(bf16)
    norm_copy.start()
    mixed[:masks, :] = jnp.dot(onehot, hidden[...], preferred_element_type=f32)
    mixed[masks:, :] = jnp.zeros((masks, feature), f32)
    rows_copy(0, 1, "d", 0).start()
    split_copy.wait()
    table = jnp.dot(jnp.concatenate(onehots, axis=0), split[...], preferred_element_type=f32)
    query_cos = table[:, :LANES] + table[:, LANES : 2 * LANES]
    query_sin = table[:, 2 * LANES : 3 * LANES] + table[:, 3 * LANES :]
    lane = lax.broadcasted_iota(jnp.int32, (1, LANES), 1)
    first = lane % head_size < head_size // 2
    low = lane < head_size
    transposed = (((1,), (1,)), ((), ()))

    def rotate(inputs, cosine, sine):
        turned = jnp.where(
            first,
            pltpu.roll(inputs, LANES - head_size // 2, 1),
            pltpu.roll(inputs, head_size // 2, 1),
        )
        return inputs * cosine + turned * sine

    span = seq_span

    def stack(refs):
        return jnp.concatenate([ref[...] for ref in refs], axis=0)

    def rows_of(start, count):
        return pl.ds(start if isinstance(start, int) else pl.multiple_of(start, head_size), count)

    def project(unit, buffer, slot):
        straight, turned = [], []
        for relation, head in unit:
            start = head * head_rows + head_size
            straight.append(wbuf[relation, rows_of(start, 2 * head_size), :])
            for offset, count in ((half_rows, half_rows), (0, half_rows), (head_size, head_size)):
                place = start + offset
                place = place if isinstance(place, int) else pl.multiple_of(place, half_rows)
                turned.append(wbuf[relation, pl.ds(place, count), :])
        keys = jnp.concatenate(straight + turned, axis=0)

        def step_of(step, carry):
            rows = pl.ds(pl.multiple_of(step * span, 16), span)
            made = lax.dot_general(normed[slot, rows, :], keys, transposed, preferred_element_type=f32)
            for head in range(2):
                block = made[:, head * LANES : (head + 1) * LANES] * cos[rows, :]
                block += made[:, (head + 2) * LANES : (head + 3) * LANES] * sin[rows, :]
                pbuf[buffer, slot, rows, head * LANES : (head + 1) * LANES] = block.astype(bf16)
            return carry

        lax.fori_loop(0, seq_span // span, step_of, 0)

    def queries(relation, low_slot, high_slot):
        weights = stack([wbuf.at[relation, head * head_rows : head * head_rows + head_size, :] for head in range(2)])
        rows = slice(low_slot * masks, high_slot * masks)
        source = rows_buf[low_slot:high_slot].reshape((high_slot - low_slot) * masks, feature)
        made = lax.dot_general(source, weights, transposed, preferred_element_type=f32)
        return rotate(made * head_size ** (-0.5), query_cos[rows], query_sin[rows]).astype(bf16)

    def project_queries(relation):
        if relation == 1:
            rows_copy(2, 3, "d", 2).wait_recv()
        made = queries(relation, 0, 4)
        gbuf[relation] = made[2 * masks :]
        qbuf[relation] = made[: 2 * masks]
        query_copy(relation).start()

    def of_head(query, head):
        query = query.astype(f32)
        if isinstance(head, int):
            return pltpu.roll(query, head_size, 1) if head else query
        return jnp.where(head == 1, pltpu.roll(query, head_size, 1), query)

    def attend(which, buffer, slot, near, far):
        empty = jnp.zeros((masks, LANES), bf16)
        near = jnp.where(low, near, 0.0).astype(bf16)
        far = jnp.where(low, far, 0.0).astype(bf16)
        both = jnp.concatenate(
            [jnp.concatenate([near, empty], axis=1), jnp.concatenate([empty, far], axis=1)], axis=0
        )
        block = pbuf[buffer, slot]
        logits = lax.dot_general(both, block, transposed, preferred_element_type=f32)
        logits = jnp.where(alive[slot], logits, -1e30)
        weight = jnp.exp(logits - jnp.max(logits, axis=-1, keepdims=True))
        probs = (weight / jnp.sum(weight, axis=-1, keepdims=True)).astype(bf16)
        vectors = jnp.dot(probs, block, preferred_element_type=f32)
        total = jnp.where(low, pltpu.roll(vectors[:masks, :LANES], head_size, 1), vectors[masks:, LANES:])
        context[slot * masks : (slot + 1) * masks, which * LANES : (which + 1) * LANES] = total.astype(bf16)

    def attend_both(which, unit, buffer):
        for slot in range(2):
            rows = slice(slot * masks, (slot + 1) * masks)
            near, far = [of_head(qbuf[relation, rows, :], head) for relation, head in unit]
            attend(which, buffer, slot, near, far)

    def mix(low_unit, *units):
        out_weights = stack([obuf.at[relation, rows_of(head * head_size, head_size), :] for unit in units for relation, head in unit])
        lanes = slice(low_unit * LANES, (low_unit + len(units)) * LANES)
        mixed[...] += jnp.dot(context[:, lanes], out_weights, preferred_element_type=f32)

    early = middle.astype(jnp.int32)
    own = ((0, 0), (0, 1))
    firsts = ((1, early), (2, early))
    seconds = ((1, 1 - early), (2, 1 - early))
    across = ((3, 0), (3, 1))

    cos_copy.wait()
    sin_copy.wait()
    service(1)
    project(own, 0, 0)
    service(2)
    query = queries(0, 0, 1)
    attend(0, 0, 0, of_head(query, 0), of_head(query, 1))
    tokens_step(0)
    service(3)
    norm_copy.wait_recv()
    rows_copy(0, 1, "d", 0).wait_recv()
    project(own, 0, 1)
    service(4)
    query = queries(0, 1, 2)
    attend(0, 0, 1, of_head(query, 0), of_head(query, 1))
    mix(0, own)
    tokens_step(1)
    service(5)
    project(firsts, 1, 0)
    service(6)
    project(firsts, 1, 1)
    tokens_step(2)
    service(7)
    attend_both(1, firsts, 1)
    tokens_step(3)
    service(8)
    project(seconds, 0, 0)
    service(9)
    project(seconds, 0, 1)
    service(10)
    attend_both(2, seconds, 0)
    tokens_step(4)
    service(11)
    project(across, 1, 0)
    service(12)
    project(across, 1, 1)
    service(13)
    attend_both(3, across, 1)
    tokens_step(5)
    service(14)
    out_weights = [
        obuf.at[relation, rows_of(head * head_size, head_size), :]
        for unit in (firsts, seconds, across)
        for relation, head in unit
    ]

    def inbox_copy(part):
        lanes = pl.ds(part * (feature // 2), feature // 2)
        return pltpu.make_async_remote_copy(
            src_ref=mixed.at[pl.ds(masks, masks), lanes],
            dst_ref=inbox.at[:, lanes],
            send_sem=swap_send_sem.at[3 + part],
            recv_sem=swap_sem.at[3 + part],
            device_id=(partner, mp),
            device_id_type=MESH,
        )

    for part in range(2):
        lanes = slice(part * (feature // 2), (part + 1) * (feature // 2))
        weights = jnp.concatenate([ref[:, lanes] for ref in out_weights], axis=0)
        mixed[:, lanes] += jnp.dot(context[:, LANES:], weights, preferred_element_type=f32)
        inbox_copy(part).start()
    dense_copy.wait()
    for copy in late_copies:
        copy.wait()
    inbox_copy(0).wait_recv()
    inbox_copy(1).wait_recv()
    residual = mixed[:masks, :] + inbox[...]
    normed_final = (layer_norm(residual) * final_gain_ref[...].reshape(1, feature)).astype(bf16)
    dense_out = jnp.dot(normed_final, dense[...], preferred_element_type=f32)
    headed = layer_norm(0.5 * dense_out * (1.0 + lax.erf(dense_out * 0.5**0.5))).astype(bf16)
    logits = lax.dot_general(headed, decoder_ref[...], transposed, preferred_element_type=f32) + bias_ref[...]
    largest = jnp.max(logits, axis=-1, keepdims=True)
    scale = jnp.log(jnp.sum(jnp.exp(logits - largest), axis=-1, keepdims=True)) + largest
    vocabulary = lax.broadcasted_iota(jnp.int32, logits.shape, 1).astype(f32)
    picked = jnp.sum(jnp.where(vocabulary == targets, logits - scale, 0.0), axis=1, keepdims=True)
    row = jnp.sum(jnp.where(eye, picked, 0.0), axis=0, keepdims=True)
    padded = jnp.concatenate([row] * (LANES // masks), axis=1)
    scores[me] = padded

    def score_copy(step):
        other_dp, other_mp = flip(dp, step // n_mp), flip(mp, step % n_mp)
        return pltpu.make_async_remote_copy(
            src_ref=scores.at[me],
            dst_ref=scores.at[me],
            send_sem=score_sem.at[0],
            recv_sem=score_sem.at[1],
            device_id=(other_dp, other_mp),
            device_id_type=MESH,
        )

    for step in reversed(range(1, devices)):
        score_copy(step).start()
    inbox_copy(0).wait_send()
    inbox_copy(1).wait_send()
    norm_copy.wait_send()
    rows_copy(0, 1, "d", 0).wait_send()

    for place in range(layers):

        @pl.when(layer == place)
        def _():
            for group in range(0, len(sent[place]), 12):
                count = min(12, len(sent[place]) - group)
                bulk = wbuf.at[0, pl.ds(0, count * half_rows), :]
                pltpu.make_async_copy(bulk, bulk, send_sem.at[group // 12]).wait()
            if 0 < place < layers - 1:
                rows_copy(2, 3, "d", 2).wait_send()
                for relation in (1, 2, 3):
                    query_copy(relation).wait_send()
            else:
                rows_copy(0, 2, "e", 1).wait_send()

    group = out_ref.shape[0]
    square = lax.broadcasted_iota(jnp.int32, (devices, devices), 0) == lax.broadcasted_iota(
        jnp.int32, (devices, devices), 1
    )
    owners = jnp.sum(jnp.where(square, owner_ref[...].astype(f32), 0.0), axis=1, keepdims=True)
    selects = [jnp.where(owners == (dp * group + place).astype(f32), 1.0, 0.0) for place in range(group)]
    everyone = scores.at[pl.ds(0, devices - 1)]
    pltpu.make_async_copy(everyone, everyone, score_sem.at[1]).wait()
    pltpu.make_async_copy(everyone, everyone, score_sem.at[0]).wait()
    gathered = scores[...].reshape(devices, LANES)
    result = jnp.concatenate([jnp.sum(gathered * select, axis=0, keepdims=True) for select in selects], axis=0)
    out_ref[...] = pltpu.roll(result, LANES - mp * out_ref.shape[1], 1)[:, : out_ref.shape[1]]


def split_call(shape, inputs, weight, out_weight, hidden, dense_weight, cosine, sine, group, head_size):
    n_dp, n_mp = shape
    devices = n_dp * n_mp
    seq_span, feature = hidden.shape
    width = weight.shape[1]
    masks = inputs[2].shape[1]
    high = [t.astype(jnp.bfloat16).astype(np.float32) for t in (cosine, sine)]
    parts = [high[0], cosine - high[0], high[1], sine - high[1]]
    split = np.concatenate(parts, axis=1).astype(jnp.bfloat16)
    dma = pltpu.SemaphoreType.DMA
    vmem = pl.BlockSpec(memory_space=pltpu.VMEM)
    anywhere = pl.BlockSpec(memory_space=pl.ANY)
    return pl.pallas_call(
        functools.partial(split_kernel, (n_dp, n_mp, head_size)),
        name="score_split",
        out_shape=jax.ShapeDtypeStruct((group, masks // n_mp), f32),
        in_specs=[anywhere] * 16,
        out_specs=vmem,
        scratch_shapes=[(pltpu.SMEM if place < 2 else pltpu.VMEM)(x.shape, x.dtype) for place, x in enumerate(inputs)]
        + [
            pltpu.VMEM((seq_span, feature), bf16),
            pltpu.VMEM((2, seq_span, feature), bf16),
            pltpu.VMEM((4, masks, feature), bf16),
            pltpu.VMEM((n_mp, width, feature), bf16),
            pltpu.VMEM((head_size, 2, feature), bf16),
            pltpu.VMEM((n_mp, 2 * head_size, feature), bf16),
            pltpu.VMEM((feature, feature), bf16),
            pltpu.VMEM((seq_span, LANES), f32),
            pltpu.VMEM((seq_span, LANES), f32),
            pltpu.VMEM((seq_span, 4 * LANES), bf16),
            pltpu.VMEM((2, 2, seq_span, 2 * LANES), bf16),
            pltpu.VMEM((2 * masks, 4 * LANES), bf16),
            pltpu.VMEM((n_mp, 2 * masks, LANES), bf16),
            pltpu.VMEM((n_mp, 2 * masks, LANES), bf16),
            pltpu.VMEM((2 * masks, feature), f32),
            pltpu.VMEM((masks, feature), f32),
            pltpu.VMEM((devices, 1, LANES), f32),
            dma((16,)),
            dma((6,)),
            dma((n_mp - 1, 16)),
            dma((2, n_mp - 1)),
            dma((2,)),
            dma((5,)),
            dma((5,)),
            dma((2,)),
            pltpu.SemaphoreType.REGULAR((5,)),
        ],
        compiler_params=pltpu.CompilerParams(collective_id=1, has_side_effects=True),
    )(
        *inputs,
        hidden,
        weight,
        out_weight,
        dense_weight,
        jnp.asarray(np.where(np.arange(LANES) < head_size, cosine, np.float32(1))),
        jnp.asarray(np.where(np.arange(LANES) < head_size, sine, np.float32(0))),
        jnp.asarray(split),
    )


def on_device(
    shape,
    hidden_states,
    ln_attn_gain,
    w_qkv,
    output_weight,
    ln_final_gain,
    dense_weight,
    decoder_weight,
    decoder_bias,
    seq_tokens,
    seq_lengths,
    copy_sequence,
    mask_code,
    copy_owner,
):
    n_dp, n_mp = shape
    devices = n_dp * n_mp
    lane_copies, seq_span, feature = hidden_states.shape
    head_size, heads, _ = output_weight.shape
    copies, masks = mask_code.shape
    assert lane_copies == 1 and copies == devices and n_dp % 2 == 0
    assert 2 * head_size == LANES and masks <= LANES
    in_chunk = 2 if heads % 2 == 0 else 1
    chunks = heads // in_chunk
    width = in_chunk * 3 * head_size
    weight = jnp.transpose(w_qkv.reshape(feature, chunks, width), (1, 2, 0))
    cosine, sine = rotary_tables(seq_span, head_size)
    group = copies // n_dp
    items = 2 * chunks + 2
    dma = pltpu.SemaphoreType.DMA
    vmem = pl.BlockSpec(memory_space=pltpu.VMEM)
    smem = pl.BlockSpec(memory_space=pltpu.SMEM)
    anywhere = pl.BlockSpec(memory_space=pl.ANY)
    own = masks // n_mp
    inputs = (
        copy_sequence,
        seq_lengths,
        mask_code,
        seq_tokens,
        copy_owner.reshape(1, -1),
        ln_attn_gain,
        ln_final_gain,
        decoder_weight.T,
        decoder_bias.reshape(1, -1),
    )
    if n_mp == 4 and n_dp == 8 and heads == 4 and seq_span % 128 == 0:
        hidden = hidden_states.reshape(seq_span, feature)
        return split_call(shape, inputs, weight, output_weight, hidden, dense_weight, cosine, sine, group, head_size)
    out_weight = jnp.swapaxes(output_weight, 0, 1).reshape(heads * head_size, feature)
    rows = pl.pallas_call(
        functools.partial(kernel, (n_dp, n_mp, head_size, in_chunk, chunks)),
        name="score_copies",
        out_shape=jax.ShapeDtypeStruct((group, LANES), f32),
        in_specs=[smem] * 2 + [vmem] * 7 + [anywhere] * 6,
        out_specs=vmem,
        scratch_shapes=[
            pltpu.VMEM((seq_span, feature), bf16),
            pltpu.VMEM((seq_span, feature), bf16),
            pltpu.VMEM((n_mp, chunks, width, feature), bf16),
            pltpu.VMEM((n_mp, heads * head_size, feature), bf16),
            pltpu.VMEM((feature, feature), bf16),
            pltpu.VMEM((seq_span, LANES), f32),
            pltpu.VMEM((seq_span, LANES), f32),
            pltpu.VMEM((seq_span, in_chunk * LANES), bf16),
            pltpu.VMEM((n_mp, chunks, masks, in_chunk * head_size), bf16),
            pltpu.VMEM((masks, feature), f32),
            pltpu.VMEM((devices, 8, LANES), f32),
            dma((6,)),
            dma((n_mp, items)),
            dma((items,)),
            dma((n_mp, chunks)),
            dma((n_mp, items)),
            dma((n_mp, items)),
            dma((n_mp, items)),
            dma((devices,)),
            dma((devices,)),
        ],
        compiler_params=pltpu.CompilerParams(collective_id=0, has_side_effects=True),
    )(
        copy_sequence,
        seq_lengths,
        mask_code,
        seq_tokens,
        copy_owner.reshape(1, -1),
        ln_attn_gain,
        ln_final_gain,
        decoder_weight.T,
        decoder_bias.reshape(1, -1),
        hidden_states.reshape(seq_span, feature),
        weight,
        out_weight,
        dense_weight,
        jnp.asarray(cosine),
        jnp.asarray(sine),
    )
    return lax.dynamic_slice_in_dim(rows, lax.axis_index("mp") * own, own, 1)


def solution(mesh):
    placed = (
        P(("dp", "mp"), None, None),
        P(),
        P(None, "mp", None),
        P(None, "mp", None),
        P(),
        P(),
        P(),
        P(),
        P(),
        P(),
        P(),
        P(),
        P(),
    )
    shape = (mesh.shape["dp"], mesh.shape["mp"])
    return jax.shard_map(
        functools.partial(on_device, shape),
        mesh=mesh,
        in_specs=placed,
        out_specs=P("dp", "mp"),
        check_vma=False,
    )
```
